32 devices in a mesh: dp: 8 (over z, x), seq: 4 (over y, core).
Axes of the slice: x: 2, y: 2, z: 4, core: 2. Of those that a mesh axis runs over, the one named last changes fastest.
Arguments:
- hidden_in: bfloat16 [8, 1536, 1280], P('dp', 'seq'), may hold values from -6 to 6
- cotangent: bfloat16 [8, 1536, 1280], P('dp', 'seq'), may hold values from -6 to 6
- clip_lengths: int32 [8], replicated, may hold values from 384 to 1500, as said below
- clip_order: int32 [8], P('dp'), may hold values from 0 to 7, each once
- first_gain: bfloat16 [1280], P('dp'), may hold values from 0.099609375 to 1.8984375
- first_shift: bfloat16 [1280], P('dp'), may hold values from -3 to 3
- query_weight: bfloat16 [1280, 1280], P('dp'), may hold values from -0.15625 to 0.15625
- query_bias: bfloat16 [1280], P('dp'), may hold values from -3 to 3
- key_weight: bfloat16 [1280, 1280], P('dp'), may hold values from -0.15625 to 0.15625
- value_weight: bfloat16 [1280, 1280], P('dp'), may hold values from -0.15625 to 0.15625
- value_bias: bfloat16 [1280], P('dp'), may hold values from -3 to 3
- output_weight: bfloat16 [1280, 1280], P('dp'), may hold values from -3.5 to 3.5
- output_bias: bfloat16 [1280], P('dp'), may hold values from -3 to 3
- second_gain: bfloat16 [1280], P('dp'), may hold values from 0.099609375 to 1.8984375
- second_shift: bfloat16 [1280], P('dp'), may hold values from -3 to 3
- expand_weight: bfloat16 [1280, 5120], P('dp'), may hold values from -0.15625 to 0.15625
- expand_bias: bfloat16 [5120], P('dp'), may hold values from -3 to 3
- reduce_weight: bfloat16 [5120, 1280], P('dp'), may hold values from -0.078125 to 0.078125
- reduce_bias: bfloat16 [1280], P('dp'), may hold values from -3 to 3
Outputs:
- layer_output: bfloat16 [8, 1536, 1280], P('dp', 'seq')
- input_grad: bfloat16 [8, 1536, 1280], P('dp', 'seq')
- first_gain_grad: float32 [1280], P('dp')
- first_shift_grad: float32 [1280], P('dp')
- query_weight_grad: float32 [1280, 1280], P('dp')
- query_bias_grad: float32 [1280], P('dp')
- key_weight_grad: float32 [1280, 1280], P('dp')
- value_weight_grad: float32 [1280, 1280], P('dp')
- value_bias_grad: float32 [1280], P('dp')
- output_weight_grad: float32 [1280, 1280], P('dp')
- output_bias_grad: float32 [1280], P('dp')
- second_gain_grad: float32 [1280], P('dp')
- second_shift_grad: float32 [1280], P('dp')
- expand_weight_grad: float32 [1280, 5120], P('dp')
- expand_bias_grad: float32 [5120], P('dp')
- reduce_weight_grad: float32 [5120, 1280], P('dp')
- reduce_bias_grad: float32 [1280], P('dp')
The draws below stay inside these ranges and needn't reach their ends.
Inputs may be any that keep to these rules, and one draw needn't show every extreme that they name: `clip_lengths`: some clip is exactly 1500 long and some other exactly 384. `clip_order`: A permutation of the clips.
All inputs are finite; a program needn't handle non-finite values.
Results may differ from the reference program's by a relative error of at most 0.018.
Values may be sent and summed in bfloat16 or wider, within the bound.
A program may use at most 256 MiB of HBM per device.

```python
import jax
import jax.numpy as jnp
from jax import lax

D = 1280
FF = 5120
HEADS = 16
HEAD_DIM = 80
SLOTS = 1536
CLIPS = 8
MAXLEN = 1500
MINLEN = 384


def draw_clip_lengths(key, part):
    lengths_drawn = jax.random.randint(jax.random.fold_in(key, 11), (CLIPS,), MINLEN, MAXLEN + 1, dtype=jnp.int32)
    longest = jax.random.randint(jax.random.fold_in(key, 12), (), 0, CLIPS, dtype=jnp.int32)
    offset = jax.random.randint(jax.random.fold_in(key, 13), (), 0, CLIPS - 1, dtype=jnp.int32)
    shortest = (longest + 1 + offset) % CLIPS
    clip_index = jnp.arange(CLIPS, dtype=jnp.int32)
    lengths_drawn = jnp.where(clip_index == longest, MAXLEN, lengths_drawn)
    return jnp.where(clip_index == shortest, MINLEN, lengths_drawn).astype(jnp.int32)


def level_of(rng, dims, cuts, smallest, largest):
    loudness = 1.0
    for axis_at, parts in cuts:
        draws = jax.random.uniform(jax.random.fold_in(jax.random.fold_in(rng, 6), axis_at), (parts,), jnp.float32, smallest / len(cuts), largest / len(cuts))
        loudness = loudness * jnp.repeat(jnp.exp(draws), dims[axis_at] // parts).reshape((-1,) + (1,) * (len(dims) - 1 - axis_at))
    return loudness


def centred(rng, shape, width, reach, cuts=(), kind=jnp.bfloat16):
    values = width * jax.random.normal(rng, shape, jnp.float32)
    if cuts:
        values = values * level_of(rng, shape, cuts, -0.22, 0.18)
    return jnp.clip(values, -reach, reach).astype(kind)


def setup_inputs(seed: int = 0) -> dict:
    seeds = jax.random.split(jax.random.key(seed), 20)
    return {
        "hidden_in": centred(seeds[0], (CLIPS, SLOTS, D), 1.0, 6.0, ((0, 8), (1, 4))),
        "cotangent": centred(seeds[1], (CLIPS, SLOTS, D), 1.0, 6.0, ((0, 8), (1, 4))),
        "clip_lengths": draw_clip_lengths(jax.random.fold_in(seeds[19], 71), 0),
        "clip_order": jax.random.permutation(seeds[3], CLIPS).astype(jnp.int32),
        "first_gain": jnp.clip(1.0 + 0.18 * jax.random.normal(seeds[4], (D,), jnp.float32), 0.099609375, 1.8984375).astype(jnp.bfloat16),
        "first_shift": centred(seeds[5], (D,), 0.5, 3.0, ((0, 8),)),
        "query_weight": centred(seeds[6], (D, D), D ** -0.5, 0.15625, ((0, 8),)),
        "query_bias": centred(seeds[7], (D,), 0.5, 3.0, ((0, 8),)),
        "key_weight": centred(seeds[8], (D, D), D ** -0.5, 0.15625, ((0, 8),)),
        "value_weight": centred(seeds[9], (D, D), D ** -0.5, 0.15625, ((0, 8),)),
        "value_bias": centred(seeds[10], (D,), 0.5, 3.0, ((0, 8),)),
        "output_weight": centred(seeds[11], (D, D), (max(1, D * 4 // SLOTS)) ** -0.5, 3.5, ((0, 8),)),
        "output_bias": centred(seeds[12], (D,), 0.5, 3.0, ((0, 8),)),
        "second_gain": jnp.clip(1.0 + 0.18 * jax.random.normal(seeds[13], (D,), jnp.float32), 0.099609375, 1.8984375).astype(jnp.bfloat16),
        "second_shift": centred(seeds[14], (D,), 0.5, 3.0, ((0, 8),)),
        "expand_weight": centred(seeds[15], (D, FF), D ** -0.5, 0.15625, ((0, 8),)),
        "expand_bias": centred(seeds[16], (FF,), 0.5, 3.0, ((0, 8),)),
        "reduce_weight": centred(seeds[17], (FF, D), FF ** -0.5, 0.078125, ((0, 8),)),
        "reduce_bias": centred(seeds[18], (D,), 0.5, 3.0, ((0, 8),)),
    }


@jax.custom_vjp
def low(v):
    return lax.optimization_barrier(v.astype(jnp.bfloat16)).astype(jnp.float32)

@jax.custom_vjp
def low_back(v):
    return v

def low_keep(v):
    return (low(v), None)

def low_pass(kept, grad):
    return (grad,)

def back_keep(v):
    return (v, None)

def back_low(kept, grad):
    return (low(grad),)
low.defvjp(low_keep, low_pass)
low_back.defvjp(back_keep, back_low)
EPSILON = 1e-05

def layer_norm(values, norm_gain, norm_shift):
    average = lax.optimization_barrier(jnp.mean(values, axis=-1, keepdims=True))
    centered = values - average
    variance = lax.optimization_barrier(jnp.mean(centered * centered, axis=-1, keepdims=True))
    return centered * lax.rsqrt(variance + EPSILON) * norm_gain + norm_shift

def matmul(left, right):
    return jnp.dot(left, right, precision=lax.Precision.HIGHEST, preferred_element_type=jnp.float32)

def attend_clip(queries, keys_all, values_all, length):
    key_valid = jnp.arange(SLOTS, dtype=jnp.int32) < length
    block_rows = min(SLOTS, 512)
    score_scale = HEAD_DIM ** (-0.5)
    blocks = queries.reshape(SLOTS // block_rows, block_rows, HEADS, HEAD_DIM)

    def one_block(query_block):
        scores = jnp.einsum('qhd,khd->hqk', query_block, keys_all, precision=lax.Precision.HIGHEST) * score_scale
        scores = low_back(scores)
        scores = jnp.where(key_valid[None, None, :], scores, -1e+30)
        probability = low(jax.nn.softmax(scores, axis=-1))
        return jnp.einsum('hqk,khd->qhd', probability, values_all, precision=lax.Precision.HIGHEST)
    mixture = lax.map(jax.checkpoint(one_block), blocks)
    return mixture.reshape(SLOTS, D)

def forward(hidden, params, length):
    first_gain, first_shift, query_weight, query_bias, key_weight, value_weight, value_bias, output_weight, output_bias, second_gain, second_shift, expand_weight, expand_bias, reduce_weight, reduce_bias = params
    normed = low(layer_norm(hidden, first_gain, first_shift))
    queries = low_back(low(matmul(normed, query_weight) + query_bias))
    keys_all = low_back(low(matmul(normed, key_weight)))
    values_all = low_back(low(matmul(normed, value_weight) + value_bias))
    mixture = attend_clip(queries.reshape(SLOTS, HEADS, HEAD_DIM), keys_all.reshape(SLOTS, HEADS, HEAD_DIM), values_all.reshape(SLOTS, HEADS, HEAD_DIM), length)
    mixture = low_back(low(mixture))
    branch = low_back(matmul(mixture, output_weight) + output_bias)
    middle = hidden + branch
    second = low(layer_norm(middle, second_gain, second_shift))
    expanded = low_back(matmul(second, expand_weight) + expand_bias)
    activated = low(jax.nn.gelu(expanded, approximate=False))
    branch_two = low_back(matmul(activated, reduce_weight) + reduce_bias)
    return middle + branch_two

def reference(hidden_in, cotangent, clip_lengths, clip_order, first_gain, first_shift, query_weight, query_bias, key_weight, value_weight, value_bias, output_weight, output_bias, second_gain, second_shift, expand_weight, expand_bias, reduce_weight, reduce_bias):
    params = tuple((entry.astype(jnp.float32) for entry in (first_gain, first_shift, query_weight, query_bias, key_weight, value_weight, value_bias, output_weight, output_bias, second_gain, second_shift, expand_weight, expand_bias, reduce_weight, reduce_bias)))
    lengths_stored = clip_lengths[clip_order.astype(jnp.int32)].astype(jnp.int32)
    positions = jnp.arange(SLOTS, dtype=jnp.int32)

    def one_clip(totals, clip_item):
        clip_hidden, clip_cot, length = clip_item

        def forward_clip(hidden, weights):
            return forward(hidden, weights, length)
        output, pullback = jax.vjp(forward_clip, clip_hidden.astype(jnp.float32), params)
        row_valid = (positions < length).astype(jnp.float32)
        grad_hidden, grad_params = pullback(clip_cot.astype(jnp.float32) * row_valid[:, None])
        totals = jax.tree.map(jnp.add, totals, grad_params)
        return (totals, (output.astype(jnp.bfloat16), grad_hidden.astype(jnp.bfloat16)))
    start = jax.tree.map(jnp.zeros_like, params)
    totals, (outputs, grads) = lax.scan(one_clip, start, (hidden_in, cotangent, lengths_stored))
    return (outputs, grads, totals[0], totals[1], totals[2], totals[3], totals[4], totals[5], totals[6], totals[7], totals[8], totals[9], totals[10], totals[11], totals[12], totals[13], totals[14])
```

```python
import functools

import jax
import jax.numpy as jnp
from jax import lax
from jax.experimental import pallas as pl
from jax.experimental.pallas import tpu as pltpu
from jax.sharding import PartitionSpec as P

D = 1280
FF = 5120
HEADS = 16
HEAD_DIM = D // HEADS
EPSILON = 1e-05
SCALE = HEAD_DIM ** (-0.5)
F32 = jnp.float32
BF16 = jnp.bfloat16
VMEM_LIMIT = 60 * 1024 * 1024


def dot(left, right, contract=((1,), (0,))):
    return lax.dot_general(left, right, (contract, ((), ())), preferred_element_type=F32)


def normalize(values):
    average = jnp.mean(values, axis=-1, keepdims=True)
    centered = values - average
    variance = jnp.mean(centered * centered, axis=-1, keepdims=True)
    spread = lax.rsqrt(variance + EPSILON)
    return centered * spread, spread


def norm_backward(unit, spread, grad_unit):
    inner = jnp.mean(grad_unit * unit, axis=-1, keepdims=True)
    return spread * (grad_unit - jnp.mean(grad_unit, axis=-1, keepdims=True) - unit * inner)


def params(**extra):
    return pltpu.CompilerParams(vmem_limit_bytes=VMEM_LIMIT, **extra)


def whole(shape):
    return pl.BlockSpec(shape, lambda *_: (0,) * len(shape), pipeline_mode=pl.Buffered(1))


def project_kernel(heads, x_ref, w_ref, gain_ref, shift_ref, bias_ref, normed_ref, qkv_ref):
    unit, _ = normalize(x_ref[...].astype(F32))
    normed = (unit * gain_ref[...] + shift_ref[...]).astype(BF16)
    normed_ref[...] = normed
    tokens = (dot(normed, w_ref[...]) + bias_ref[...]).astype(BF16)
    for item in range(3 * heads):
        qkv_ref[item] = tokens[:, item * HEAD_DIM : (item + 1) * HEAD_DIM]


def project(x, w, gain, shift, bias):
    slots = x.shape[0]
    items = w.shape[1] // HEAD_DIM
    block = 256
    return pl.pallas_call(
        functools.partial(project_kernel, items // 3),
        grid=(slots // block,),
        in_specs=[
            pl.BlockSpec((block, D), lambda i: (i, 0)),
            whole(w.shape),
            whole((1, D)),
            whole((1, D)),
            whole((1, w.shape[1])),
        ],
        out_specs=[
            pl.BlockSpec((block, D), lambda i: (i, 0)),
            pl.BlockSpec((items, block, HEAD_DIM), lambda i: (0, i, 0)),
        ],
        out_shape=[
            jax.ShapeDtypeStruct((slots, D), BF16),
            jax.ShapeDtypeStruct((items, slots, HEAD_DIM), BF16),
        ],
        compiler_params=params(),
        name="project",
    )(x, w, gain, shift, bias)


def attend_kernel(heads, slots, length_ref, q_ref, k_ref, v_ref, mix_ref, lse_ref, own_ref):
    length = length_ref[0]
    block = q_ref.shape[1]
    invalid = lax.broadcasted_iota(jnp.int32, (1, slots), 1) >= length

    def one_head(head, _):
        scores = dot(q_ref[head], k_ref[head], ((1,), (1,))) * SCALE
        scores = jnp.where(invalid, -1e30, scores)
        top = jnp.max(scores, axis=-1, keepdims=True)
        exponent = jnp.exp(scores - top)
        total = jnp.sum(exponent, axis=-1, keepdims=True)
        mixed = dot(exponent.astype(BF16), v_ref[head])
        own_ref[head] = mixed / total
        lse_ref[head] = jnp.transpose(top + jnp.log(total))
        return 0

    lax.fori_loop(0, heads, one_head, 0)
    for head in range(heads):
        mix_ref[:, head * HEAD_DIM : (head + 1) * HEAD_DIM] = own_ref[head].astype(BF16)


def attend(qkv, length):
    items, slots, _ = qkv.shape
    heads = items // 3
    block = 256
    return pl.pallas_call(
        functools.partial(attend_kernel, heads, slots),
        grid_spec=pltpu.PrefetchScalarGridSpec(
            num_scalar_prefetch=1,
            grid=(slots // block,),
            in_specs=[
                pl.BlockSpec((heads, block, HEAD_DIM), lambda i, n: (0, i, 0)),
                pl.BlockSpec((heads, slots, HEAD_DIM), lambda i, n: (1, 0, 0)),
                pl.BlockSpec((heads, slots, HEAD_DIM), lambda i, n: (2, 0, 0)),
            ],
            out_specs=[
                pl.BlockSpec((block, heads * HEAD_DIM), lambda i, n: (i, 0)),
                pl.BlockSpec((heads, 1, block), lambda i, n: (0, 0, i)),
            ],
            scratch_shapes=[pltpu.VMEM((heads, block, HEAD_DIM), F32)],
        ),
        out_shape=[
            jax.ShapeDtypeStruct((slots, heads * HEAD_DIM), BF16),
            jax.ShapeDtypeStruct((heads, 1, slots), F32),
        ],
        compiler_params=params(),
        name="attend",
    )(length, qkv, qkv, qkv)


def attend_back_kernel(
    slots, length_ref, q_ref, k_ref, v_ref, go_ref, mix_ref, lse_ref,
    dq_ref, dk_ref, dv_ref, turned_ref, dk_sum, dv_sum,
):
    step = pl.program_id(1)
    length = length_ref[0]

    @pl.when(step == 0)
    def _():
        turned_ref[...] = jnp.transpose(k_ref[0])
        dk_sum[...] = jnp.zeros_like(dk_sum)
        dv_sum[...] = jnp.zeros_like(dv_sum)

    invalid = lax.broadcasted_iota(jnp.int32, (slots, 1), 0) >= length
    query = q_ref[0]
    grad = go_ref[0]
    delta = jnp.sum(
        jnp.transpose(grad.astype(F32) * mix_ref[0].astype(F32)), axis=0, keepdims=True
    )
    scores = dot(k_ref[0], query, ((1,), (1,))) * SCALE
    probs = jnp.where(invalid, 0.0, jnp.exp(scores - lse_ref[0]))
    grad_probs = dot(v_ref[0], grad, ((1,), (1,)))
    grad_scores = (probs * (grad_probs - delta)).astype(BF16)
    dv_sum[...] += dot(probs.astype(BF16), grad)
    dk_sum[...] += dot(grad_scores, query)
    dq_ref[0] = (jnp.transpose(dot(turned_ref[...], grad_scores)) * SCALE).astype(BF16)

    @pl.when(step == pl.num_programs(1) - 1)
    def _():
        dk_ref[0] = (dk_sum[...] * SCALE).astype(BF16)
        dv_ref[0] = dv_sum[...].astype(BF16)


def attend_back(qkv, length, grad_mix, mix, lse):
    items, slots, _ = qkv.shape
    heads = items // 3
    block = 256
    part = jax.ShapeDtypeStruct((heads, slots, HEAD_DIM), BF16)
    per_block = pl.BlockSpec((1, block, HEAD_DIM), lambda h, i, n: (h, i, 0))
    per_head = pl.BlockSpec((1, slots, HEAD_DIM), lambda h, i, n: (h, 0, 0))
    return pl.pallas_call(
        functools.partial(attend_back_kernel, slots),
        grid_spec=pltpu.PrefetchScalarGridSpec(
            num_scalar_prefetch=1,
            grid=(heads, slots // block),
            in_specs=[
                per_block,
                pl.BlockSpec((1, slots, HEAD_DIM), lambda h, i, n: (heads + h, 0, 0)),
                pl.BlockSpec((1, slots, HEAD_DIM), lambda h, i, n: (2 * heads + h, 0, 0)),
                per_block,
                per_block,
                pl.BlockSpec((1, 1, block), lambda h, i, n: (h, 0, i)),
            ],
            out_specs=[per_block, per_head, per_head],
            scratch_shapes=[
                pltpu.VMEM((HEAD_DIM, slots), BF16),
                pltpu.VMEM((slots, HEAD_DIM), F32),
                pltpu.VMEM((slots, HEAD_DIM), F32),
            ],
        ),
        out_shape=[part, part, part],
        compiler_params=params(),
        name="attend_back",
    )(length, qkv, qkv, qkv, grad_mix, mix, lse)


def feed_kernel(
    place_ref, x_ref, mix_ref, cot_ref, wo_ref, w1_ref, w2_ref, bo_ref, gain_ref, shift_ref, b1_ref,
    out_ref, ds_ref, second_ref, act_ref, de_ref, middle_ref, gain_sum, shift_sum, b1_sum,
):
    step = pl.program_id(0)
    count = pl.num_programs(0)
    block = x_ref.shape[0]
    owner = lax.rem(place_ref[0] + 1 + step, count)

    @pl.when(step == 0)
    def _():
        gain_sum[...] = jnp.zeros_like(gain_sum)
        shift_sum[...] = jnp.zeros_like(shift_sum)
        b1_sum[...] = jnp.zeros_like(b1_sum)

    middle = x_ref[...].astype(F32) + (dot(mix_ref[...], wo_ref[...]) + bo_ref[...])
    middle_ref[...] = middle
    unit, _ = normalize(middle)
    second = (unit * gain_ref[...] + shift_ref[...]).astype(BF16)
    second_ref[...] = second
    valid = owner * block + lax.broadcasted_iota(jnp.int32, (block, 1), 0) < place_ref[1]
    grad_two = jnp.where(valid, cot_ref[...].astype(F32), 0.0).astype(BF16)
    expanded = dot(second, w1_ref[...]) + b1_ref[...]
    phi = 0.5 * (1.0 + lax.erf(expanded * (0.5**0.5)))
    activated = (expanded * phi).astype(BF16)
    act_ref[...] = activated
    slope = phi + expanded * (jnp.exp(-0.5 * expanded * expanded) * 0.3989422804014327)
    out_ref[...] = dot(activated, w2_ref[...]).astype(BF16)
    grad_act = dot(grad_two, w2_ref[...], ((1,), (1,)))
    grad_expanded = (grad_act * slope).astype(BF16)
    de_ref[...] = grad_expanded
    b1_sum[...] += jnp.sum(grad_expanded.astype(F32), axis=0, keepdims=True)
    grad_second = dot(grad_expanded, w1_ref[...], ((1,), (1,)))
    ds_ref[...] = grad_second.astype(BF16)
    gain_sum[...] += jnp.sum(grad_second * unit, axis=0, keepdims=True)
    shift_sum[...] += jnp.sum(grad_second, axis=0, keepdims=True)


def feed(place, count, x, mix, cot, wo, w1, w2, bo, gain, shift, b1):
    slots = x.shape[0]
    block = slots // count
    width = w1.shape[1]

    def turn(i, place):
        return lax.rem(place[0] + 1 + i, count)

    rows = pl.BlockSpec((block, D), lambda i, p: (turn(i, p), 0))
    wide = pl.BlockSpec((block, width), lambda i, p: (turn(i, p), 0))
    return pl.pallas_call(
        feed_kernel,
        grid_spec=pltpu.PrefetchScalarGridSpec(
            num_scalar_prefetch=1,
            grid=(count,),
            in_specs=[rows, rows, rows, whole(wo.shape), whole(w1.shape), whole(w2.shape)]
            + [whole((1, D))] * 3
            + [whole((1, width))],
            out_specs=[
                rows,
                rows,
                rows,
                wide,
                wide,
                pl.BlockSpec((block, D), lambda i, p: (0, 0)),
                pl.BlockSpec((1, D), lambda i, p: (0, 0)),
                pl.BlockSpec((1, D), lambda i, p: (0, 0)),
                pl.BlockSpec((1, width), lambda i, p: (0, 0)),
            ],
        ),
        out_shape=[
            jax.ShapeDtypeStruct((slots, D), BF16),
            jax.ShapeDtypeStruct((slots, D), BF16),
            jax.ShapeDtypeStruct((slots, D), BF16),
            jax.ShapeDtypeStruct((slots, width), BF16),
            jax.ShapeDtypeStruct((slots, width), BF16),
            jax.ShapeDtypeStruct((block, D), F32),
            jax.ShapeDtypeStruct((1, D), F32),
            jax.ShapeDtypeStruct((1, D), F32),
            jax.ShapeDtypeStruct((1, width), F32),
        ],
        compiler_params=params(),
        name="feed",
    )(place, x, mix, cot, wo, w1, w2, bo, gain, shift, b1)


def gather(value, axes, axis=0):
    return lax.all_gather(value, axes, axis=axis, tiled=True)


def scatter_sum(value, axes, axis=0):
    return lax.psum_scatter(value, axes, scatter_dimension=axis, tiled=True)


def per_device(
    hidden_in, cotangent, clip_lengths, clip_order, first_gain, first_shift, query_weight,
    query_bias, key_weight, value_weight, value_bias, output_weight, output_bias, second_gain,
    second_shift, expand_weight, expand_bias, reduce_weight, reduce_bias,
):
    dp = lax.axis_size("dp")
    seq = lax.axis_size("seq")
    me = lax.axis_index("seq")
    rows_here = hidden_in.shape[1]
    slots = rows_here * seq
    share = D // dp
    head_cols = D // seq
    heads = HEADS // seq
    units = FF // (dp * seq)
    quarter = dp * units

    hidden_own = hidden_in[0]
    matches = clip_order[0] == jnp.arange(clip_lengths.shape[0], dtype=jnp.int32)
    length = jnp.sum(jnp.where(matches, clip_lengths, 0)).reshape(1)

    def columns(weight):
        return lax.dynamic_slice_in_dim(weight, me * head_cols, head_cols, 1)

    small = jnp.concatenate(
        [first_gain, first_shift, query_bias, value_bias, output_bias, second_gain, second_shift,
         reduce_bias, expand_bias]
    )
    width = 3 * head_cols
    extra = -(-small.shape[0] // width)
    tall = -(-(share + extra) // 16) * 16
    small = jnp.pad(small, (0, (tall - share) * width - small.shape[0])).reshape(-1, width)
    qkv_share = jnp.concatenate(
        [columns(query_weight), columns(key_weight), columns(value_weight)], axis=1
    )
    packed = gather(jnp.concatenate([qkv_share, small], axis=0), "dp").reshape(dp, tall, width)
    w_qkv = packed[:, :share].reshape(D, width)
    flat = packed[:, share : share + extra].reshape(dp, extra * width)

    def vector(index, size=share):
        return flat[:, index * share : index * share + size].reshape(1, dp * size).astype(F32)

    gain_one, shift_one, bias_query, bias_value, bias_out, gain_two, shift_two, bias_reduce = (
        vector(i) for i in range(8)
    )
    expand_all = flat[:, 8 * share : 8 * share + FF // dp]
    bias_expand = lax.dynamic_slice_in_dim(expand_all, me * units, units, 1)
    bias_expand = bias_expand.reshape(1, quarter).astype(F32)
    bias_qkv = jnp.concatenate(
        [columns(bias_query), jnp.zeros((1, head_cols), F32), columns(bias_value)], axis=1
    )

    x = gather(hidden_own, "seq")
    cot = gather(cotangent[0], "seq")
    wo_share = lax.dynamic_slice_in_dim(output_weight, me * (share // seq), share // seq, 0)
    w_out = gather(wo_share, ("dp", "seq"))
    w1_share = jnp.concatenate(
        [
            lax.dynamic_slice_in_dim(expand_weight, d * (FF // dp) + me * units, units, 1)
            for d in range(dp)
        ],
        axis=1,
    )
    w2_share = lax.dynamic_slice_in_dim(reduce_weight, me * units, units, 0)
    w_expand = gather(w1_share, "dp")
    w_reduce = gather(w2_share, "dp")

    normed, qkv = project(x, w_qkv, gain_one, shift_one, bias_qkv)
    mix_own, lse = attend(qkv, length)
    mix = gather(mix_own, "seq", axis=1)
    place = jnp.stack([me.astype(jnp.int32), length[0]])
    (
        out_part, ds_part, second, act, grad_expanded, middle_own, gain_two_grad, shift_two_grad,
        bias_expand_grad,
    ) = feed(
        place, seq, x, mix, cot, w_out, w_expand, w_reduce, bias_out, gain_two, shift_two,
        bias_expand,
    )
    positions = jnp.arange(slots, dtype=jnp.int32)
    valid = (positions < length)[:, None]
    grad_two = jnp.where(valid, cot, 0).astype(BF16)
    grad_out = lax.dynamic_slice_in_dim(grad_two, me * rows_here, rows_here, 0).astype(F32)

    layer_output = (
        middle_own + (scatter_sum(out_part, "seq").astype(F32) + bias_reduce)
    ).astype(BF16)
    grad_second = scatter_sum(ds_part, "seq").astype(F32)
    unit_two, spread_two = normalize(middle_own)
    grad_middle = grad_out + norm_backward(unit_two, spread_two, grad_second * gain_two)
    grad_branch = grad_middle.astype(BF16)
    reduce_bias_grad = jnp.sum(grad_out, axis=0)
    output_bias_grad = jnp.sum(grad_branch.astype(F32), axis=0)

    w1_grad = dot(second, grad_expanded, ((0,), (0,))).astype(BF16)
    w2_grad = dot(act, grad_two, ((0,), (0,))).astype(BF16)
    w1_grad = scatter_sum(w1_grad, "dp")
    w2_grad = scatter_sum(w2_grad, "dp")

    grad_branch_all = gather(grad_branch, "seq")
    wo_grad = dot(mix, columns(grad_branch_all), ((0,), (0,))).astype(BF16)
    wo_rows = lax.dynamic_slice_in_dim(w_out, me * head_cols, head_cols, 0)
    grad_mix = dot(grad_branch_all, wo_rows, ((1,), (1,))).astype(BF16)

    def split_heads(value):
        return value.reshape(slots, heads, HEAD_DIM).transpose(1, 0, 2)

    dq, dk, dv = attend_back(qkv, length, split_heads(grad_mix), split_heads(mix_own), lse)
    dqkv = jnp.concatenate([dq, dk, dv], axis=0).transpose(1, 0, 2).reshape(slots, width)
    qkv_grad = dot(normed, dqkv, ((0,), (0,))).astype(BF16)
    bias_qkv_grad = jnp.sum(dqkv.astype(F32), axis=0)
    grad_normed = dot(dqkv, w_qkv, ((1,), (1,)))
    unit_all, _ = normalize(x.astype(F32))
    gain_one_grad = jnp.sum(grad_normed * unit_all, axis=0)
    shift_one_grad = jnp.sum(grad_normed, axis=0)
    grad_normed_own = scatter_sum(grad_normed.astype(BF16), "seq").astype(F32)
    unit_one, spread_one = normalize(hidden_own.astype(F32))
    grad_front = grad_middle + norm_backward(unit_one, spread_one, grad_normed_own * gain_one)
    input_grad = grad_front.astype(BF16)

    def mine(value):
        return lax.dynamic_update_slice_in_dim(
            jnp.zeros((D,), F32), value.reshape(-1), me * head_cols, 0
        )

    expand_vec = lax.dynamic_update_slice_in_dim(
        jnp.zeros((dp, FF // dp), F32), bias_expand_grad.reshape(dp, units), me * units, 1
    )
    vectors = [
        gain_one_grad, shift_one_grad, mine(bias_qkv_grad[:head_cols]),
        mine(bias_qkv_grad[2 * head_cols :]), output_bias_grad, gain_two_grad.reshape(-1),
        shift_two_grad.reshape(-1), reduce_bias_grad,
    ]
    small_grad = jnp.concatenate([v.reshape(dp, share) for v in vectors] + [expand_vec], axis=1)
    small_grad = jnp.pad(
        small_grad.astype(BF16), ((0, 0), (0, (tall - share) * width - small_grad.shape[1]))
    ).reshape(dp, tall - share, width)
    packed_grad = jnp.concatenate([qkv_grad.reshape(dp, share, width), small_grad], axis=1)
    packed_grad = scatter_sum(packed_grad, "dp")[0]
    wo_grad = scatter_sum(wo_grad, "dp")

    packed_grad = gather(packed_grad[None], "seq")
    wo_grad = gather(wo_grad[None], "seq")
    w1_grad = gather(w1_grad[None], "seq")
    w2_grad = gather(w2_grad, "seq").astype(F32)
    w1_grad = (
        w1_grad.reshape(seq, share, dp, units).transpose(1, 2, 0, 3).reshape(share, FF).astype(F32)
    )
    wo_grad = wo_grad.transpose(1, 0, 2).reshape(share, D).astype(F32)
    qkv_grad = packed_grad[:, :share].reshape(seq, share, 3, head_cols).astype(F32)
    qkv_grad = qkv_grad.transpose(2, 1, 0, 3).reshape(3, share, D)
    small_grad = jnp.sum(
        packed_grad[:, share : share + extra].reshape(seq, extra * width).astype(F32), axis=0
    )
    pieces = [small_grad[i * share : (i + 1) * share] for i in range(8)]
    expand_bias_grad = small_grad[8 * share : 8 * share + FF // dp]
    return (
        layer_output[None],
        input_grad[None],
        pieces[0],
        pieces[1],
        qkv_grad[0],
        pieces[2],
        qkv_grad[1],
        qkv_grad[2],
        pieces[3],
        wo_grad,
        pieces[4],
        pieces[5],
        pieces[6],
        w1_grad,
        expand_bias_grad,
        w2_grad,
        pieces[7],
    )


def solution(mesh):
    clip = P("dp", "seq", None)
    vec = P("dp")
    mat = P("dp", None)
    return jax.shard_map(
        per_device,
        mesh=mesh,
        in_specs=(
            clip, clip, P(), vec, vec, vec, mat, vec, mat, mat, vec, mat, vec, vec, vec, mat, vec,
            mat, vec,
        ),
        out_specs=(
            clip, clip, vec, vec, mat, vec, mat, mat, vec, mat, vec, vec, vec, mat, vec, mat, vec,
        ),
        check_vma=False,
    )
```

```python
import functools

import jax
import jax.numpy as jnp
from jax import lax
from jax.experimental import pallas as pl
from jax.experimental.pallas import tpu as pltpu
from jax.sharding import PartitionSpec as P

D = 1280
FF = 5120
HEADS = 16
HEAD_DIM = D // HEADS
EPSILON = 1e-05
SCALE = HEAD_DIM ** (-0.5)
F32 = jnp.float32
BF16 = jnp.bfloat16
VMEM_LIMIT = 60 * 1024 * 1024
MESH = pl.DeviceIdType.MESH


def dot(left, right, contract=((1,), (0,))):
    return lax.dot_general(left, right, (contract, ((), ())), preferred_element_type=F32)


def normalize(values):
    average = jnp.mean(values, axis=-1, keepdims=True)
    centered = values - average
    variance = jnp.mean(centered * centered, axis=-1, keepdims=True)
    spread = lax.rsqrt(variance + EPSILON)
    return centered * spread, spread


def norm_backward(unit, spread, grad_unit):
    inner = jnp.mean(grad_unit * unit, axis=-1, keepdims=True)
    return spread * (grad_unit - jnp.mean(grad_unit, axis=-1, keepdims=True) - unit * inner)


def params(**extra):
    return pltpu.CompilerParams(vmem_limit_bytes=VMEM_LIMIT, **extra)


def whole(shape):
    return pl.BlockSpec(shape, lambda *_: (0,) * len(shape), pipeline_mode=pl.Buffered(1))


def chunk_of(slots):
    return slots // 4 if slots % 512 == 0 else slots


class Place:
    def __init__(self, dp, seq):
        self.dp, self.seq = dp, seq
        self.xs = 1 << ((dp.bit_length() - 1) // 2)
        self.zs = dp // self.xs
        self.ys = seq // 2

    def locate(self):
        self.d, self.s = lax.axis_index("dp"), lax.axis_index("seq")
        self.z, self.x = self.d // self.xs, lax.rem(self.d, self.xs)
        self.y, self.c = self.s // 2, lax.rem(self.s, 2)
        self.partner = self.y * 2 + 1 - self.c

    def at_z(self, k):
        return lax.rem(self.z + k + self.zs, self.zs) * self.xs + self.x

    def block(self, k, j):
        return lax.rem(self.z - k + self.zs, self.zs) * self.xs + lax.rem(
            self.x - j + self.xs, self.xs
        )

    def at_x(self, j):
        return self.z * self.xs + lax.rem(self.x + j, self.xs)

    def at_y(self, j, core):
        return lax.rem(self.y + j + self.ys, self.ys) * 2 + core

    def peers(self, over_dp=True, over_seq=True):
        found = []
        if over_dp:
            found += [(self.at_z(k), self.s) for k in range(1, self.zs)]
            found += [(self.at_x(j), self.s) for j in range(1, self.xs)]
        if over_seq:
            found += [(self.d, self.partner)]
            found += [(self.d, self.at_y(j, self.c)) for j in range(1, self.ys)]
        return found

    def barrier(self, **which):
        semaphore = pltpu.get_barrier_semaphore()
        peers = self.peers(**which)
        for peer in peers:
            pl.semaphore_signal(semaphore, inc=1, device_id=peer, device_id_type=MESH)
        pl.semaphore_wait(semaphore, len(peers))


def send(src, dst, send_sem, recv_sem, device):
    return pltpu.make_async_remote_copy(
        src_ref=src, dst_ref=dst, send_sem=send_sem, recv_sem=recv_sem, device_id=device,
        device_id_type=MESH,
    )


def dp_semaphores(place, groups):
    return [
        pltpu.SemaphoreType.DMA((groups, place.zs)),
        pltpu.SemaphoreType.DMA((groups, place.zs)),
        pltpu.SemaphoreType.DMA((groups, place.zs, place.xs)),
        pltpu.SemaphoreType.DMA((groups, place.zs, place.xs)),
    ]


def seq_semaphores(place, groups):
    return [pltpu.SemaphoreType.DMA((groups, 2, place.ys))] * 2


class GatherDp:
    def __init__(self, place, group, sems, own, slab):
        self.p, self.g, self.own, self.slab = place, group, own, slab
        self.zsend, self.zrecv, self.xsend, self.xrecv = sems

    def z_copy(self, k):
        src = self.own
        return send(src, self.slab(self.p.d), self.zsend.at[self.g, k], self.zrecv.at[self.g, k],
                    (self.p.at_z(k), self.p.s))

    def x_copy(self, k, j):
        block = self.p.block(k, 0)
        src = self.own if k == 0 else self.slab(block)
        return send(src, self.slab(block), self.xsend.at[self.g, k, j],
                    self.xrecv.at[self.g, k, j], (self.p.at_x(j), self.p.s))

    def start(self):
        for j in range(1, self.p.xs):
            self.x_copy(0, j).start()
        for k in range(self.p.zs - 1, 0, -1):
            self.z_copy(k).start()

    def forward(self, k):
        place = self.p
        send(self.own, self.slab(place.block(k, 0)), self.zsend.at[self.g, k],
             self.zrecv.at[self.g, k], (place.at_z(k), place.s)).wait_recv()
        for j in range(1, place.xs):
            self.x_copy(k, j).start()

    def forward_all(self):
        for k in range(1, self.p.zs):
            self.forward(k)

    def arrive(self):
        place = self.p
        for k in range(place.zs):
            for j in range(1, place.xs):
                send(self.own, self.slab(place.block(k, j)), self.xsend.at[self.g, k, j],
                     self.xrecv.at[self.g, k, j], (place.at_x(j), place.s)).wait_recv()

    def drain(self):
        place = self.p
        for k in range(1, place.zs):
            self.z_copy(k).wait_send()
        for k in range(place.zs):
            for j in range(1, place.xs):
                self.x_copy(k, j).wait_send()


class GatherSeq:
    def __init__(self, place, group, sems, own, slab):
        self.p, self.g, self.own, self.slab = place, group, own, slab
        self.sends, self.recvs = sems

    def y_copy(self, j):
        place = self.p
        return send(self.own, self.slab(place.s), self.sends.at[self.g, 0, j],
                    self.recvs.at[self.g, 0, j], (place.d, place.at_y(j, place.c)))

    def core_copy(self, j):
        place = self.p
        block = place.at_y(-j, place.c)
        src = self.own if j == 0 else self.slab(block)
        return send(src, self.slab(block), self.sends.at[self.g, 1, j],
                    self.recvs.at[self.g, 1, j], (place.d, place.partner))

    def start(self):
        for j in range(1, self.p.ys):
            self.y_copy(j).start()
        self.core_copy(0).start()

    def arrive_y(self, j):
        place = self.p
        block = place.at_y(-j, place.c)
        send(self.own, self.slab(block), self.sends.at[self.g, 0, j], self.recvs.at[self.g, 0, j],
             (place.d, place.at_y(j, place.c))).wait_recv()
        self.core_copy(j).start()
        return block

    def arrive_core(self, j):
        place = self.p
        block = place.at_y(-j, 1 - place.c)
        send(self.own, self.slab(block), self.sends.at[self.g, 1, j], self.recvs.at[self.g, 1, j],
             (place.d, place.partner)).wait_recv()
        return block

    def drain(self):
        for j in range(1, self.p.ys):
            self.y_copy(j).wait_send()
        for j in range(self.p.ys):
            self.core_copy(j).wait_send()


LOG2E = 1.4426950408889634
QSCALE = SCALE * LOG2E


def front_kernel(
    place, length_ref, x_in, cot_in, sm_in, wq_in, wo_in, w1_in, w2_in,
    x_out, cot_out, sm_out, wq_out, wo_out, w1_out, w2_out, normed_out, qt_out, kt_out, k_out,
    v_out, mix_out, lse_ref,
    xs, nr, sm, wq, wt, qt, kt, vt, kn, vn, mix,
    zsend, zrecv, xsend, xrecv, ssend, srecv, local,
):
    place.locate()
    seq, rows = x_out.shape[0], x_out.shape[1]
    slots = seq * rows
    heads = k_out.shape[0]
    wide = heads * HEAD_DIM
    place.barrier()
    dp_sems = (zsend, zrecv, xsend, xrecv)
    seq_sems = (ssend, srecv)

    def over_dp(group, own, buffer):
        return GatherDp(place, group, dp_sems, own, lambda d: buffer.at[d])

    def over_seq(group, own, buffer):
        return GatherSeq(place, group, seq_sems, own, lambda s: buffer.at[s])

    g_sm = over_dp(0, sm_in, sm)
    g_wq = over_dp(1, wq_in, wq)
    g_wo = over_dp(2, wo_in, wo_out)
    g_w1 = over_dp(3, w1_in, w1_out)
    g_w2 = over_dp(4, w2_in, w2_out)
    g_x = over_seq(0, x_in, xs)
    g_cot = over_seq(1, cot_in, cot_out)

    locals_in = [
        pltpu.make_async_copy(x_in, xs.at[place.s], local.at[0]),
        pltpu.make_async_copy(sm_in, sm.at[place.d], local.at[1]),
        pltpu.make_async_copy(wq_in, wq.at[place.d], local.at[2]),
    ]
    own_blocks = [
        pltpu.make_async_copy(cot_in, cot_out.at[place.s], local.at[3]),
        pltpu.make_async_copy(wo_in, wo_out.at[place.d], local.at[4]),
        pltpu.make_async_copy(w1_in, w1_out.at[place.d], local.at[5]),
        pltpu.make_async_copy(w2_in, w2_out.at[place.d], local.at[6]),
    ]
    for copy in locals_in:
        copy.start()
    g_sm.start()
    g_x.start()
    g_wq.start()
    for copy in own_blocks:
        copy.start()

    column = lax.broadcasted_iota(jnp.int32, (slots, 1), 0)
    penalty = jnp.where(column >= length_ref[0], -1e30, 0.0).astype(BF16)
    ones_row = jnp.where(
        lax.broadcasted_iota(jnp.int32, (128 - HEAD_DIM, slots), 0) == 0, 1.0, 0.0
    ).astype(BF16)
    for head in range(heads):
        kn[head] = jnp.zeros((slots, 128), BF16)
        kn[head, :, HEAD_DIM : HEAD_DIM + 1] = penalty
        qt[head, HEAD_DIM:, :] = ones_row

    for copy in locals_in:
        copy.wait()
    g_sm.forward_all()
    g_wq.forward_all()
    g_wo.start()
    g_w1.start()
    g_cot.start()
    g_sm.arrive()
    vectors = jnp.sum(sm[...].astype(F32), axis=0)
    gain, shift = vectors[0:1], vectors[1:2]

    def norm_block(block):
        unit, _ = normalize(xs[block].astype(F32))
        lines = pl.ds(pl.multiple_of(block * rows, 16), rows)
        nr[lines, :] = (unit * gain + shift).astype(BF16)

    norm_block(place.s)
    norm_block(g_x.arrive_core(0))
    for j in range(1, place.ys):
        norm_block(g_x.arrive_y(j))
        norm_block(g_x.arrive_core(j))
    g_wq.arrive()
    share = wq.shape[1]
    wt[...] = jnp.transpose(wq[...].reshape(place.dp * share, 3 * wide))
    bias = jnp.transpose(vectors[8:16])

    chunk = chunk_of(slots)

    def project_block(block, _):
        cols = pl.ds(pl.multiple_of(block * chunk, 128), chunk)
        lines = pl.ds(pl.multiple_of(block * chunk, 128), chunk)
        tokens = dot(wt[...], nr[lines, :], ((1,), (1,)))
        query = (tokens[:wide] + bias[:wide, 0:1]).astype(BF16)
        key = tokens[wide : 2 * wide].astype(BF16)
        value = (tokens[2 * wide :] + bias[:wide, 1:2]).astype(BF16)
        for head in range(heads):
            part = slice(head * HEAD_DIM, (head + 1) * HEAD_DIM)
            qt[head, :HEAD_DIM, cols] = query[part]
            kt[head, :, cols] = key[part]
            vt[head, :, cols] = value[part]
            kn[head, lines, :HEAD_DIM] = jnp.transpose(key[part])
            vn[head, lines, :] = jnp.transpose(value[part])
        return 0

    lax.fori_loop(0, slots // chunk, project_block, 0)
    results = [
        pltpu.make_async_copy(src, dst, local.at[7 + i])
        for i, (src, dst) in enumerate(
            [(xs, x_out), (sm, sm_out), (wq, wq_out), (nr, normed_out), (qt, qt_out), (kt, kt_out),
             (kn, k_out), (vn, v_out)]
        )
    ]
    for copy in results:
        copy.start()

    block = 256

    def attend(head):
        def one(i, _):
            cols = pl.ds(pl.multiple_of(i * block, 128), block)
            scores = dot(kn[head], qt[head, :, cols])
            top = jnp.max(scores, axis=0, keepdims=True)
            exponent = jnp.exp2((scores - top) * QSCALE)
            total = jnp.sum(exponent, axis=0, keepdims=True)
            mixed = dot(vt[head], exponent.astype(BF16)) / total
            mix[place.s, head, :, cols] = mixed.astype(BF16)
            lse_ref[head, :, cols] = top * QSCALE + jnp.log2(total)
            return 0

        lax.fori_loop(0, slots // block, one, 0)

    g_mix = [
        GatherSeq(place, 2 + head, seq_sems, mix.at[place.s, head],
                  lambda s, head=head: mix.at[s, head])
        for head in range(heads)
    ]
    for head in range(heads):
        attend(head)
        g_mix[head].start()
        if head == 0:
            g_wo.forward_all()
            for j in range(1, place.ys):
                g_cot.arrive_y(j)
        if head == 1:
            g_w1.forward_all()
            g_w2.start()
    for head in range(heads):
        for j in range(1, place.ys):
            g_mix[head].arrive_y(j)
    for head in range(heads):
        for j in range(place.ys):
            g_mix[head].arrive_core(j)
    mix_copy = pltpu.make_async_copy(mix, mix_out, local.at[15])
    mix_copy.start()
    g_w2.forward_all()
    for j in range(place.ys):
        g_cot.arrive_core(j)
    for group in (g_wo, g_w1, g_w2):
        group.arrive()
    for group in (g_sm, g_wq, g_wo, g_w1, g_w2, g_x, g_cot, *g_mix):
        group.drain()
    for copy in (*own_blocks, *results, mix_copy):
        copy.wait()


def front(place, length, x, cot, small, wqkv, wo, w1, w2):
    dp, seq = place.dp, place.seq
    rows = x.shape[0]
    slots = rows * seq
    heads = HEADS // seq
    share, width = wqkv.shape
    anyspace = pl.BlockSpec(memory_space=pl.ANY)
    shapes = [
        (seq, rows, D),
        (seq, rows, D),
        (dp, *small.shape),
        (dp, share, width),
        (dp, *wo.shape),
        (dp, *w1.shape),
        (dp, *w2.shape),
        (slots, D),
        (heads, 128, slots),
        (heads, HEAD_DIM, slots),
        (heads, slots, 128),
        (heads, slots, HEAD_DIM),
        (seq, heads, HEAD_DIM, slots),
    ]
    vm = lambda *shape: pltpu.VMEM(shape, BF16)
    return pl.pallas_call(
        functools.partial(front_kernel, place),
        in_specs=[pl.BlockSpec(memory_space=pltpu.SMEM)] + [anyspace] * 7,
        out_specs=[anyspace] * len(shapes) + [pl.BlockSpec(memory_space=pltpu.VMEM)],
        out_shape=[jax.ShapeDtypeStruct(shape, BF16) for shape in shapes]
        + [jax.ShapeDtypeStruct((heads, 1, slots), F32)],
        scratch_shapes=[
            vm(seq, rows, D),
            vm(slots, D),
            vm(dp, *small.shape),
            vm(dp, share, width),
            vm(width, D),
            vm(heads, 128, slots),
            vm(heads, HEAD_DIM, slots),
            vm(heads, HEAD_DIM, slots),
            vm(heads, slots, 128),
            vm(heads, slots, HEAD_DIM),
            vm(seq, heads, HEAD_DIM, slots),
        ]
        + dp_semaphores(place, 5)
        + seq_semaphores(place, 2 + heads)
        + [pltpu.SemaphoreType.DMA((16,))],
        compiler_params=params(collective_id=0, has_side_effects=True),
        name="front",
    )(length, x, cot, small, wqkv, wo, w1, w2)


def attend_back_kernel(
    qt_ref, kt_ref, k_ref, v_ref, got_ref, mix_ref, lse_ref,
    dqt_ref, dk_ref, dv_ref, dk_sum, dv_sum,
):
    step = pl.program_id(1)

    @pl.when(step == 0)
    def _():
        dk_sum[...] = jnp.zeros_like(dk_sum)
        dv_sum[...] = jnp.zeros_like(dv_sum)

    grad = got_ref[0]
    delta = jnp.sum(grad.astype(F32) * mix_ref[0].astype(F32), axis=0, keepdims=True)
    probs = jnp.exp2(dot(k_ref[0], qt_ref[0]) * QSCALE - lse_ref[0])
    grad_probs = dot(v_ref[0], grad)
    grad_scores = (probs * (grad_probs - delta)).astype(BF16)
    dv_sum[...] += dot(probs.astype(BF16), grad, ((1,), (1,)))
    dk_sum[...] += dot(grad_scores, qt_ref[0, :HEAD_DIM], ((1,), (1,)))
    dqt_ref[0] = (dot(kt_ref[0], grad_scores) * SCALE).astype(BF16)

    @pl.when(step == pl.num_programs(1) - 1)
    def _():
        dk_ref[0] = (dk_sum[...] * SCALE).astype(BF16)
        dv_ref[0] = dv_sum[...].astype(BF16)


def attend_back(qt, kt, k, v, grad_mix, mix, lse):
    heads, _, slots = qt.shape
    block = 256
    turned = jax.ShapeDtypeStruct((heads, HEAD_DIM, slots), BF16)
    part = jax.ShapeDtypeStruct((heads, slots, HEAD_DIM), BF16)
    cols = pl.BlockSpec((1, HEAD_DIM, block), lambda h, i: (h, 0, i))
    rows = pl.BlockSpec((1, slots, HEAD_DIM), lambda h, i: (h, 0, 0))
    return pl.pallas_call(
        attend_back_kernel,
        grid=(heads, slots // block),
        in_specs=[
            pl.BlockSpec((1, 128, block), lambda h, i: (h, 0, i)),
            pl.BlockSpec((1, HEAD_DIM, slots), lambda h, i: (h, 0, 0)),
            pl.BlockSpec((1, slots, 128), lambda h, i: (h, 0, 0)),
            rows,
            cols,
            cols,
            pl.BlockSpec((1, 1, block), lambda h, i: (h, 0, i)),
        ],
        out_specs=[cols, rows, rows],
        scratch_shapes=[pltpu.VMEM((slots, HEAD_DIM), F32), pltpu.VMEM((slots, HEAD_DIM), F32)],
        out_shape=[turned, part, part],
        compiler_params=params(),
        name="attend_back",
    )(qt, kt, k, v, grad_mix, mix, lse)


def feed_kernel(
    place_ref, x_ref, mix_ref, cot_ref, wo_ref, w1_ref, w2_ref, bo_ref, gain_ref, shift_ref, b1_ref,
    out_ref, ds_ref, second_ref, act_ref, de_ref, middle_ref, gain_sum, shift_sum, b1_sum,
):
    step = pl.program_id(0)
    count = pl.num_programs(0)
    block = x_ref.shape[0]
    owner = lax.rem(place_ref[0] + 1 + step, count)

    @pl.when(step == 0)
    def _():
        gain_sum[...] = jnp.zeros_like(gain_sum)
        shift_sum[...] = jnp.zeros_like(shift_sum)
        b1_sum[...] = jnp.zeros_like(b1_sum)

    middle = x_ref[...].astype(F32) + (dot(mix_ref[...], wo_ref[...], ((0,), (0,))) + bo_ref[...])
    middle_ref[...] = middle
    unit, _ = normalize(middle)
    second = (unit * gain_ref[...] + shift_ref[...]).astype(BF16)
    second_ref[...] = second
    valid = owner * block + lax.broadcasted_iota(jnp.int32, (block, 1), 0) < place_ref[1]
    grad_two = jnp.where(valid, cot_ref[...].astype(F32), 0.0).astype(BF16)
    expanded = dot(second, w1_ref[...]) + b1_ref[...]
    phi = 0.5 * (1.0 + lax.erf(expanded * (0.5**0.5)))
    activated = (expanded * phi).astype(BF16)
    act_ref[...] = activated
    slope = phi + expanded * (jnp.exp(-0.5 * expanded * expanded) * 0.3989422804014327)
    out_ref[...] = dot(activated, w2_ref[...]).astype(BF16)
    grad_act = dot(grad_two, w2_ref[...], ((1,), (1,)))
    grad_expanded = (grad_act * slope).astype(BF16)
    de_ref[...] = grad_expanded
    b1_sum[...] += jnp.sum(grad_expanded.astype(F32), axis=0, keepdims=True)
    grad_second = dot(grad_expanded, w1_ref[...], ((1,), (1,)))
    ds_ref[...] = grad_second.astype(BF16)
    gain_sum[...] += jnp.sum(grad_second * unit, axis=0, keepdims=True)
    shift_sum[...] += jnp.sum(grad_second, axis=0, keepdims=True)


def feed(place, x, mix, cot, wo, w1, w2, bo, gain, shift, b1):
    slots = x.shape[0]
    block = chunk_of(slots)
    count = slots // block
    width = w1.shape[1]

    def turn(i, place):
        return lax.rem(place[0] + 1 + i, count)

    rows = pl.BlockSpec((block, D), lambda i, p: (turn(i, p), 0))
    wide = pl.BlockSpec((block, width), lambda i, p: (turn(i, p), 0))
    return pl.pallas_call(
        feed_kernel,
        grid_spec=pltpu.PrefetchScalarGridSpec(
            num_scalar_prefetch=1,
            grid=(count,),
            in_specs=[
                rows,
                pl.BlockSpec((D, block), lambda i, p: (0, turn(i, p))),
                rows,
                whole(wo.shape), whole(w1.shape), whole(w2.shape)]
            + [whole((1, D))] * 3
            + [whole((1, width))],
            out_specs=[
                rows,
                rows,
                rows,
                wide,
                wide,
                pl.BlockSpec((block, D), lambda i, p: (0, 0)),
                pl.BlockSpec((1, D), lambda i, p: (0, 0)),
                pl.BlockSpec((1, D), lambda i, p: (0, 0)),
                pl.BlockSpec((1, width), lambda i, p: (0, 0)),
            ],
        ),
        out_shape=[
            jax.ShapeDtypeStruct((slots, D), BF16),
            jax.ShapeDtypeStruct((slots, D), BF16),
            jax.ShapeDtypeStruct((slots, D), BF16),
            jax.ShapeDtypeStruct((slots, width), BF16),
            jax.ShapeDtypeStruct((slots, width), BF16),
            jax.ShapeDtypeStruct((block, D), F32),
            jax.ShapeDtypeStruct((1, D), F32),
            jax.ShapeDtypeStruct((1, D), F32),
            jax.ShapeDtypeStruct((1, width), F32),
        ],
        compiler_params=params(),
        name="feed",
    )(place, x, mix, cot, wo, w1, w2, bo, gain, shift, b1)


def gather(value, axes, axis=0):
    return lax.all_gather(value, axes, axis=axis, tiled=True)


def scatter_sum(value, axes, axis=0):
    return lax.psum_scatter(value, axes, scatter_dimension=axis, tiled=True)


def per_device(
    hidden_in, cotangent, clip_lengths, clip_order, first_gain, first_shift, query_weight,
    query_bias, key_weight, value_weight, value_bias, output_weight, output_bias, second_gain,
    second_shift, expand_weight, expand_bias, reduce_weight, reduce_bias,
):
    dp = lax.axis_size("dp")
    seq = lax.axis_size("seq")
    me = lax.axis_index("seq")
    rows_here = hidden_in.shape[1]
    slots = rows_here * seq
    share = D // dp
    head_cols = D // seq
    heads = HEADS // seq
    units = FF // (dp * seq)
    quarter = dp * units

    hidden_own = hidden_in[0]
    matches = clip_order[0] == jnp.arange(clip_lengths.shape[0], dtype=jnp.int32)
    length = jnp.sum(jnp.where(matches, clip_lengths, 0)).reshape(1)

    spot = Place(dp, seq)
    mine_dp = lax.axis_index("dp")

    def columns(weight):
        return lax.dynamic_slice_in_dim(weight, me * head_cols, head_cols, 1)

    width = 3 * head_cols
    extra = -(-(8 * share + FF // dp) // width)
    tall = -(-(share + extra) // 16) * 16

    def spread(vector):
        return lax.dynamic_update_slice_in_dim(jnp.zeros((D,), BF16), vector, mine_dp * share, 0)

    def head_part(vector):
        part = lax.dynamic_slice_in_dim(spread(vector), me * head_cols, head_cols, 0)
        return jnp.pad(part, (0, D - head_cols))

    expand_own = lax.dynamic_slice_in_dim(expand_bias, me * units, units, 0)
    expand_row = lax.dynamic_update_slice_in_dim(
        jnp.zeros((quarter,), BF16), expand_own, mine_dp * units, 0
    )
    blank = jnp.zeros((D,), BF16)
    small = jnp.stack(
        [spread(first_gain), spread(first_shift), spread(output_bias), spread(second_gain),
         spread(second_shift), spread(reduce_bias), jnp.pad(expand_row, (0, D - quarter)), blank,
         head_part(query_bias), head_part(value_bias)] + [blank] * 6
    )
    wqkv_share = jnp.concatenate(
        [columns(query_weight), columns(key_weight), columns(value_weight)], axis=1
    )
    w1_share = jnp.concatenate(
        [
            lax.dynamic_slice_in_dim(expand_weight, d * (FF // dp) + me * units, units, 1)
            for d in range(dp)
        ],
        axis=1,
    )
    w2_share = lax.dynamic_slice_in_dim(reduce_weight, me * units, units, 0)
    (
        x, cot, small, w_qkv, w_out, w_expand, w_reduce, normed, qt, kt, keys, values, mix, lse,
    ) = front(spot, length, hidden_own, cotangent[0], small, wqkv_share, output_weight, w1_share, w2_share)
    x, cot = (value.reshape(slots, D) for value in (x, cot))
    w_qkv = w_qkv.reshape(D, width)
    w_out = w_out.reshape(D, D)
    w_expand = w_expand.reshape(D, quarter)
    w_reduce = w_reduce.reshape(quarter, D)
    vectors = jnp.sum(small.astype(F32), axis=0)
    gain_one, shift_one, bias_out, gain_two, shift_two, bias_reduce = (
        vectors[i : i + 1] for i in range(6)
    )
    bias_expand = vectors[6:7, :quarter]
    mix_own = lax.dynamic_index_in_dim(mix, me, 0, keepdims=False)
    mix = mix.reshape(D, slots)
    joined = chunk_of(slots) // rows_here
    place = jnp.stack([me.astype(jnp.int32) // joined, length[0]])
    (
        out_part, ds_part, second, act, grad_expanded, middle_own, gain_two_grad, shift_two_grad,
        bias_expand_grad,
    ) = feed(
        place, x, mix, cot, w_out, w_expand, w_reduce, bias_out, gain_two, shift_two,
        bias_expand,
    )
    middle_own = lax.dynamic_slice_in_dim(
        middle_own, lax.rem(me.astype(jnp.int32), joined) * rows_here, rows_here, 0
    )
    positions = jnp.arange(slots, dtype=jnp.int32)
    valid = (positions < length)[:, None]
    grad_two = jnp.where(valid, cot, 0).astype(BF16)
    grad_out = lax.dynamic_slice_in_dim(grad_two, me * rows_here, rows_here, 0).astype(F32)

    layer_output = (
        middle_own + (scatter_sum(out_part, "seq").astype(F32) + bias_reduce)
    ).astype(BF16)
    grad_second = scatter_sum(ds_part, "seq").astype(F32)
    unit_two, spread_two = normalize(middle_own)
    grad_middle = grad_out + norm_backward(unit_two, spread_two, grad_second * gain_two)
    grad_branch = grad_middle.astype(BF16)
    reduce_bias_grad = jnp.sum(grad_out, axis=0)
    output_bias_grad = jnp.sum(grad_branch.astype(F32), axis=0)

    w1_grad = dot(second, grad_expanded, ((0,), (0,))).astype(BF16)
    w2_grad = dot(act, grad_two, ((0,), (0,))).astype(BF16)
    w1_grad = scatter_sum(w1_grad, "dp")
    w2_grad = scatter_sum(w2_grad, "dp")

    grad_branch_all = gather(grad_branch, "seq")
    wo_grad = dot(mix, columns(grad_branch_all)).astype(BF16)
    wo_rows = lax.dynamic_slice_in_dim(w_out, me * head_cols, head_cols, 0)
    grad_mix = dot(wo_rows, grad_branch_all, ((1,), (1,))).astype(BF16)
    dqt, dk, dv = attend_back(
        qt, kt, keys, values, grad_mix.reshape(heads, HEAD_DIM, slots), mix_own, lse
    )
    dqkv = jnp.concatenate(
        [
            dqt.reshape(head_cols, slots).T,
            jnp.concatenate([dk, dv], axis=0).transpose(1, 0, 2).reshape(slots, 2 * head_cols),
        ],
        axis=1,
    )
    qkv_grad = dot(normed, dqkv, ((0,), (0,))).astype(BF16)
    bias_qkv_grad = jnp.sum(dqkv.astype(F32), axis=0)
    grad_normed = dot(dqkv, w_qkv, ((1,), (1,)))
    unit_all, _ = normalize(x.astype(F32))
    gain_one_grad = jnp.sum(grad_normed * unit_all, axis=0)
    shift_one_grad = jnp.sum(grad_normed, axis=0)
    grad_normed_own = scatter_sum(grad_normed.astype(BF16), "seq").astype(F32)
    unit_one, spread_one = normalize(hidden_own.astype(F32))
    grad_front = grad_middle + norm_backward(unit_one, spread_one, grad_normed_own * gain_one)
    input_grad = grad_front.astype(BF16)

    def mine(value):
        return lax.dynamic_update_slice_in_dim(
            jnp.zeros((D,), F32), value.reshape(-1), me * head_cols, 0
        )

    expand_vec = lax.dynamic_update_slice_in_dim(
        jnp.zeros((dp, FF // dp), F32), bias_expand_grad.reshape(dp, units), me * units, 1
    )
    vectors = [
        gain_one_grad, shift_one_grad, mine(bias_qkv_grad[:head_cols]),
        mine(bias_qkv_grad[2 * head_cols :]), output_bias_grad, gain_two_grad.reshape(-1),
        shift_two_grad.reshape(-1), reduce_bias_grad,
    ]
    small_grad = jnp.concatenate([v.reshape(dp, share) for v in vectors] + [expand_vec], axis=1)
    small_grad = jnp.pad(
        small_grad.astype(BF16), ((0, 0), (0, (tall - share) * width - small_grad.shape[1]))
    ).reshape(dp, tall - share, width)
    packed_grad = jnp.concatenate([qkv_grad.reshape(dp, share, width), small_grad], axis=1)
    packed_grad = scatter_sum(packed_grad, "dp")[0]
    wo_grad = scatter_sum(wo_grad, "dp")

    packed_grad = gather(packed_grad[None], "seq")
    wo_grad = gather(wo_grad[None], "seq")
    w1_grad = gather(w1_grad[None], "seq")
    w2_grad = gather(w2_grad, "seq").astype(F32)
    w1_grad = (
        w1_grad.reshape(seq, share, dp, units).transpose(1, 2, 0, 3).reshape(share, FF).astype(F32)
    )
    wo_grad = wo_grad.transpose(1, 0, 2).reshape(share, D).astype(F32)
    qkv_grad = packed_grad[:, :share].reshape(seq, share, 3, head_cols).astype(F32)
    qkv_grad = qkv_grad.transpose(2, 1, 0, 3).reshape(3, share, D)
    small_grad = jnp.sum(
        packed_grad[:, share : share + extra].reshape(seq, extra * width).astype(F32), axis=0
    )
    pieces = [small_grad[i * share : (i + 1) * share] for i in range(8)]
    expand_bias_grad = small_grad[8 * share : 8 * share + FF // dp]
    return (
        layer_output[None],
        input_grad[None],
        pieces[0],
        pieces[1],
        qkv_grad[0],
        pieces[2],
        qkv_grad[1],
        qkv_grad[2],
        pieces[3],
        wo_grad,
        pieces[4],
        pieces[5],
        pieces[6],
        w1_grad,
        expand_bias_grad,
        w2_grad,
        pieces[7],
    )


def solution(mesh):
    clip = P("dp", "seq", None)
    vec = P("dp")
    mat = P("dp", None)
    return jax.shard_map(
        per_device,
        mesh=mesh,
        in_specs=(
            clip, clip, P(), vec, vec, vec, mat, vec, mat, mat, vec, mat, vec, vec, vec, mat, vec,
            mat, vec,
        ),
        out_specs=(
            clip, clip, vec, vec, mat, vec, mat, mat, vec, mat, vec, vec, vec, mat, vec, mat, vec,
        ),
        check_vma=False,
    )
```

```python
import functools

import jax
import jax.numpy as jnp
from jax import lax
from jax.experimental import pallas as pl
from jax.experimental.pallas import tpu as pltpu
from jax.sharding import PartitionSpec as P

D = 1280
FF = 5120
HEADS = 16
HEAD_DIM = D // HEADS
EPSILON = 1e-05
SCALE = HEAD_DIM ** (-0.5)
F32 = jnp.float32
BF16 = jnp.bfloat16
VMEM_LIMIT = 66_000_000
MESH = pl.DeviceIdType.MESH


def dot(left, right, contract=((1,), (0,))):
    return lax.dot_general(left, right, (contract, ((), ())), preferred_element_type=F32)


def normalize(values):
    average = jnp.mean(values, axis=-1, keepdims=True)
    centered = values - average
    variance = jnp.mean(centered * centered, axis=-1, keepdims=True)
    spread = lax.rsqrt(variance + EPSILON)
    return centered * spread, spread


def norm_backward(unit, spread, grad_unit):
    inner = jnp.mean(grad_unit * unit, axis=-1, keepdims=True)
    return spread * (grad_unit - jnp.mean(grad_unit, axis=-1, keepdims=True) - unit * inner)


def params(**extra):
    return pltpu.CompilerParams(vmem_limit_bytes=VMEM_LIMIT, **extra)


def whole(shape):
    return pl.BlockSpec(shape, lambda *_: (0,) * len(shape), pipeline_mode=pl.Buffered(1))


def chunk_of(slots):
    return slots // 4 if slots % 512 == 0 else slots


class Place:
    def __init__(self, dp, seq):
        self.dp, self.seq = dp, seq
        self.xs = 1 << ((dp.bit_length() - 1) // 2)
        self.zs = dp // self.xs
        self.ys = seq // 2

    def locate(self):
        self.d, self.s = lax.axis_index("dp"), lax.axis_index("seq")
        self.z, self.x = self.d // self.xs, lax.rem(self.d, self.xs)
        self.y, self.c = self.s // 2, lax.rem(self.s, 2)
        self.partner = self.y * 2 + 1 - self.c

    def at_z(self, k):
        return lax.rem(self.z + k + self.zs, self.zs) * self.xs + self.x

    def block(self, k, j):
        return lax.rem(self.z - k + self.zs, self.zs) * self.xs + lax.rem(
            self.x - j + self.xs, self.xs
        )

    def at_x(self, j):
        return self.z * self.xs + lax.rem(self.x + j, self.xs)

    def at_y(self, j, core):
        return lax.rem(self.y + j + self.ys, self.ys) * 2 + core

    def peers(self, over_dp=True, over_seq=True):
        found = []
        if over_dp:
            found += [(self.at_z(k), self.s) for k in range(1, self.zs)]
            found += [(self.at_x(j), self.s) for j in range(1, self.xs)]
        if over_seq:
            found += [(self.d, self.partner)]
            found += [(self.d, self.at_y(j, self.c)) for j in range(1, self.ys)]
        return found

    def barrier(self, **which):
        semaphore = pltpu.get_barrier_semaphore()
        peers = self.peers(**which)
        for peer in peers:
            pl.semaphore_signal(semaphore, inc=1, device_id=peer, device_id_type=MESH)
        pl.semaphore_wait(semaphore, len(peers))


def send(src, dst, send_sem, recv_sem, device):
    return pltpu.make_async_remote_copy(
        src_ref=src, dst_ref=dst, send_sem=send_sem, recv_sem=recv_sem, device_id=device,
        device_id_type=MESH,
    )


def dp_semaphores(place, groups):
    return [
        pltpu.SemaphoreType.DMA((groups, place.zs)),
        pltpu.SemaphoreType.DMA((groups, place.zs)),
        pltpu.SemaphoreType.DMA((groups, place.zs, place.xs)),
        pltpu.SemaphoreType.DMA((groups, place.zs, place.xs)),
    ]


def seq_semaphores(place, groups):
    return [pltpu.SemaphoreType.DMA((groups, 2, place.ys))] * 2


class GatherDp:
    def __init__(self, place, group, sems, own, slab):
        self.p, self.g, self.own, self.slab = place, group, own, slab
        self.zsend, self.zrecv, self.xsend, self.xrecv = sems

    def z_copy(self, k):
        src = self.own
        return send(src, self.slab(self.p.d), self.zsend.at[self.g, k], self.zrecv.at[self.g, k],
                    (self.p.at_z(k), self.p.s))

    def x_copy(self, k, j):
        block = self.p.block(k, 0)
        src = self.own if k == 0 else self.slab(block)
        return send(src, self.slab(block), self.xsend.at[self.g, k, j],
                    self.xrecv.at[self.g, k, j], (self.p.at_x(j), self.p.s))

    def start(self):
        for j in range(1, self.p.xs):
            self.x_copy(0, j).start()
        for k in range(self.p.zs - 1, 0, -1):
            self.z_copy(k).start()

    def forward(self, k):
        place = self.p
        send(self.own, self.slab(place.block(k, 0)), self.zsend.at[self.g, k],
             self.zrecv.at[self.g, k], (place.at_z(k), place.s)).wait_recv()
        for j in range(1, place.xs):
            self.x_copy(k, j).start()

    def forward_all(self):
        for k in range(1, self.p.zs):
            self.forward(k)

    def arrive(self):
        place = self.p
        for k in range(place.zs):
            for j in range(1, place.xs):
                send(self.own, self.slab(place.block(k, j)), self.xsend.at[self.g, k, j],
                     self.xrecv.at[self.g, k, j], (place.at_x(j), place.s)).wait_recv()

    def drain(self):
        place = self.p
        for k in range(1, place.zs):
            self.z_copy(k).wait_send()
        for k in range(place.zs):
            for j in range(1, place.xs):
                self.x_copy(k, j).wait_send()


class GatherSeq:
    def __init__(self, place, group, sems, own, slab):
        self.p, self.g, self.own, self.slab = place, group, own, slab
        self.sends, self.recvs = sems

    def y_copy(self, j):
        place = self.p
        return send(self.own, self.slab(place.s), self.sends.at[self.g, 0, j],
                    self.recvs.at[self.g, 0, j], (place.d, place.at_y(j, place.c)))

    def core_copy(self, j):
        place = self.p
        block = place.at_y(-j, place.c)
        src = self.own if j == 0 else self.slab(block)
        return send(src, self.slab(block), self.sends.at[self.g, 1, j],
                    self.recvs.at[self.g, 1, j], (place.d, place.partner))

    def start(self):
        for j in range(1, self.p.ys):
            self.y_copy(j).start()
        self.core_copy(0).start()

    def arrive_y(self, j):
        place = self.p
        block = place.at_y(-j, place.c)
        send(self.own, self.slab(block), self.sends.at[self.g, 0, j], self.recvs.at[self.g, 0, j],
             (place.d, place.at_y(j, place.c))).wait_recv()
        self.core_copy(j).start()
        return block

    def arrive_core(self, j):
        place = self.p
        block = place.at_y(-j, 1 - place.c)
        send(self.own, self.slab(block), self.sends.at[self.g, 1, j], self.recvs.at[self.g, 1, j],
             (place.d, place.partner)).wait_recv()
        return block

    def drain(self):
        for j in range(1, self.p.ys):
            self.y_copy(j).wait_send()
        for j in range(self.p.ys):
            self.core_copy(j).wait_send()


LOG2E = 1.4426950408889634
QSCALE = SCALE * LOG2E


def front_kernel(
    place, length_ref, x_in, cot_in, sm_in, wq_in, wo_in, w1_in,
    x_out, cot_out, sm_out, wq_out, wo_out, w1_out, normed_out, qt_out, kt_out, k_out,
    v_out, mix_out, lse_ref,
    xs, nr, sm, wq, wt, qt, kt, vt, kn, vn, mix,
    zsend, zrecv, xsend, xrecv, ssend, srecv, local,
):
    place.locate()
    seq, rows = x_out.shape[0], x_out.shape[1]
    slots = seq * rows
    heads = k_out.shape[0]
    wide = heads * HEAD_DIM
    place.barrier()
    dp_sems = (zsend, zrecv, xsend, xrecv)
    seq_sems = (ssend, srecv)

    def over_dp(group, own, buffer):
        return GatherDp(place, group, dp_sems, own, lambda d: buffer.at[d])

    def over_seq(group, own, buffer):
        return GatherSeq(place, group, seq_sems, own, lambda s: buffer.at[s])

    g_sm = over_dp(0, sm_in, sm)
    g_wq = over_dp(1, wq_in, wq)
    g_wo = over_dp(2, wo_in, wo_out)
    g_w1 = over_dp(3, w1_in, w1_out)
    g_x = over_seq(0, x_in, xs)
    g_cot = over_seq(1, cot_in, cot_out)

    locals_in = [
        pltpu.make_async_copy(x_in, xs.at[place.s], local.at[0]),
        pltpu.make_async_copy(sm_in, sm.at[place.d], local.at[1]),
        pltpu.make_async_copy(wq_in, wq.at[place.d], local.at[2]),
    ]
    own_blocks = [
        pltpu.make_async_copy(cot_in, cot_out.at[place.s], local.at[3]),
        pltpu.make_async_copy(wo_in, wo_out.at[place.d], local.at[4]),
        pltpu.make_async_copy(w1_in, w1_out.at[place.d], local.at[5]),
    ]
    for copy in locals_in:
        copy.start()
    g_sm.start()
    g_x.start()
    g_wq.start()
    for copy in own_blocks:
        copy.start()

    column = lax.broadcasted_iota(jnp.int32, (slots, 1), 0)
    penalty = jnp.where(column >= length_ref[0], -1e30, 0.0).astype(BF16)
    ones_row = jnp.where(
        lax.broadcasted_iota(jnp.int32, (128 - HEAD_DIM, slots), 0) == 0, 1.0, 0.0
    ).astype(BF16)
    for head in range(heads):
        kn[head] = jnp.zeros((slots, 128), BF16)
        kn[head, :, HEAD_DIM : HEAD_DIM + 1] = penalty
        qt[head, HEAD_DIM:, :] = ones_row

    for copy in locals_in:
        copy.wait()
    g_sm.forward_all()
    g_wq.forward_all()
    g_wo.start()
    g_w1.start()
    g_cot.start()
    g_sm.arrive()
    vectors = jnp.sum(sm[...].astype(F32), axis=0)
    gain, shift = vectors[0:1], vectors[1:2]

    def norm_block(block):
        unit, _ = normalize(xs[block].astype(F32))
        lines = pl.ds(pl.multiple_of(block * rows, 16), rows)
        nr[lines, :] = (unit * gain + shift).astype(BF16)

    norm_block(place.s)
    norm_block(g_x.arrive_core(0))
    for j in range(1, place.ys):
        norm_block(g_x.arrive_y(j))
        norm_block(g_x.arrive_core(j))
    g_wq.arrive()
    share = wq.shape[1]
    wt[...] = jnp.transpose(wq[...].reshape(place.dp * share, 3 * wide))
    bias = jnp.transpose(vectors[8:16])

    chunk = chunk_of(slots)

    def project_block(block, _):
        cols = pl.ds(pl.multiple_of(block * chunk, 128), chunk)
        lines = pl.ds(pl.multiple_of(block * chunk, 128), chunk)
        tokens = dot(wt[...], nr[lines, :], ((1,), (1,)))
        query = (tokens[:wide] + bias[:wide, 0:1]).astype(BF16)
        key = tokens[wide : 2 * wide].astype(BF16)
        value = (tokens[2 * wide :] + bias[:wide, 1:2]).astype(BF16)
        for head in range(heads):
            part = slice(head * HEAD_DIM, (head + 1) * HEAD_DIM)
            qt[head, :HEAD_DIM, cols] = query[part]
            kt[head, :, cols] = key[part]
            vt[head, :, cols] = value[part]
            kn[head, lines, :HEAD_DIM] = jnp.transpose(key[part])
            vn[head, lines, :] = jnp.transpose(value[part])
        return 0

    lax.fori_loop(0, slots // chunk, project_block, 0)
    results = [
        pltpu.make_async_copy(src, dst, local.at[7 + i])
        for i, (src, dst) in enumerate(
            [(xs, x_out), (sm, sm_out), (wq, wq_out), (nr, normed_out), (qt, qt_out), (kt, kt_out),
             (kn, k_out), (vn, v_out)]
        )
    ]
    for copy in results:
        copy.start()

    block = 256

    def attend(head):
        def one(i, _):
            cols = pl.ds(pl.multiple_of(i * block, 128), block)
            scores = dot(kn[head], qt[head, :, cols])
            top = jnp.max(scores, axis=0, keepdims=True)
            exponent = jnp.exp2((scores - top) * QSCALE)
            total = jnp.sum(exponent, axis=0, keepdims=True)
            mixed = dot(vt[head], exponent.astype(BF16)) / total
            mix[place.s, head, :, cols] = mixed.astype(BF16)
            lse_ref[head, :, cols] = top * QSCALE + jnp.log2(total)
            return 0

        lax.fori_loop(0, slots // block, one, 0)

    g_mix = [
        GatherSeq(place, 2 + head, seq_sems, mix.at[place.s, head],
                  lambda s, head=head: mix.at[s, head])
        for head in range(heads)
    ]
    for head in range(heads):
        attend(head)
        g_mix[head].start()
        if head == 0:
            g_wo.forward_all()
            for j in range(1, place.ys):
                g_cot.arrive_y(j)
        if head == 1:
            g_w1.forward_all()
    for head in range(heads):
        for j in range(1, place.ys):
            g_mix[head].arrive_y(j)
    for head in range(heads):
        for j in range(place.ys):
            g_mix[head].arrive_core(j)
    mix_copy = pltpu.make_async_copy(mix, mix_out, local.at[15])
    mix_copy.start()
    for j in range(place.ys):
        g_cot.arrive_core(j)
    for group in (g_wo, g_w1):
        group.arrive()
    for group in (g_sm, g_wq, g_wo, g_w1, g_x, g_cot, *g_mix):
        group.drain()
    for copy in (*own_blocks, *results, mix_copy):
        copy.wait()


def front(place, length, x, cot, small, wqkv, wo, w1):
    dp, seq = place.dp, place.seq
    rows = x.shape[0]
    slots = rows * seq
    heads = HEADS // seq
    share, width = wqkv.shape
    anyspace = pl.BlockSpec(memory_space=pl.ANY)
    shapes = [
        (seq, rows, D),
        (seq, rows, D),
        (dp, *small.shape),
        (dp, share, width),
        (dp, *wo.shape),
        (dp, *w1.shape),
        (slots, D),
        (heads, 128, slots),
        (heads, HEAD_DIM, slots),
        (heads, slots, 128),
        (heads, slots, HEAD_DIM),
        (seq, heads, HEAD_DIM, slots),
    ]
    vm = lambda *shape: pltpu.VMEM(shape, BF16)
    return pl.pallas_call(
        functools.partial(front_kernel, place),
        in_specs=[pl.BlockSpec(memory_space=pltpu.SMEM)] + [anyspace] * 6,
        out_specs=[anyspace] * len(shapes) + [pl.BlockSpec(memory_space=pltpu.VMEM)],
        out_shape=[jax.ShapeDtypeStruct(shape, BF16) for shape in shapes]
        + [jax.ShapeDtypeStruct((heads, 1, slots), F32)],
        scratch_shapes=[
            vm(seq, rows, D),
            vm(slots, D),
            vm(dp, *small.shape),
            vm(dp, share, width),
            vm(width, D),
            vm(heads, 128, slots),
            vm(heads, HEAD_DIM, slots),
            vm(heads, HEAD_DIM, slots),
            vm(heads, slots, 128),
            vm(heads, slots, HEAD_DIM),
            vm(seq, heads, HEAD_DIM, slots),
        ]
        + dp_semaphores(place, 4)
        + seq_semaphores(place, 2 + heads)
        + [pltpu.SemaphoreType.DMA((16,))],
        compiler_params=params(collective_id=0, has_side_effects=True),
        name="front",
    )(length, x, cot, small, wqkv, wo, w1)


class ScatterSeq:
    def __init__(self, place, group, sems, part, from_core, from_y):
        self.p, self.g, self.part, self.from_core, self.from_y = place, group, part, from_core, from_y
        self.sends, self.recvs = sems

    def core_copy(self, j):
        place = self.p
        return send(self.part(place.at_y(j, 1 - place.c)), self.from_core(j),
                    self.sends.at[self.g, 1, j], self.recvs.at[self.g, 1, j],
                    (place.d, place.partner))

    def y_copy(self, j, src):
        place = self.p
        return send(src, self.from_y(j), self.sends.at[self.g, 0, j], self.recvs.at[self.g, 0, j],
                    (place.d, place.at_y(j, place.c)))


class ScatterDp:
    def __init__(self, place, group, sems, part, from_x, total, from_z):
        self.p, self.g = place, group
        self.part, self.from_x, self.total, self.from_z = part, from_x, total, from_z
        self.zsend, self.zrecv, self.xsend, self.xrecv = sems

    def x_copy(self, j, zi):
        place = self.p
        target = lax.rem(place.x + j, place.xs)
        return send(self.part(zi * place.xs + target), self.from_x(j, zi),
                    self.xsend.at[self.g, zi, j], self.xrecv.at[self.g, zi, j],
                    (place.at_x(j), place.s))

    def start_x(self):
        for zi in range(self.p.zs):
            for j in range(1, self.p.xs):
                self.x_copy(j, zi).start()

    def fold(self, zi):
        place = self.p
        value = self.part(zi * place.xs + place.x)[...].astype(F32)
        for j in range(1, place.xs):
            self.x_copy(j, zi).wait_recv()
            value = value + self.from_x(j, zi)[...].astype(F32)
        self.total(zi)[...] = value.astype(BF16)

    def fold_all(self):
        for zi in range(self.p.zs):
            self.fold(zi)

    def z_copy(self, k):
        place = self.p
        return send(self.total(lax.rem(place.z + k, place.zs)), self.from_z(k),
                    self.zsend.at[self.g, k], self.zrecv.at[self.g, k], (place.at_z(k), place.s))

    def start_z(self):
        for k in range(self.p.zs - 1, 0, -1):
            self.z_copy(k).start()

    def finish(self, own):
        value = own[...].astype(F32)
        for k in range(1, self.p.zs):
            self.z_copy(k).wait_recv()
            value = value + self.from_z(k)[...].astype(F32)
        return value

    def drain_x(self):
        for zi in range(self.p.zs):
            for j in range(1, self.p.xs):
                self.x_copy(j, zi).wait_send()

    def drain_z(self):
        for k in range(1, self.p.zs):
            self.z_copy(k).wait_send()


def whole_tiles(*heights):
    return all(height % 16 == 0 for height in heights)


def feed_kernel(
    place, length_ref, x_in, mix_in, cot_in, wo_in, w1_in, w2_in, vec_ref,
    gb_out, middle_out, grad_out, part_out, s1_out, s2_out, sums_ref,
    xa, mixv, gv, wo, w1, w2, second, act, slope, unit, ds, own, from_core, from_y,
    from_x1, from_x2, *rest,
):
    zsend, zrecv, xsend, xrecv, ssend, srecv, local = rest[-7:]
    gb = xa
    place.locate()
    seq, rows, _ = x_in.shape
    slots = seq * rows
    chunk = chunk_of(slots)
    joined = chunk // rows
    width = w1.shape[1]
    share = D // place.dp
    units = width // place.dp
    place.barrier()
    dp_sems = (zsend, zrecv, xsend, xrecv)
    seq_sems = (ssend, srecv)
    if whole_tiles(share, units):
        w1_part = lambda d: w1.at[pl.ds(pl.multiple_of(d * share, 16), share), :]
        w2_part = lambda d: w2.at[pl.ds(pl.multiple_of(d * units, 16), units), :]
        total1 = lambda zi: wo.at[pl.ds(zi * share, share), pl.ds(0, width)]
        total2 = lambda zi: wo.at[pl.ds(place.zs * share + zi * units, units), :]
    else:
        w1_split, w2_split, total1_split, total2_split = rest[:4]
        w1_part, w2_part = (lambda d: w1_split.at[d]), (lambda d: w2_split.at[d])
        total1, total2 = (lambda zi: total1_split.at[zi]), (lambda zi: total2_split.at[zi])
    gather = GatherDp(place, 0, dp_sems, w2_in, w2_part)
    gather.start()
    loads = [
        pltpu.make_async_copy(src, dst, local.at[i])
        for i, (src, dst) in enumerate(
            [(mix_in, mixv), (wo_in, wo), (w1_in, w1), (cot_in, gv), (x_in, xa)]
        )
    ]
    w2_own = pltpu.make_async_copy(w2_in, w2_part(place.d), local.at[5])
    for copy in (*loads, w2_own):
        copy.start()
    gain, shift, bias_out, bias1 = vec_ref[3:4], vec_ref[4:5], vec_ref[2:3], vec_ref[6:7, :width]
    own_chunk = place.s // joined
    sums_ref[...] = jnp.zeros_like(sums_ref)
    for copy in loads:
        copy.wait()

    def lines_of(index, size, step=16):
        return pl.ds(pl.multiple_of(index * size, step), size)

    def forward(i, _):
        lines = lines_of(i, chunk)
        hidden = xa[pl.ds(i * joined, joined)].reshape(chunk, D).astype(F32)
        cols = pl.ds(pl.multiple_of(i * chunk, 128), chunk)
        middle = hidden + (dot(mixv[:, cols], wo[...], ((0,), (0,))) + bias_out)

        @pl.when(i == own_chunk)
        def _():
            own[...] = middle

        normal, _ = normalize(middle)
        unit[lines, :] = normal.astype(BF16)
        tokens = (normal * gain + shift).astype(BF16)
        second[lines, :] = tokens
        expanded = dot(tokens, w1[...]) + bias1
        phi = 0.5 * (1.0 + lax.erf(expanded * (0.5**0.5)))
        act[lines, :] = (expanded * phi).astype(BF16)
        density = jnp.exp(-0.5 * expanded * expanded) * 0.3989422804014327
        slope[lines, :] = (phi + expanded * density).astype(BF16)
        valid = (
            i * chunk + lax.broadcasted_iota(jnp.int32, (chunk, 1), 0) < length_ref[0]
        )
        cot = gv[pl.ds(i * joined, joined)].reshape(chunk, D)
        gv[pl.ds(i * joined, joined)] = jnp.where(valid, cot.astype(F32), 0.0).astype(BF16).reshape(
            joined, rows, D
        )
        return 0

    lax.fori_loop(0, slots // chunk, forward, 0)
    gather.forward_all()
    w2_own.wait()
    gather.arrive()
    if not whole_tiles(share, units):
        for d in range(place.dp):
            w2[d * units : (d + 1) * units, :] = w2_split[d]

    scatter = ScatterSeq(place, 0, seq_sems, lambda s: ds.at[s], lambda j: from_core.at[j],
                         lambda j: from_y.at[j - 1])
    def backward(i):
        lines = lines_of(i, chunk)
        grad_two = gv[pl.ds(i * joined, joined)].reshape(chunk, D)
        grad_act = dot(grad_two, w2[...], ((1,), (1,)))
        grad_expanded = (grad_act * slope[lines, :].astype(F32)).astype(BF16)
        slope[lines, :] = grad_expanded
        grad_second = dot(grad_expanded, w1[...], ((1,), (1,)))
        ds[pl.ds(i * joined, joined)] = grad_second.astype(BF16).reshape(joined, rows, D)
        sums_ref[3:4] += jnp.sum(grad_second * unit[lines, :].astype(F32), axis=0, keepdims=True)
        sums_ref[4:5] += jnp.sum(grad_second, axis=0, keepdims=True)
        sums_ref[7:8, :width] += jnp.sum(grad_expanded.astype(F32), axis=0, keepdims=True)

    def fold_y(j):
        block = place.at_y(j, place.c)
        scatter.core_copy(j).wait_recv()
        ds[block] = (ds[block].astype(F32) + from_core[j].astype(F32)).astype(BF16)
        scatter.y_copy(j, ds.at[block]).start()

    for j in list(range(1, place.ys)) + [0]:
        if joined == 1:
            backward(place.at_y(j, 1 - place.c))
            scatter.core_copy(j).start()
            backward(place.at_y(j, place.c))
        else:
            backward(lax.rem(place.y + j, place.ys))
            scatter.core_copy(j).start()
        if j:
            fold_y(j)

    gather.drain()

    def emit(i, _):
        lines = lines_of(i, chunk)
        unit[lines, :] = dot(act[lines, :], w2[...]).astype(BF16)
        return 0

    lax.fori_loop(0, slots // chunk, emit, 0)
    keep_parts = [
        pltpu.make_async_copy(
            unit.at[pl.ds(i * rows, rows), :], part_out.at[i], local.at[9 + i]
        )
        for i in range(seq)
    ]
    for copy in keep_parts:
        copy.start()

    step = 256 if width % 256 == 0 else 128

    def w2_grad(i, _):
        cols = pl.ds(pl.multiple_of(i * step, 128), step)
        value = dot(act[:, cols], gv[...].reshape(slots, D), ((0,), (0,)))
        w2[pl.ds(pl.multiple_of(i * step, 128), step), :] = value.astype(BF16)
        return 0

    def w1_grad(i, _):
        cols = pl.ds(pl.multiple_of(i * 256, 128), 256)
        value = dot(second[:, cols], slope[...], ((0,), (0,)))
        w1[pl.ds(pl.multiple_of(i * 256, 128), 256), :] = value.astype(BF16)
        return 0

    lax.fori_loop(0, width // step, w2_grad, 0)
    if not whole_tiles(share, units):
        for d in range(place.dp):
            w2_split[d] = w2[d * units : (d + 1) * units, :]
    r2 = ScatterDp(place, 1, dp_sems, w2_part, lambda j, zi: from_x2.at[j - 1, zi], total2, None)
    r1 = ScatterDp(place, 2, dp_sems, w1_part, lambda j, zi: from_x1.at[j - 1, zi], total1, None)
    r2.start_x()

    scatter.core_copy(0).wait_recv()
    value = ds[place.s].astype(F32) + from_core[0].astype(F32)
    for j in range(1, place.ys):
        scatter.y_copy(j, ds.at[place.s]).wait_recv()
        value = value + from_y[j - 1].astype(F32)
    mine = pl.ds(pl.multiple_of(lax.rem(place.s, joined) * rows, 8), rows)
    middle = own[mine, :]
    normal, spread = normalize(middle)
    grad_two = gv[place.s].astype(F32)
    grad_middle = grad_two + norm_backward(normal, spread, value * gain)
    branch = grad_middle.astype(BF16)
    gb[place.s] = branch
    sums_ref[5:6] = jnp.sum(grad_two, axis=0, keepdims=True)
    sums_ref[2:3] = jnp.sum(branch.astype(F32), axis=0, keepdims=True)
    spread_out = GatherSeq(place, 1, seq_sems, gb.at[place.s], lambda s: gb.at[s])
    spread_out.start()
    middle_out[...] = middle
    grad_out[...] = grad_middle

    lax.fori_loop(0, D // 256, w1_grad, 0)
    if not whole_tiles(share, units):
        for d in range(place.dp):
            w1_split[d] = w1[d * share : (d + 1) * share, :]
    r1.start_x()
    r2.fold_all()
    keep = [
        pltpu.make_async_copy(total2(zi), s2_out.at[zi], local.at[9 + seq + zi])
        for zi in range(place.zs)
    ] + [
        pltpu.make_async_copy(total1(zi), s1_out.at[zi], local.at[9 + seq + place.zs + zi])
        for zi in range(place.zs)
    ]
    for copy in keep[: place.zs]:
        copy.start()
    for j in range(1, place.ys):
        spread_out.arrive_y(j)
    r1.fold_all()
    for copy in keep[place.zs :]:
        copy.start()
    for j in range(place.ys):
        spread_out.arrive_core(j)
    save = pltpu.make_async_copy(gb, gb_out, local.at[8])
    save.start()
    for j in range(place.ys):
        scatter.core_copy(j).wait_send()
    for j in range(1, place.ys):
        scatter.y_copy(j, ds.at[place.s]).wait_send()
    spread_out.drain()
    r2.drain_x()
    r1.drain_x()
    for copy in (*keep_parts, *keep, save):
        copy.wait()


def feed(place, length, x, mix, cot, wo, w1, w2, vectors):
    seq, rows, _ = x.shape
    slots = seq * rows
    chunk = chunk_of(slots)
    width = w1.shape[1]
    share, units = D // place.dp, width // place.dp
    split = []
    anyspace = pl.BlockSpec(memory_space=pl.ANY)
    inside = pl.BlockSpec(memory_space=pltpu.VMEM)
    vm = lambda *shape: pltpu.VMEM(shape, BF16)
    if not whole_tiles(share, units):
        split = [
            vm(place.dp, share, width), vm(place.dp, units, D), vm(place.zs, share, width),
            vm(place.zs, units, D),
        ]
    outs = [
        ((seq, rows, D), BF16, anyspace),
        ((rows, D), F32, inside),
        ((rows, D), F32, inside),
        ((seq, rows, D), BF16, anyspace),
        ((place.zs, share, width), BF16, anyspace),
        ((place.zs, units, D), BF16, anyspace),
        ((8, D), F32, inside),
    ]
    return pl.pallas_call(
        functools.partial(feed_kernel, place),
        in_specs=[pl.BlockSpec(memory_space=pltpu.SMEM)] + [anyspace] * 6 + [inside],
        out_specs=[spec for _, _, spec in outs],
        out_shape=[jax.ShapeDtypeStruct(shape, kind) for shape, kind, _ in outs],
        scratch_shapes=[
            vm(seq, rows, D),
            vm(D, slots),
            vm(seq, rows, D),
            vm(D, D),
            vm(D, width),
            vm(width, D),
            vm(slots, D),
            vm(slots, width),
            vm(slots, width),
            vm(slots, D),
            vm(seq, rows, D),
            pltpu.VMEM((chunk, D), F32),
            vm(place.ys, rows, D),
            vm(max(place.ys - 1, 1), rows, D),
            vm(max(place.xs - 1, 1), place.zs, share, width),
            vm(max(place.xs - 1, 1), place.zs, units, D),
        ]
        + split
        + dp_semaphores(place, 3)
        + seq_semaphores(place, 2)
        + [pltpu.SemaphoreType.DMA((9 + seq + 2 * place.zs,))],
        compiler_params=params(collective_id=1, has_side_effects=True),
        name="feed",
    )(length, x, mix, cot, wo, w1, w2, vectors)


class SumSmall:
    def __init__(self, place, values, landing, sems):
        self.p, self.values, self.landing = place, values, landing
        self.sends, self.recvs = sems
        self.hops = [
            [((place.d, place.partner))],
            [(place.d, place.at_y(j, place.c)) for j in range(1, place.ys)],
            [(place.at_x(j), place.s) for j in range(1, place.xs)],
            [(place.at_z(k), place.s) for k in range(1, place.zs)],
        ]

    def copies(self, hop):
        first = sum(len(peers) for peers in self.hops[:hop])
        return [
            (first + i, send(self.values.at[hop], self.landing.at[first + i],
                             self.sends.at[first + i], self.recvs.at[first + i], peer))
            for i, peer in enumerate(self.hops[hop])
        ]

    def start(self, hop):
        for _, copy in self.copies(hop):
            copy.start()

    def fold(self, hop):
        value = self.values[hop]
        for i, copy in self.copies(hop):
            copy.wait_recv()
            value = value + self.landing[i]
        return value

    def drain(self):
        for hop in range(4):
            for _, copy in self.copies(hop):
                copy.wait_send()


def small_hops(place):
    return 1 + (place.ys - 1) + (place.xs - 1) + (place.zs - 1)


def tail_kernel(
    place, vec_ref, sums_ref, lse_ref, middle_ref, gmid_ref,
    qt_in, kt_in, k_in, v_in, gb_in, mix_in, wo_in, wq_in, normed_in, x_in, part_in, s1_in, s2_in,
    layer_ref, input_ref, total_ref, w1_out, w2_out, wq_out, wo_out,
    qt, kt, kn, vn, got, gbv, mixv, normed, wq, dqkv, wo_rows, gbs, dk_sum, dv_sum, xbuf, outp,
    core_a, y_a, core_b, y_b, pq, po, xq, xo, tq, to, zq, zo, z1, z2, r1, r2, rq, ro, own1, own2,
    values, landing, *rest,
):
    zsend, zrecv, xsend, xrecv, ssend, srecv, vsend, vrecv, local = rest[-9:]
    place.locate()
    seq, rows, _ = x_in.shape
    slots = seq * rows
    chunk = chunk_of(slots)
    joined = chunk // rows
    count = slots // chunk
    heads = kt.shape[0]
    wide = heads * HEAD_DIM
    share = D // place.dp
    place.barrier()
    dp_sems, seq_sems = (zsend, zrecv, xsend, xrecv), (ssend, srecv)
    e1 = gbv
    if whole_tiles(share):
        q_part = lambda d: pq.at[pl.ds(pl.multiple_of(d * share, 16), share), :]
        o_part = lambda d: po.at[pl.ds(pl.multiple_of(d * share, 16), share), :]
    else:
        pq_split, po_split = rest[:2]
        q_part, o_part = (lambda d: pq_split.at[d]), (lambda d: po_split.at[d])
    g1 = ScatterDp(place, 0, dp_sems, None, None, lambda zi: s1_in.at[zi], lambda k: z1.at[k - 1])
    g2 = ScatterDp(place, 1, dp_sems, None, None, lambda zi: s2_in.at[zi], lambda k: z2.at[k - 1])
    gq = ScatterDp(place, 2, dp_sems, q_part, lambda j, zi: xq.at[j - 1, zi],
                   lambda zi: tq.at[zi], lambda k: zq.at[k - 1])
    go = ScatterDp(place, 3, dp_sems, o_part, lambda j, zi: xo.at[j - 1, zi],
                   lambda zi: to.at[zi], lambda k: zo.at[k - 1])
    out_sum = ScatterSeq(place, 0, seq_sems, lambda s: part_in.at[s], lambda j: core_a.at[j],
                         lambda j: y_a.at[j - 1])
    e1_sum = ScatterSeq(place, 1, seq_sems, lambda s: e1.at[s], lambda j: core_b.at[j],
                        lambda j: y_b.at[j - 1])
    final2 = GatherSeq(place, 2, seq_sems, r2, lambda s: w2_out.at[s])
    final1 = GatherSeq(place, 3, seq_sems, r1, lambda s: w1_out.at[s])
    final_o = GatherSeq(place, 4, seq_sems, ro, lambda s: wo_out.at[s])
    final_q = GatherSeq(place, 5, seq_sems, rq, lambda s: wq_out.at[s])

    first = [(gb_in, gbv), (wo_in.at[pl.ds(pl.multiple_of(place.s * wide, 16), wide), :], wo_rows),
             (mix_in, mixv), (qt_in, qt), (kt_in, kt), (k_in, kn), (v_in, vn)]
    later = [(normed_in, normed), (wq_in, wq), (s1_in.at[place.z], own1), (s2_in.at[place.z], own2)]
    later += [(part_in.at[place.at_y(j, place.c)], outp.at[j]) for j in range(place.ys)]
    loads = [
        pltpu.make_async_copy(src, dst, local.at[i]) for i, (src, dst) in enumerate(first + later)
    ]
    free = len(loads)
    for copy in loads:
        copy.start()
    g2.start_z()
    g1.start_z()
    for j in list(range(1, place.ys)) + [0]:
        out_sum.core_copy(j).start()
    for copy in loads[: len(first)]:
        copy.wait()

    def lines_of(index, size, step=16):
        return pl.ds(pl.multiple_of(index * size, step), size)

    def turn(i, _):
        cols = pl.ds(pl.multiple_of(i * chunk, 128), chunk)
        branch = gbv[pl.ds(i * joined, joined)].reshape(chunk, D)
        got[:, cols] = dot(wo_rows[...], branch, ((1,), (1,))).astype(BF16)
        for s in range(seq):

            @pl.when(place.s == s)
            def _():
                gbs[lines_of(i, chunk), :] = branch[:, s * wide : (s + 1) * wide]

        return 0

    lax.fori_loop(0, count, turn, 0)

    def wo_grad(i, _):
        lines = pl.ds(pl.multiple_of(i * 256, 128), 256)
        po[lines, :] = dot(mixv[lines, :], gbs[...]).astype(BF16)
        return 0

    lax.fori_loop(0, D // 256, wo_grad, 0)
    if not whole_tiles(share):
        for d in range(place.dp):
            po_split[d] = po[d * share : (d + 1) * share, :]
    go.start_x()

    block = 256

    def head_back(head):
        part = slice(head * HEAD_DIM, (head + 1) * HEAD_DIM)
        dk_sum[...] = jnp.zeros_like(dk_sum)
        dv_sum[...] = jnp.zeros_like(dv_sum)

        def one(i, _):
            cols = pl.ds(pl.multiple_of(i * block, 128), block)
            grad = got[part, cols]
            own_rows = pl.ds(pl.multiple_of(place.s * wide + head * HEAD_DIM, 16), HEAD_DIM)
            mixed = mixv[own_rows, cols]
            delta = jnp.sum(grad.astype(F32) * mixed.astype(F32), axis=0, keepdims=True)
            probs = jnp.exp2(dot(kn[head], qt[head, :, cols]) * QSCALE - lse_ref[head, :, cols])
            grad_scores = (probs * (dot(vn[head], grad) - delta)).astype(BF16)
            dv_sum[...] += dot(probs.astype(BF16), grad, ((1,), (1,)))
            dk_sum[...] += dot(grad_scores, qt[head, :HEAD_DIM, cols], ((1,), (1,)))
            turned = dot(kt[head], grad_scores) * SCALE
            dqkv[pl.ds(pl.multiple_of(i * block, 128), block), part] = jnp.transpose(turned).astype(BF16)
            return 0

        lax.fori_loop(0, slots // block, one, 0)
        dqkv[:, wide + head * HEAD_DIM : wide + (head + 1) * HEAD_DIM] = (
            dk_sum[...] * SCALE
        ).astype(BF16)
        dqkv[:, 2 * wide + head * HEAD_DIM : 2 * wide + (head + 1) * HEAD_DIM] = dv_sum[...].astype(
            BF16
        )

    def out_fold():
        for j in range(1, place.ys):
            out_sum.core_copy(j).wait_recv()
            outp[j] = (outp[j].astype(F32) + core_a[j].astype(F32)).astype(BF16)
            out_sum.y_copy(j, outp.at[j]).start()

    def publish(group, own, result, final):
        result[...] = group.finish(own).astype(BF16)
        final.start()

    for head in range(heads):
        head_back(head)
        if head == 0:
            for copy in loads[len(first) :]:
                copy.wait()
            out_fold()
            go.fold_all()
            go.start_z()
        if head == min(1, heads - 1):
            publish(g2, own2, r2, final2)
        if head == min(2, heads - 1):
            publish(g1, own1, r1, final1)
            publish(go, to.at[place.z], ro, final_o)

    def q_grad(i, _):
        cols = pl.ds(pl.multiple_of(i * 256, 128), 256)
        pq[cols, :] = dot(normed[:, cols], dqkv[...], ((0,), (0,))).astype(BF16)
        return 0

    lax.fori_loop(0, D // 256, q_grad, 0)
    if not whole_tiles(share):
        for d in range(place.dp):
            pq_split[d] = pq[d * share : (d + 1) * share, :]
    gq.start_x()
    total = sums_ref[...]
    bias_sum = jnp.sum(dqkv[...].astype(F32), axis=0, keepdims=True)
    values[0] = jnp.zeros_like(values[0])
    values[0, 0:8] = total
    values[0, pl.ds(8 + place.s, 1), :wide] = bias_sum[:, :wide]
    values[0, pl.ds(8 + place.s, 1), wide : 2 * wide] = bias_sum[:, 2 * wide :]
    values[0, pl.ds(8 + seq + place.s, 1), :] = total[7:8]
    values[0, 7:8] = jnp.zeros((1, D), F32)

    order = []
    for j in list(range(1, place.ys)) + [0]:
        if joined == 1:
            order += [(place.at_y(j, 1 - place.c), j, False), (place.at_y(j, place.c), j, True)]
        else:
            order += [(lax.rem(place.y + j, place.ys), j, True)]

    def x_load(at, slot):
        return pltpu.make_async_copy(
            x_in.at[pl.ds(at * joined, joined)], xbuf.at[slot], local.at[free + slot]
        )

    x_load(order[0][0], 0).start()
    for step, (at, j, both) in enumerate(order):
        slot = step % 2
        if step + 1 < len(order):
            x_load(order[step + 1][0], 1 - slot).start()
        x_load(at, slot).wait()
        grad = dot(dqkv[lines_of(at, chunk), :], wq[...].reshape(D, 3 * wide), ((1,), (1,)))
        normal, spread = normalize(xbuf[slot].reshape(chunk, D).astype(F32))
        values[0, 0:1] += jnp.sum(grad * normal, axis=0, keepdims=True)
        values[0, 1:2] += jnp.sum(grad, axis=0, keepdims=True)
        e1[pl.ds(at * joined, joined)] = grad.astype(BF16).reshape(joined, rows, D)
        if joined == 2 or not both:
            e1_sum.core_copy(j).start()
        if both and j:
            target = place.at_y(j, place.c)
            e1_sum.core_copy(j).wait_recv()
            e1[target] = (e1[target].astype(F32) + core_b[j].astype(F32)).astype(BF16)
            e1_sum.y_copy(j, e1.at[target]).start()
    small = SumSmall(place, values, landing, (vsend, vrecv))
    small.start(0)
    gq.fold_all()
    gq.start_z()
    for hop in range(3):
        values[hop + 1] = small.fold(hop)
        small.start(hop + 1)
    for final in (final2, final1, final_o):
        for j in range(1, place.ys):
            final.arrive_y(j)

    value = outp[0].astype(F32)
    out_sum.core_copy(0).wait_recv()
    value = value + core_a[0].astype(F32)
    for j in range(1, place.ys):
        out_sum.y_copy(j, outp.at[j]).wait_recv()
        value = value + y_a[j - 1].astype(F32)
    layer_ref[...] = (middle_ref[...] + (value + vec_ref[5:6])).astype(BF16)

    value = e1[place.s].astype(F32)
    e1_sum.core_copy(0).wait_recv()
    value = value + core_b[0].astype(F32)
    for j in range(1, place.ys):
        e1_sum.y_copy(j, e1.at[place.s]).wait_recv()
        value = value + y_b[j - 1].astype(F32)
    last = (len(order) - 1) % 2
    hidden = xbuf[last, lax.rem(place.s, joined)].astype(F32)
    normal, spread = normalize(hidden)
    input_ref[...] = (gmid_ref[...] + norm_backward(normal, spread, value * vec_ref[0:1])).astype(
        BF16
    )
    total_ref[...] = small.fold(3)
    publish(gq, tq.at[place.z], rq, final_q)
    keep = [
        pltpu.make_async_copy(src, dst.at[place.s], local.at[free + 2 + i])
        for i, (src, dst) in enumerate([(r1, w1_out), (r2, w2_out), (rq, wq_out), (ro, wo_out)])
    ]
    for copy in keep:
        copy.start()
    for final in (final2, final1, final_o):
        for j in range(place.ys):
            final.arrive_core(j)
    for j in range(1, place.ys):
        final_q.arrive_y(j)
    for j in range(place.ys):
        final_q.arrive_core(j)
    for final in (final1, final2, final_o, final_q):
        final.drain()
    for group in (out_sum, e1_sum):
        for j in range(place.ys):
            group.core_copy(j).wait_send()
        for j in range(1, place.ys):
            group.y_copy(j, outp.at[j]).wait_send()
    for group in (gq, go):
        group.drain_x()
    for group in (g1, g2, gq, go):
        group.drain_z()
    small.drain()
    for copy in keep:
        copy.wait()


def tail(place, vectors, sums, lse, middle, gmid, qt, kt, kn, vn, gb, mix, wo, wq, normed, x, part, s1, s2):
    seq, rows, _ = x.shape
    slots = seq * rows
    chunk = chunk_of(slots)
    joined = chunk // rows
    heads = kt.shape[0]
    wide = heads * HEAD_DIM
    share = D // place.dp
    width, units = s1.shape[2], s2.shape[1]
    ys, xs, zs = place.ys, max(place.xs - 1, 1), place.zs
    anyspace = pl.BlockSpec(memory_space=pl.ANY)
    inside = pl.BlockSpec(memory_space=pltpu.VMEM)
    vm = lambda *shape: pltpu.VMEM(shape, BF16)
    tall = 8 + 2 * seq
    hops = small_hops(place)
    outs = [
        ((rows, D), BF16, inside),
        ((rows, D), BF16, inside),
        ((tall, D), F32, inside),
        ((seq, share, width), BF16, anyspace),
        ((seq, units, D), BF16, anyspace),
        ((seq, share, 3 * wide), BF16, anyspace),
        ((seq, share, wide), BF16, anyspace),
    ]
    split = []
    if not whole_tiles(share):
        split = [vm(place.dp, share, 3 * wide), vm(place.dp, share, wide)]
    return pl.pallas_call(
        functools.partial(tail_kernel, place),
        in_specs=[inside] * 5 + [anyspace] * 13,
        out_specs=[spec for _, _, spec in outs],
        out_shape=[jax.ShapeDtypeStruct(shape, kind) for shape, kind, _ in outs],
        scratch_shapes=[
            vm(heads, 128, slots),
            vm(heads, HEAD_DIM, slots),
            vm(heads, slots, 128),
            vm(heads, slots, HEAD_DIM),
            vm(wide, slots),
            vm(seq, rows, D),
            vm(D, slots),
            vm(slots, D),
            vm(place.dp, share, 3 * wide),
            vm(slots, 3 * wide),
            vm(wide, D),
            vm(slots, wide),
            pltpu.VMEM((slots, HEAD_DIM), F32),
            pltpu.VMEM((slots, HEAD_DIM), F32),
            vm(2, joined, rows, D),
            vm(ys, rows, D),
            vm(ys, rows, D),
            vm(max(ys - 1, 1), rows, D),
            vm(ys, rows, D),
            vm(max(ys - 1, 1), rows, D),
            vm(D, 3 * wide),
            vm(D, wide),
            vm(xs, zs, share, 3 * wide),
            vm(xs, zs, share, wide),
            vm(zs, share, 3 * wide),
            vm(zs, share, wide),
            vm(zs - 1, share, 3 * wide),
            vm(zs - 1, share, wide),
            vm(zs - 1, share, width),
            vm(zs - 1, units, D),
            vm(share, width),
            vm(units, D),
            vm(share, 3 * wide),
            vm(share, wide),
            vm(share, width),
            vm(units, D),
            pltpu.VMEM((4, tall, D), F32),
            pltpu.VMEM((hops, tall, D), F32),
        ]
        + split
        + dp_semaphores(place, 4)
        + seq_semaphores(place, 6)
        + [
            pltpu.SemaphoreType.DMA((hops,)),
            pltpu.SemaphoreType.DMA((hops,)),
            pltpu.SemaphoreType.DMA((24 + ys,)),
        ],
        compiler_params=params(collective_id=2, has_side_effects=True),
        name="tail",
    )(vectors, sums, lse, middle, gmid, qt, kt, kn, vn, gb, mix, wo, wq, normed, x, part, s1, s2)


def gather(value, axes, axis=0):
    return lax.all_gather(value, axes, axis=axis, tiled=True)


def scatter_sum(value, axes, axis=0):
    return lax.psum_scatter(value, axes, scatter_dimension=axis, tiled=True)


def per_device(
    hidden_in, cotangent, clip_lengths, clip_order, first_gain, first_shift, query_weight,
    query_bias, key_weight, value_weight, value_bias, output_weight, output_bias, second_gain,
    second_shift, expand_weight, expand_bias, reduce_weight, reduce_bias,
):
    dp = lax.axis_size("dp")
    seq = lax.axis_size("seq")
    me = lax.axis_index("seq")
    rows_here = hidden_in.shape[1]
    slots = rows_here * seq
    share = D // dp
    head_cols = D // seq
    heads = HEADS // seq
    units = FF // (dp * seq)
    quarter = dp * units

    hidden_own = hidden_in[0]
    matches = clip_order[0] == jnp.arange(clip_lengths.shape[0], dtype=jnp.int32)
    length = jnp.sum(jnp.where(matches, clip_lengths, 0)).reshape(1)

    spot = Place(dp, seq)
    mine_dp = lax.axis_index("dp")

    def columns(weight):
        return lax.dynamic_slice_in_dim(weight, me * head_cols, head_cols, 1)

    width = 3 * head_cols
    extra = -(-(8 * share + FF // dp) // width)
    tall = -(-(share + extra) // 16) * 16

    def spread(vector):
        return lax.dynamic_update_slice_in_dim(jnp.zeros((D,), BF16), vector, mine_dp * share, 0)

    def head_part(vector):
        part = lax.dynamic_slice_in_dim(spread(vector), me * head_cols, head_cols, 0)
        return jnp.pad(part, (0, D - head_cols))

    expand_own = lax.dynamic_slice_in_dim(expand_bias, me * units, units, 0)
    expand_row = lax.dynamic_update_slice_in_dim(
        jnp.zeros((quarter,), BF16), expand_own, mine_dp * units, 0
    )
    blank = jnp.zeros((D,), BF16)
    small = jnp.stack(
        [spread(first_gain), spread(first_shift), spread(output_bias), spread(second_gain),
         spread(second_shift), spread(reduce_bias), jnp.pad(expand_row, (0, D - quarter)), blank,
         head_part(query_bias), head_part(value_bias)] + [blank] * 6
    )
    wqkv_share = jnp.concatenate(
        [columns(query_weight), columns(key_weight), columns(value_weight)], axis=1
    )
    w1_share = jnp.concatenate(
        [
            lax.dynamic_slice_in_dim(expand_weight, d * (FF // dp) + me * units, units, 1)
            for d in range(dp)
        ],
        axis=1,
    )
    w2_share = lax.dynamic_slice_in_dim(reduce_weight, me * units, units, 0)
    (
        x, cot, small, w_qkv, w_out, w_expand, normed, qt, kt, keys, values, mix, lse,
    ) = front(spot, length, hidden_own, cotangent[0], small, wqkv_share, output_weight, w1_share)
    w_out = w_out.reshape(D, D)
    w_expand = w_expand.reshape(D, quarter)
    vectors = jnp.sum(small.astype(F32), axis=0)
    mix = mix.reshape(D, slots)
    grad_branch, middle, grad_middle, out_part, s1, s2, sums = feed(
        spot, length, x, mix, cot, w_out, w_expand, w2_share, vectors
    )
    layer_output, input_grad, totals, w1_grad, w2_grad, qkv_grad, wo_grad = tail(
        spot, vectors, sums, lse, middle, grad_middle, qt, kt, keys, values, grad_branch, mix,
        w_out, w_qkv, normed, x, out_part, s1, s2,
    )

    def own(vector):
        return lax.dynamic_slice_in_dim(vector.reshape(-1), mine_dp * share, share, 0)

    w2_grad = w2_grad.reshape(FF // dp, D).astype(F32)
    w1_grad = (
        w1_grad.reshape(seq, share, dp, units).transpose(1, 2, 0, 3).reshape(share, FF).astype(F32)
    )
    wo_grad = wo_grad.transpose(1, 0, 2).reshape(share, D).astype(F32)
    qkv_grad = qkv_grad.reshape(seq, share, 3, head_cols).astype(F32)
    qkv_grad = qkv_grad.transpose(2, 1, 0, 3).reshape(3, share, D)
    bias = totals[8 : 8 + seq]
    expand_bias_grad = lax.dynamic_slice_in_dim(
        totals[8 + seq : 8 + 2 * seq, :quarter].reshape(seq, dp, units), mine_dp, 1, 1
    ).reshape(FF // dp)
    return (
        layer_output[None],
        input_grad[None],
        own(totals[0]),
        own(totals[1]),
        qkv_grad[0],
        own(bias[:, :head_cols]),
        qkv_grad[1],
        qkv_grad[2],
        own(bias[:, head_cols : 2 * head_cols]),
        wo_grad,
        own(totals[2]),
        own(totals[3]),
        own(totals[4]),
        w1_grad,
        expand_bias_grad,
        w2_grad,
        own(totals[5]),
    )


def solution(mesh):
    clip = P("dp", "seq", None)
    vec = P("dp")
    mat = P("dp", None)
    return jax.shard_map(
        per_device,
        mesh=mesh,
        in_specs=(
            clip, clip, P(), vec, vec, vec, mat, vec, mat, mat, vec, mat, vec, vec, vec, mat, vec,
            mat, vec,
        ),
        out_specs=(
            clip, clip, vec, vec, mat, vec, mat, mat, vec, mat, vec, vec, vec, mat, vec, mat, vec,
        ),
        check_vma=False,
    )
```

```python
import functools

import jax
import jax.numpy as jnp
from jax import lax
from jax.experimental import pallas as pl
from jax.experimental.pallas import tpu as pltpu
from jax.sharding import PartitionSpec as P

D = 1280
FF = 5120
HEADS = 16
HEAD_DIM = D // HEADS
EPSILON = 1e-05
SCALE = HEAD_DIM ** (-0.5)
F32 = jnp.float32
BF16 = jnp.bfloat16
VMEM_LIMIT = 66_000_000
MESH = pl.DeviceIdType.MESH


def dot(left, right, contract=((1,), (0,))):
    return lax.dot_general(left, right, (contract, ((), ())), preferred_element_type=F32)


def normalize(values):
    average = jnp.mean(values, axis=-1, keepdims=True)
    centered = values - average
    variance = jnp.mean(centered * centered, axis=-1, keepdims=True)
    spread = lax.rsqrt(variance + EPSILON)
    return centered * spread, spread


def norm_backward(unit, spread, grad_unit):
    inner = jnp.mean(grad_unit * unit, axis=-1, keepdims=True)
    return spread * (grad_unit - jnp.mean(grad_unit, axis=-1, keepdims=True) - unit * inner)


def params(**extra):
    return pltpu.CompilerParams(vmem_limit_bytes=VMEM_LIMIT, **extra)


def whole(shape):
    return pl.BlockSpec(shape, lambda *_: (0,) * len(shape), pipeline_mode=pl.Buffered(1))


def chunk_of(slots):
    return slots // 4 if slots % 512 == 0 else slots


class Place:
    def __init__(self, dp, seq):
        self.dp, self.seq = dp, seq
        self.xs = 1 << ((dp.bit_length() - 1) // 2)
        self.zs = dp // self.xs
        self.ys = seq // 2

    def locate(self):
        self.d, self.s = lax.axis_index("dp"), lax.axis_index("seq")
        self.z, self.x = self.d // self.xs, lax.rem(self.d, self.xs)
        self.y, self.c = self.s // 2, lax.rem(self.s, 2)
        self.partner = self.y * 2 + 1 - self.c

    def at_z(self, k):
        return lax.rem(self.z + k + self.zs, self.zs) * self.xs + self.x

    def block(self, k, j):
        return lax.rem(self.z - k + self.zs, self.zs) * self.xs + lax.rem(
            self.x - j + self.xs, self.xs
        )

    def at_x(self, j):
        return self.z * self.xs + lax.rem(self.x + j, self.xs)

    def at_y(self, j, core):
        return lax.rem(self.y + j + self.ys, self.ys) * 2 + core

    def peers(self, over_dp=True, over_seq=True):
        found = []
        if over_dp:
            found += [(self.at_z(k), self.s) for k in range(1, self.zs)]
            found += [(self.at_x(j), self.s) for j in range(1, self.xs)]
        if over_seq:
            found += [(self.d, self.partner)]
            found += [(self.d, self.at_y(j, self.c)) for j in range(1, self.ys)]
        return found

    def barrier(self, **which):
        semaphore = pltpu.get_barrier_semaphore()
        peers = self.peers(**which)
        for peer in peers:
            pl.semaphore_signal(semaphore, inc=1, device_id=peer, device_id_type=MESH)
        pl.semaphore_wait(semaphore, len(peers))


def send(src, dst, send_sem, recv_sem, device):
    return pltpu.make_async_remote_copy(
        src_ref=src, dst_ref=dst, send_sem=send_sem, recv_sem=recv_sem, device_id=device,
        device_id_type=MESH,
    )


def dp_semaphores(place, groups):
    return [
        pltpu.SemaphoreType.DMA((groups, place.zs)),
        pltpu.SemaphoreType.DMA((groups, place.zs)),
        pltpu.SemaphoreType.DMA((groups, place.zs, place.xs)),
        pltpu.SemaphoreType.DMA((groups, place.zs, place.xs)),
    ]


def seq_semaphores(place, groups):
    return [pltpu.SemaphoreType.DMA((groups, 2, place.ys))] * 2


class GatherDp:
    def __init__(self, place, group, sems, own, slab, on=None):
        self.p, self.g, self.own, self.slab, self.on = place, group, own, slab, on
        self.zsend, self.zrecv, self.xsend, self.xrecv = sems

    def when(self, block, act):
        if self.on is None:
            act()
        else:
            pl.when(self.on(block))(act)

    def z_copy(self, k):
        return send(self.own, self.slab(self.p.d), self.zsend.at[self.g, k],
                    self.zrecv.at[self.g, k], (self.p.at_z(k), self.p.s))

    def x_copy(self, k, j):
        block = self.p.block(k, 0)
        src = self.own if k == 0 else self.slab(block)
        return send(src, self.slab(block), self.xsend.at[self.g, k, j],
                    self.xrecv.at[self.g, k, j], (self.p.at_x(j), self.p.s))

    def start_x(self):
        def act():
            for j in range(1, self.p.xs):
                self.x_copy(0, j).start()

        self.when(self.p.d, act)

    def start_z(self):
        def act():
            for k in range(self.p.zs - 1, 0, -1):
                self.z_copy(k).start()

        self.when(self.p.d, act)

    def forward(self, k):
        place = self.p

        def act():
            send(self.own, self.slab(place.block(k, 0)), self.zsend.at[self.g, k],
                 self.zrecv.at[self.g, k], (place.at_z(k), place.s)).wait_recv()
            for j in range(1, place.xs):
                self.x_copy(k, j).start()

        self.when(place.block(k, 0), act)

    def forward_all(self):
        for k in range(1, self.p.zs):
            self.forward(k)

    def arrive(self):
        place = self.p
        for k in range(place.zs):
            for j in range(1, place.xs):
                wait = send(self.own, self.slab(place.block(k, j)), self.xsend.at[self.g, k, j],
                            self.xrecv.at[self.g, k, j], (place.at_x(j), place.s)).wait_recv
                self.when(place.block(k, j), wait)

    def drain(self):
        place = self.p

        def act():
            for k in range(1, place.zs):
                self.z_copy(k).wait_send()

        self.when(place.d, act)
        for k in range(place.zs):
            for j in range(1, place.xs):
                self.when(place.block(k, 0), self.x_copy(k, j).wait_send)


class GatherSeq:
    def __init__(self, place, group, sems, own, slab):
        self.p, self.g, self.own, self.slab = place, group, own, slab
        self.sends, self.recvs = sems

    def y_copy(self, j):
        place = self.p
        return send(self.own, self.slab(place.s), self.sends.at[self.g, 0, j],
                    self.recvs.at[self.g, 0, j], (place.d, place.at_y(j, place.c)))

    def core_copy(self, j):
        place = self.p
        block = place.at_y(-j, place.c)
        src = self.own if j == 0 else self.slab(block)
        return send(src, self.slab(block), self.sends.at[self.g, 1, j],
                    self.recvs.at[self.g, 1, j], (place.d, place.partner))

    def start(self):
        for j in range(1, self.p.ys):
            self.y_copy(j).start()
        self.core_copy(0).start()

    def arrive_y(self, j):
        place = self.p
        block = place.at_y(-j, place.c)
        send(self.own, self.slab(block), self.sends.at[self.g, 0, j], self.recvs.at[self.g, 0, j],
             (place.d, place.at_y(j, place.c))).wait_recv()
        self.core_copy(j).start()
        return block

    def arrive_core(self, j):
        place = self.p
        block = place.at_y(-j, 1 - place.c)
        send(self.own, self.slab(block), self.sends.at[self.g, 1, j], self.recvs.at[self.g, 1, j],
             (place.d, place.partner)).wait_recv()
        return block

    def drain(self):
        for j in range(1, self.p.ys):
            self.y_copy(j).wait_send()
        for j in range(self.p.ys):
            self.core_copy(j).wait_send()


LOG2E = 1.4426950408889634
QSCALE = SCALE * LOG2E


def own_length(lengths_ref, order_ref):
    length = 0
    for clip in range(lengths_ref.shape[0]):
        length = length + jnp.where(order_ref[0] == clip, lengths_ref[clip], 0)
    return length


def front_kernel(
    place, lengths_ref, order_ref, x_in, sm_in, wq_in, wo_in, w1_in,
    x_out, vec_out, wq_out, wo_out, w1_out, normed_out, qt_out, kt_out, k_out,
    v_out, mix_out, lse_ref,
    xs, nr, sm, wq, wt, qt, kt, vt, kn, vn, mix,
    zsend, zrecv, xsend, xrecv, ssend, srecv, local,
):
    place.locate()
    seq, rows = x_out.shape[0], x_out.shape[1]
    slots = seq * rows
    heads = k_out.shape[0]
    wide = heads * HEAD_DIM
    place.barrier()
    dp_sems = (zsend, zrecv, xsend, xrecv)
    seq_sems = (ssend, srecv)

    def over_dp(group, own, buffer):
        return GatherDp(place, group, dp_sems, own, lambda d: buffer.at[d])

    def over_seq(group, own, buffer):
        return GatherSeq(place, group, seq_sems, own, lambda s: buffer.at[s])

    g_sm = over_dp(0, sm_in, sm)
    g_wq = over_dp(1, wq_in, wq)
    g_wo = GatherDp(place, 2, dp_sems, wo_in, lambda d: wo_out.at[d],
                    lambda d: lax.rem(d, seq) == place.s)
    g_w1 = over_dp(3, w1_in, w1_out)
    g_x = over_seq(0, x_in, xs)
    wo_sets = [
        GatherSeq(place, 1 + heads + i, seq_sems, wo_out.at[i * seq + place.s],
                  lambda s, i=i: wo_out.at[i * seq + s])
        for i in range(place.dp // seq)
    ]
    locals_in = [
        pltpu.make_async_copy(x_in, xs.at[place.s], local.at[0]),
        pltpu.make_async_copy(sm_in, sm.at[place.d], local.at[1]),
        pltpu.make_async_copy(wq_in, wq.at[place.d], local.at[2]),
    ]
    w1_own = pltpu.make_async_copy(w1_in, w1_out.at[place.d], local.at[5])
    wo_own = pltpu.make_async_copy(wo_in, wo_out.at[place.d], local.at[4])
    for copy in locals_in:
        copy.start()
    g_sm.start_x()
    g_sm.start_z()
    g_x.start()
    g_wq.start_x()
    for group in (g_wq, g_wo, g_w1):
        group.start_z()
    w1_own.start()
    pl.when(g_wo.on(place.d))(wo_own.start)

    column = lax.broadcasted_iota(jnp.int32, (slots, 1), 0)
    penalty = jnp.where(column >= own_length(lengths_ref, order_ref), -1e30, 0.0).astype(BF16)
    ones_row = jnp.where(
        lax.broadcasted_iota(jnp.int32, (128 - HEAD_DIM, slots), 0) == 0, 1.0, 0.0
    ).astype(BF16)
    for head in range(heads):
        kn[head] = jnp.zeros((slots, 128), BF16)
        kn[head, :, HEAD_DIM : HEAD_DIM + 1] = penalty
        qt[head, HEAD_DIM:, :] = ones_row

    for copy in locals_in:
        copy.wait()
    g_sm.forward_all()
    g_wq.forward_all()
    g_wo.start_x()
    g_w1.start_x()
    g_sm.arrive()
    vectors = jnp.sum(sm[...], axis=0)
    vec_out[...] = vectors
    gain, shift = vectors[0:1], vectors[1:2]

    def norm_block(block):
        unit, _ = normalize(xs[block].astype(F32))
        lines = pl.ds(pl.multiple_of(block * rows, 16), rows)
        nr[lines, :] = (unit * gain + shift).astype(BF16)

    norm_block(place.s)
    norm_block(g_x.arrive_core(0))
    for j in range(1, place.ys):
        norm_block(g_x.arrive_y(j))
        norm_block(g_x.arrive_core(j))
    g_wq.arrive()
    share = wq.shape[1]
    wt[...] = jnp.transpose(wq[...].reshape(place.dp * share, 3 * wide))
    bias = jnp.transpose(vectors[8:16])

    chunk = chunk_of(slots)

    def project_block(block, _):
        cols = pl.ds(pl.multiple_of(block * chunk, 128), chunk)
        lines = pl.ds(pl.multiple_of(block * chunk, 128), chunk)
        tokens = dot(wt[...], nr[lines, :], ((1,), (1,)))
        query = (tokens[:wide] + bias[:wide, 0:1]).astype(BF16)
        key = tokens[wide : 2 * wide].astype(BF16)
        value = (tokens[2 * wide :] + bias[:wide, 1:2]).astype(BF16)
        for head in range(heads):
            part = slice(head * HEAD_DIM, (head + 1) * HEAD_DIM)
            qt[head, :HEAD_DIM, cols] = query[part]
            kt[head, :, cols] = key[part]
            vt[head, :, cols] = value[part]
            kn[head, lines, :HEAD_DIM] = jnp.transpose(key[part])
            vn[head, lines, :] = jnp.transpose(value[part])
        return 0

    lax.fori_loop(0, slots // chunk, project_block, 0)
    results = [
        pltpu.make_async_copy(src, dst, local.at[7 + i])
        for i, (src, dst) in enumerate(
            [(xs, x_out), (wq, wq_out), (nr, normed_out), (qt, qt_out), (kt, kt_out),
             (kn, k_out), (vn, v_out)]
        )
    ]
    for copy in results:
        copy.start()

    block = 256
    g_wo.forward_all()
    g_wo.arrive()
    pl.when(g_wo.on(place.d))(wo_own.wait)
    for group in wo_sets:
        group.start()

    def attend(head):
        def one(i, _):
            cols = pl.ds(pl.multiple_of(i * block, 128), block)
            scores = dot(kn[head], qt[head, :, cols])
            top = jnp.max(scores, axis=0, keepdims=True)
            exponent = jnp.exp2((scores - top) * QSCALE)
            total = jnp.sum(exponent, axis=0, keepdims=True)
            mixed = dot(vt[head], exponent.astype(BF16)) / total
            mix[place.s, head, :, cols] = mixed.astype(BF16)
            lse_ref[head, :, cols] = top * QSCALE + jnp.log2(total)
            return 0

        lax.fori_loop(0, slots // block, one, 0)

    g_mix = [
        GatherSeq(place, 1 + head, seq_sems, mix.at[place.s, head],
                  lambda s, head=head: mix.at[s, head])
        for head in range(heads)
    ]
    for head in range(heads):
        attend(head)
        g_mix[head].start()
        if head == 0:
            g_w1.forward(1)
        if head == min(1, heads - 1):
            for group in wo_sets:
                for j in range(1, place.ys):
                    group.arrive_y(j)
            for k in range(2, place.zs):
                g_w1.forward(k)
    for head in range(heads):
        for j in range(1, place.ys):
            g_mix[head].arrive_y(j)
    for head in range(heads):
        for j in range(place.ys):
            g_mix[head].arrive_core(j)
    mix_copy = pltpu.make_async_copy(mix, mix_out, local.at[15])
    mix_copy.start()
    for group in wo_sets:
        for j in range(place.ys):
            group.arrive_core(j)
    g_w1.arrive()
    for group in (g_sm, g_wq, g_wo, g_w1, g_x, *wo_sets, *g_mix):
        group.drain()
    for copy in (w1_own, *results, mix_copy):
        copy.wait()


def front(place, lengths, order, x, small, wqkv, wo, w1):
    dp, seq = place.dp, place.seq
    rows = x.shape[0]
    slots = rows * seq
    heads = HEADS // seq
    share, width = wqkv.shape
    anyspace = pl.BlockSpec(memory_space=pl.ANY)
    shapes = [
        (seq, rows, D),
        small.shape,
        (dp, share, width),
        (dp, *wo.shape),
        (dp, *w1.shape),
        (slots, D),
        (heads, 128, slots),
        (heads, HEAD_DIM, slots),
        (heads, slots, 128),
        (heads, slots, HEAD_DIM),
        (seq, heads, HEAD_DIM, slots),
    ]
    vm = lambda *shape: pltpu.VMEM(shape, BF16)
    return pl.pallas_call(
        functools.partial(front_kernel, place),
        in_specs=[pl.BlockSpec(memory_space=pltpu.SMEM)] * 2 + [anyspace] * 5,
        out_specs=[anyspace, pl.BlockSpec(memory_space=pltpu.VMEM)]
        + [anyspace] * (len(shapes) - 2)
        + [pl.BlockSpec(memory_space=pltpu.VMEM)],
        out_shape=[
            jax.ShapeDtypeStruct(shape, F32 if i == 1 else BF16) for i, shape in enumerate(shapes)
        ]
        + [jax.ShapeDtypeStruct((heads, 1, slots), F32)],
        scratch_shapes=[
            vm(seq, rows, D),
            vm(slots, D),
            pltpu.VMEM((dp, *small.shape), F32),
            vm(dp, share, width),
            vm(width, D),
            vm(heads, 128, slots),
            vm(heads, HEAD_DIM, slots),
            vm(heads, HEAD_DIM, slots),
            vm(heads, slots, 128),
            vm(heads, slots, HEAD_DIM),
            vm(seq, heads, HEAD_DIM, slots),
        ]
        + dp_semaphores(place, 4)
        + seq_semaphores(place, 1 + heads + dp // seq)
        + [pltpu.SemaphoreType.DMA((16,))],
        compiler_params=params(collective_id=0, has_side_effects=True),
        name="front",
    )(lengths, order, x, small, wqkv, wo, w1)


class ScatterSeq:
    def __init__(self, place, group, sems, part, from_core, from_y):
        self.p, self.g, self.part, self.from_core, self.from_y = place, group, part, from_core, from_y
        self.sends, self.recvs = sems

    def core_copy(self, j):
        place = self.p
        return send(self.part(place.at_y(j, 1 - place.c)), self.from_core(j),
                    self.sends.at[self.g, 1, j], self.recvs.at[self.g, 1, j],
                    (place.d, place.partner))

    def y_copy(self, j, src):
        place = self.p
        return send(src, self.from_y(j), self.sends.at[self.g, 0, j], self.recvs.at[self.g, 0, j],
                    (place.d, place.at_y(j, place.c)))


class ScatterDp:
    def __init__(self, place, group, sems, out, part, from_x, from_z):
        self.p, self.g, self.out, self.part = place, group, out, part
        self.from_x, self.from_z = from_x, from_z
        self.zsend, self.zrecv, self.xsend, self.xrecv = sems
        self.order = list(range(1, place.zs)) + [0]

    def block(self, k, j):
        place = self.p
        return lax.rem(place.z + k, place.zs) * place.xs + lax.rem(place.x + j, place.xs)

    def x_copy(self, j, k):
        return send(self.out(self.block(k, j)), self.from_x(j - 1, k),
                    self.xsend.at[self.g, k, j], self.xrecv.at[self.g, k, j],
                    (self.p.at_x(j), self.p.s))

    def start_x(self):
        for k in self.order:
            for j in range(1, self.p.xs):
                self.x_copy(j, k).start()

    def z_copy(self, k):
        return send(self.part(k, self.block(k, 0)), self.from_z(k - 1),
                    self.zsend.at[self.g, k], self.zrecv.at[self.g, k], (self.p.at_z(k), self.p.s))

    def fold(self, k):
        own = self.part(k, self.block(k, 0))
        value = own[...].astype(F32)
        for j in range(1, self.p.xs):
            self.x_copy(j, k).wait_recv()
            value = value + self.from_x(j - 1, k)[...].astype(F32)
        own[...] = value.astype(BF16)
        if k:
            self.z_copy(k).start()

    def fold_all(self):
        for k in self.order:
            self.fold(k)

    def finish(self):
        value = self.part(0, self.block(0, 0))[...].astype(F32)
        for k in range(1, self.p.zs):
            self.z_copy(k).wait_recv()
            value = value + self.from_z(k - 1)[...].astype(F32)
        return value.astype(BF16)

    def drain(self):
        for k in self.order:
            for j in range(1, self.p.xs):
                self.x_copy(j, k).wait_send()
            if k:
                self.z_copy(k).wait_send()


def whole_tiles(*heights):
    return all(height % 16 == 0 for height in heights)


def feed_kernel(
    place, lengths_ref, order_ref, x_in, mix_in, cot_in, wo_in, w1_in, w2_in, vec_ref,
    gb_out, middle_out, grad_out, part_out, g1_out, s2_ref, sums_ref,
    xa, mixv, gv, wo, w1, w2, second, act, slope, unit, ds, own, from_core, from_y,
    from_x2, from_z2, *rest,
):
    zsend, zrecv, xsend, xrecv, ssend, srecv, local = rest[-7:]
    gb = xa
    place.locate()
    seq, rows, _ = x_in.shape
    slots = seq * rows
    chunk = chunk_of(slots)
    joined = chunk // rows
    width = w1.shape[1]
    share = D // place.dp
    units = width // place.dp
    place.barrier()
    dp_sems = (zsend, zrecv, xsend, xrecv)
    seq_sems = (ssend, srecv)
    aligned = whole_tiles(share, units)
    if aligned:
        w2_part = lambda d: w2.at[pl.ds(pl.multiple_of(d * units, 16), units), :]
        g2_part = lambda d: wo.at[pl.ds(pl.multiple_of(d * units, 16), units), :]
        g1_part = lambda d: w1.at[pl.ds(pl.multiple_of(d * share, 16), share), :]
    else:
        w2_split, g2_split, g1_split = rest[:3]
        w2_part, g2_part = (lambda d: w2_split.at[d]), (lambda d: g2_split.at[d])
        g1_part = lambda d: g1_split.at[d]
    if aligned:
        w2_in = w2_in.at[pl.ds(pl.multiple_of(place.s * units, 16), units), :]
    gather = GatherDp(place, 0, dp_sems, w2_in, w2_part)
    cots = GatherSeq(place, 2, seq_sems, cot_in, lambda s: gv.at[s])
    gather.start_x()
    gather.start_z()
    cots.start()
    loads = [
        pltpu.make_async_copy(src, dst, local.at[i])
        for i, (src, dst) in enumerate([(mix_in, mixv), (wo_in, wo), (w1_in, w1), (x_in, xa)])
    ]
    w2_own = pltpu.make_async_copy(w2_in, w2_part(place.d), local.at[5])
    cot_own = pltpu.make_async_copy(cot_in, gv.at[place.s], local.at[6])
    for copy in (*loads, w2_own, cot_own):
        copy.start()
    gain, shift, bias_out, bias1 = vec_ref[3:4], vec_ref[4:5], vec_ref[2:3], vec_ref[6:7, :width]
    own_chunk = place.s // joined
    sums_ref[...] = jnp.zeros_like(sums_ref)
    for copy in loads:
        copy.wait()

    def lines_of(index, size, step=16):
        return pl.ds(pl.multiple_of(index * size, step), size)

    def forward(i, _):
        lines = lines_of(i, chunk)
        hidden = xa[pl.ds(i * joined, joined)].reshape(chunk, D).astype(F32)
        cols = pl.ds(pl.multiple_of(i * chunk, 128), chunk)
        middle = hidden + (dot(mixv[:, cols], wo[...], ((0,), (0,))) + bias_out)

        @pl.when(i == own_chunk)
        def _():
            own[...] = middle

        normal, _ = normalize(middle)
        unit[lines, :] = normal.astype(BF16)
        tokens = (normal * gain + shift).astype(BF16)
        second[lines, :] = tokens
        expanded = dot(tokens, w1[...]) + bias1
        phi = 0.5 * (1.0 + lax.erf(expanded * (0.5**0.5)))
        act[lines, :] = (expanded * phi).astype(BF16)
        density = jnp.exp(-0.5 * expanded * expanded) * 0.3989422804014327
        slope[lines, :] = (phi + expanded * density).astype(BF16)
        return 0

    lax.fori_loop(0, slots // chunk, forward, 0)
    cot_own.wait()
    for j in range(1, place.ys):
        cots.arrive_y(j)
    for j in range(place.ys):
        cots.arrive_core(j)
    cots.drain()

    length = own_length(lengths_ref, order_ref)

    def mask(i, _):
        valid = i * chunk + lax.broadcasted_iota(jnp.int32, (chunk, 1), 0) < length
        cot = gv[pl.ds(i * joined, joined)].reshape(chunk, D)
        gv[pl.ds(i * joined, joined)] = jnp.where(valid, cot.astype(F32), 0.0).astype(BF16).reshape(
            joined, rows, D
        )
        return 0

    lax.fori_loop(0, slots // chunk, mask, 0)
    gather.forward(1)

    step = 256 if width % 256 == 0 else 128

    def w2_grad(i, _):
        cols = pl.ds(pl.multiple_of(i * step, 128), step)
        value = dot(act[:, cols], gv[...].reshape(slots, D), ((0,), (0,)))
        wo[pl.ds(pl.multiple_of(i * step, 128), step), :] = value.astype(BF16)
        return 0

    lax.fori_loop(0, width // step, w2_grad, 0)
    for k in range(2, place.zs):
        gather.forward(k)
    if not aligned:
        for d in range(place.dp):
            g2_split[d] = wo[d * units : (d + 1) * units, :]
    r2 = ScatterDp(place, 1, dp_sems, g2_part, lambda k, d: g2_part(d),
                   lambda j, k: from_x2.at[j, k], lambda k: from_z2.at[k])
    r2.start_x()
    w2_own.wait()
    gather.arrive()
    if not aligned:
        for d in range(place.dp):
            w2[d * units : (d + 1) * units, :] = w2_split[d]

    scatter = ScatterSeq(place, 0, seq_sems, lambda s: ds.at[s], lambda j: from_core.at[j],
                         lambda j: from_y.at[j - 1])
    def backward(i):
        lines = lines_of(i, chunk)
        grad_two = gv[pl.ds(i * joined, joined)].reshape(chunk, D)
        grad_act = dot(grad_two, w2[...], ((1,), (1,)))
        grad_expanded = (grad_act * slope[lines, :].astype(F32)).astype(BF16)
        slope[lines, :] = grad_expanded
        grad_second = dot(grad_expanded, w1[...], ((1,), (1,)))
        ds[pl.ds(i * joined, joined)] = grad_second.astype(BF16).reshape(joined, rows, D)
        sums_ref[3:4] += jnp.sum(grad_second * unit[lines, :].astype(F32), axis=0, keepdims=True)
        sums_ref[4:5] += jnp.sum(grad_second, axis=0, keepdims=True)
        sums_ref[7:8, :width] += jnp.sum(grad_expanded.astype(F32), axis=0, keepdims=True)

    def fold_y(j):
        block = place.at_y(j, place.c)
        scatter.core_copy(j).wait_recv()
        ds[block] = (ds[block].astype(F32) + from_core[j].astype(F32)).astype(BF16)
        scatter.y_copy(j, ds.at[block]).start()

    for j in list(range(1, place.ys)) + [0]:
        if joined == 1:
            backward(place.at_y(j, 1 - place.c))
            scatter.core_copy(j).start()
            backward(place.at_y(j, place.c))
        else:
            backward(lax.rem(place.y + j, place.ys))
            scatter.core_copy(j).start()
        if j:
            fold_y(j)

    gather.drain()

    def emit(i, _):
        lines = lines_of(i, chunk)
        unit[lines, :] = dot(act[lines, :], w2[...]).astype(BF16)
        return 0

    lax.fori_loop(0, slots // chunk, emit, 0)
    keep_parts = [
        pltpu.make_async_copy(
            unit.at[pl.ds(i * rows, rows), :], part_out.at[i], local.at[9 + i]
        )
        for i in range(seq)
    ]
    for copy in keep_parts:
        copy.start()

    r2.fold(r2.order[0])

    def w1_grad(i, _):
        cols = pl.ds(pl.multiple_of(i * 256, 128), 256)
        value = dot(second[:, cols], slope[...], ((0,), (0,)))
        w1[pl.ds(pl.multiple_of(i * 256, 128), 256), :] = value.astype(BF16)
        return 0

    lax.fori_loop(0, D // 256, w1_grad, 0)
    if not aligned:
        for d in range(place.dp):
            g1_split[d] = w1[d * share : (d + 1) * share, :]
    keep = [
        pltpu.make_async_copy(g1_part(d), g1_out.at[d], local.at[9 + seq + d])
        for d in range(place.dp)
    ]
    for copy in keep:
        copy.start()
    for k in r2.order[1:-1]:
        r2.fold(k)
    scatter.core_copy(0).wait_recv()
    value = ds[place.s].astype(F32) + from_core[0].astype(F32)
    for j in range(1, place.ys):
        scatter.y_copy(j, ds.at[place.s]).wait_recv()
        value = value + from_y[j - 1].astype(F32)
    mine = pl.ds(pl.multiple_of(lax.rem(place.s, joined) * rows, 8), rows)
    middle = own[mine, :]
    normal, spread = normalize(middle)
    grad_two = gv[place.s].astype(F32)
    grad_middle = grad_two + norm_backward(normal, spread, value * gain)
    branch = grad_middle.astype(BF16)
    gb[place.s] = branch
    sums_ref[5:6] = jnp.sum(grad_two, axis=0, keepdims=True)
    sums_ref[2:3] = jnp.sum(branch.astype(F32), axis=0, keepdims=True)
    spread_out = GatherSeq(place, 1, seq_sems, gb.at[place.s], lambda s: gb.at[s])
    spread_out.start()
    middle_out[...] = middle
    grad_out[...] = grad_middle

    r2.fold(0)
    for j in range(1, place.ys):
        spread_out.arrive_y(j)
    s2_ref[...] = r2.finish()
    for j in range(place.ys):
        spread_out.arrive_core(j)
    save = pltpu.make_async_copy(gb, gb_out, local.at[8])
    save.start()
    for j in range(place.ys):
        scatter.core_copy(j).wait_send()
    for j in range(1, place.ys):
        scatter.y_copy(j, ds.at[place.s]).wait_send()
    spread_out.drain()
    r2.drain()
    for copy in (*keep_parts, *keep, save):
        copy.wait()


def feed(place, lengths, order, x, mix, cot, wo, w1, w2, vectors):
    seq, rows, _ = x.shape
    slots = seq * rows
    chunk = chunk_of(slots)
    width = w1.shape[1]
    share, units = D // place.dp, width // place.dp
    split = []
    anyspace = pl.BlockSpec(memory_space=pl.ANY)
    inside = pl.BlockSpec(memory_space=pltpu.VMEM)
    vm = lambda *shape: pltpu.VMEM(shape, BF16)
    if not whole_tiles(share, units):
        split = [
            vm(place.dp, units, D), vm(place.dp, units, D), vm(place.dp, share, width),
        ]
    outs = [
        ((seq, rows, D), BF16, anyspace),
        ((rows, D), F32, inside),
        ((rows, D), F32, inside),
        ((seq, rows, D), BF16, anyspace),
        ((place.dp, share, width), BF16, anyspace),
        ((units, D), BF16, inside),
        ((8, D), F32, inside),
    ]
    return pl.pallas_call(
        functools.partial(feed_kernel, place),
        in_specs=[pl.BlockSpec(memory_space=pltpu.SMEM)] * 2 + [anyspace] * 6 + [inside],
        out_specs=[spec for _, _, spec in outs],
        out_shape=[jax.ShapeDtypeStruct(shape, kind) for shape, kind, _ in outs],
        scratch_shapes=[
            vm(seq, rows, D),
            vm(D, slots),
            vm(seq, rows, D),
            vm(D, D),
            vm(D, width),
            vm(width, D),
            vm(slots, D),
            vm(slots, width),
            vm(slots, width),
            vm(slots, D),
            vm(seq, rows, D),
            pltpu.VMEM((chunk, D), F32),
            vm(place.ys, rows, D),
            vm(max(place.ys - 1, 1), rows, D),
            vm(max(place.xs - 1, 1), place.zs, units, D),
            vm(place.zs - 1, units, D),
        ]
        + split
        + dp_semaphores(place, 2)
        + seq_semaphores(place, 3)
        + [pltpu.SemaphoreType.DMA((9 + seq + place.dp,))],
        compiler_params=params(collective_id=1, has_side_effects=True),
        name="feed",
    )(lengths, order, x, mix, cot, wo, w1, w2, vectors)


class SumSmall:
    def __init__(self, place, values, landing, sems):
        self.p, self.values, self.landing = place, values, landing
        self.sends, self.recvs = sems
        self.hops = [
            [((place.d, place.partner))],
            [(place.d, place.at_y(j, place.c)) for j in range(1, place.ys)],
            [(place.at_x(j), place.s) for j in range(1, place.xs)],
            [(place.at_z(k), place.s) for k in range(1, place.zs)],
        ]

    def copies(self, hop):
        first = sum(len(peers) for peers in self.hops[:hop])
        return [
            (first + i, send(self.values.at[hop], self.landing.at[first + i],
                             self.sends.at[first + i], self.recvs.at[first + i], peer))
            for i, peer in enumerate(self.hops[hop])
        ]

    def start(self, hop):
        for _, copy in self.copies(hop):
            copy.start()

    def fold(self, hop):
        value = self.values[hop]
        for i, copy in self.copies(hop):
            copy.wait_recv()
            value = value + self.landing[i]
        return value

    def drain(self):
        for hop in range(4):
            for _, copy in self.copies(hop):
                copy.wait_send()


def small_hops(place):
    return 1 + (place.ys - 1) + (place.xs - 1) + (place.zs - 1)


def tail_kernel(
    place, vec_ref, sums_ref, lse_ref, middle_ref, gmid_ref,
    qt_in, kt_in, k_in, v_in, gb_in, mix_in, wo_in, wq_in, normed_in, x_in, part_in, g1_in, s2_in,
    layer_ref, input_ref, total_ref, w1_out, w2_out, wq_out, wo_out,
    qt, kt, kn, vn, got, gbv, mixv, normed, wq, dqkv, wo_rows, gbs, dk_sum, dv_sum, xbuf, outp,
    core_a, y_a, core_b, y_b, pq, po, p1, xq, xo, x1, zq, zo, z1, r1, rq, ro,
    values, landing, *rest,
):
    zsend, zrecv, xsend, xrecv, ssend, srecv, vsend, vrecv, local = rest[-9:]
    place.locate()
    seq, rows, _ = x_in.shape
    slots = seq * rows
    chunk = chunk_of(slots)
    joined = chunk // rows
    count = slots // chunk
    heads = kt.shape[0]
    wide = heads * HEAD_DIM
    share = D // place.dp
    place.barrier()
    dp_sems, seq_sems = (zsend, zrecv, xsend, xrecv), (ssend, srecv)
    e1 = gbv
    if whole_tiles(share):
        q_part = lambda d: pq.at[pl.ds(pl.multiple_of(d * share, 16), share), :]
        o_part = lambda d: po.at[pl.ds(pl.multiple_of(d * share, 16), share), :]
    else:
        pq_split, po_split = rest[:2]
        q_part, o_part = (lambda d: pq_split.at[d]), (lambda d: po_split.at[d])
    g1 = ScatterDp(place, 0, dp_sems, lambda d: g1_in.at[d], lambda k, d: p1.at[k],
                   lambda j, k: x1.at[j, k], lambda k: z1.at[k])
    gq = ScatterDp(place, 1, dp_sems, q_part, lambda k, d: q_part(d),
                   lambda j, k: xq.at[j, k], lambda k: zq.at[k])
    go = ScatterDp(place, 2, dp_sems, o_part, lambda k, d: o_part(d),
                   lambda j, k: xo.at[j, k], lambda k: zo.at[k])
    out_sum = ScatterSeq(place, 0, seq_sems, lambda s: part_in.at[s], lambda j: core_a.at[j],
                         lambda j: y_a.at[j - 1])
    e1_sum = ScatterSeq(place, 1, seq_sems, lambda s: e1.at[s], lambda j: core_b.at[j],
                        lambda j: y_b.at[j - 1])
    final2 = GatherSeq(place, 2, seq_sems, s2_in, lambda s: w2_out.at[s])
    final1 = GatherSeq(place, 3, seq_sems, r1, lambda s: w1_out.at[s])
    final_o = GatherSeq(place, 4, seq_sems, ro, lambda s: wo_out.at[s])
    final_q = GatherSeq(place, 5, seq_sems, rq, lambda s: wq_out.at[s])

    first = [(gb_in, gbv), (wo_in.at[pl.ds(pl.multiple_of(place.s * wide, 16), wide), :], wo_rows),
             (mix_in, mixv), (qt_in, qt), (kt_in, kt), (k_in, kn), (v_in, vn)]
    later = [(normed_in, normed), (wq_in, wq)]
    later += [(g1_in.at[g1.block(k, 0)], p1.at[k]) for k in range(place.zs)]
    later += [(part_in.at[place.at_y(j, place.c)], outp.at[j]) for j in range(place.ys)]
    loads = [
        pltpu.make_async_copy(src, dst, local.at[i]) for i, (src, dst) in enumerate(first + later)
    ]
    free = len(loads)
    for copy in loads:
        copy.start()
    g1.start_x()
    for j in list(range(1, place.ys)) + [0]:
        out_sum.core_copy(j).start()
    for copy in loads[: len(first)]:
        copy.wait()

    def lines_of(index, size, step=16):
        return pl.ds(pl.multiple_of(index * size, step), size)

    def turn(i, _):
        cols = pl.ds(pl.multiple_of(i * chunk, 128), chunk)
        branch = gbv[pl.ds(i * joined, joined)].reshape(chunk, D)
        got[:, cols] = dot(wo_rows[...], branch, ((1,), (1,))).astype(BF16)
        for s in range(seq):

            @pl.when(place.s == s)
            def _():
                gbs[lines_of(i, chunk), :] = branch[:, s * wide : (s + 1) * wide]

        return 0

    lax.fori_loop(0, count, turn, 0)

    def wo_grad(i, _):
        lines = pl.ds(pl.multiple_of(i * 256, 128), 256)
        po[lines, :] = dot(mixv[lines, :], gbs[...]).astype(BF16)
        return 0

    lax.fori_loop(0, D // 256, wo_grad, 0)
    if not whole_tiles(share):
        for d in range(place.dp):
            po_split[d] = po[d * share : (d + 1) * share, :]
    go.start_x()

    block = 256

    def head_back(head):
        part = slice(head * HEAD_DIM, (head + 1) * HEAD_DIM)
        dk_sum[...] = jnp.zeros_like(dk_sum)
        dv_sum[...] = jnp.zeros_like(dv_sum)

        def one(i, _):
            cols = pl.ds(pl.multiple_of(i * block, 128), block)
            grad = got[part, cols]
            own_rows = pl.ds(pl.multiple_of(place.s * wide + head * HEAD_DIM, 16), HEAD_DIM)
            mixed = mixv[own_rows, cols]
            delta = jnp.sum(grad.astype(F32) * mixed.astype(F32), axis=0, keepdims=True)
            probs = jnp.exp2(dot(kn[head], qt[head, :, cols]) * QSCALE - lse_ref[head, :, cols])
            grad_scores = (probs * (dot(vn[head], grad) - delta)).astype(BF16)
            dv_sum[...] += dot(probs.astype(BF16), grad, ((1,), (1,)))
            dk_sum[...] += dot(grad_scores, qt[head, :HEAD_DIM, cols], ((1,), (1,)))
            turned = dot(kt[head], grad_scores) * SCALE
            dqkv[pl.ds(pl.multiple_of(i * block, 128), block), part] = jnp.transpose(turned).astype(BF16)
            return 0

        lax.fori_loop(0, slots // block, one, 0)
        dqkv[:, wide + head * HEAD_DIM : wide + (head + 1) * HEAD_DIM] = (
            dk_sum[...] * SCALE
        ).astype(BF16)
        dqkv[:, 2 * wide + head * HEAD_DIM : 2 * wide + (head + 1) * HEAD_DIM] = dv_sum[...].astype(
            BF16
        )

    def out_fold():
        for j in range(1, place.ys):
            out_sum.core_copy(j).wait_recv()
            outp[j] = (outp[j].astype(F32) + core_a[j].astype(F32)).astype(BF16)
            out_sum.y_copy(j, outp.at[j]).start()

    def publish(group, result, final):
        result[...] = group.finish()
        final.start()

    for head in range(heads):
        head_back(head)
        if head == 0:
            for copy in loads[len(first) :]:
                copy.wait()
            out_fold()
            final2.start()
            g1.fold(g1.order[0])
        if head == min(1, heads - 1):
            for k in g1.order[1:-1]:
                g1.fold(k)
        if head == heads - 1:
            g1.fold(0)
            go.fold_all()

    def q_grad(i, _):
        cols = pl.ds(pl.multiple_of(i * 256, 128), 256)
        pq[cols, :] = dot(normed[:, cols], dqkv[...], ((0,), (0,))).astype(BF16)
        return 0

    lax.fori_loop(0, D // 256, q_grad, 0)
    if not whole_tiles(share):
        for d in range(place.dp):
            pq_split[d] = pq[d * share : (d + 1) * share, :]
    gq.start_x()
    total = sums_ref[...]
    bias_sum = jnp.sum(dqkv[...].astype(F32), axis=0, keepdims=True)
    values[0] = jnp.zeros_like(values[0])
    values[0, 0:8] = total
    values[0, pl.ds(8 + place.s, 1), :wide] = bias_sum[:, :wide]
    values[0, pl.ds(8 + place.s, 1), wide : 2 * wide] = bias_sum[:, 2 * wide :]
    values[0, pl.ds(8 + seq + place.s, 1), :] = total[7:8]
    values[0, 7:8] = jnp.zeros((1, D), F32)

    order = []
    for j in list(range(1, place.ys)) + [0]:
        if joined == 1:
            order += [(place.at_y(j, 1 - place.c), j, False), (place.at_y(j, place.c), j, True)]
        else:
            order += [(lax.rem(place.y + j, place.ys), j, True)]

    def x_load(at, slot):
        return pltpu.make_async_copy(
            x_in.at[pl.ds(at * joined, joined)], xbuf.at[slot], local.at[free + slot]
        )

    x_load(order[0][0], 0).start()
    for step, (at, j, both) in enumerate(order):
        slot = step % 2
        if step + 1 < len(order):
            x_load(order[step + 1][0], 1 - slot).start()
        x_load(at, slot).wait()
        grad = dot(dqkv[lines_of(at, chunk), :], wq[...].reshape(D, 3 * wide), ((1,), (1,)))
        normal, spread = normalize(xbuf[slot].reshape(chunk, D).astype(F32))
        values[0, 0:1] += jnp.sum(grad * normal, axis=0, keepdims=True)
        values[0, 1:2] += jnp.sum(grad, axis=0, keepdims=True)
        e1[pl.ds(at * joined, joined)] = grad.astype(BF16).reshape(joined, rows, D)
        if joined == 2 or not both:
            e1_sum.core_copy(j).start()
        if both and j:
            target = place.at_y(j, place.c)
            e1_sum.core_copy(j).wait_recv()
            e1[target] = (e1[target].astype(F32) + core_b[j].astype(F32)).astype(BF16)
            e1_sum.y_copy(j, e1.at[target]).start()
    small = SumSmall(place, values, landing, (vsend, vrecv))
    small.start(0)
    gq.fold_all()
    publish(g1, r1, final1)
    publish(go, ro, final_o)
    for hop in range(3):
        values[hop + 1] = small.fold(hop)
        small.start(hop + 1)
    for final in (final2, final1, final_o):
        for j in range(1, place.ys):
            final.arrive_y(j)

    value = outp[0].astype(F32)
    out_sum.core_copy(0).wait_recv()
    value = value + core_a[0].astype(F32)
    for j in range(1, place.ys):
        out_sum.y_copy(j, outp.at[j]).wait_recv()
        value = value + y_a[j - 1].astype(F32)
    layer_ref[...] = (middle_ref[...] + (value + vec_ref[5:6])).astype(BF16)

    value = e1[place.s].astype(F32)
    e1_sum.core_copy(0).wait_recv()
    value = value + core_b[0].astype(F32)
    for j in range(1, place.ys):
        e1_sum.y_copy(j, e1.at[place.s]).wait_recv()
        value = value + y_b[j - 1].astype(F32)
    last = (len(order) - 1) % 2
    hidden = xbuf[last, lax.rem(place.s, joined)].astype(F32)
    normal, spread = normalize(hidden)
    input_ref[...] = (gmid_ref[...] + norm_backward(normal, spread, value * vec_ref[0:1])).astype(
        BF16
    )
    total_ref[...] = small.fold(3)
    publish(gq, rq, final_q)
    keep = [
        pltpu.make_async_copy(src, dst.at[place.s], local.at[free + 2 + i])
        for i, (src, dst) in enumerate([(r1, w1_out), (s2_in, w2_out), (rq, wq_out), (ro, wo_out)])
    ]
    for copy in keep:
        copy.start()
    for final in (final2, final1, final_o):
        for j in range(place.ys):
            final.arrive_core(j)
    for j in range(1, place.ys):
        final_q.arrive_y(j)
    for j in range(place.ys):
        final_q.arrive_core(j)
    for final in (final1, final2, final_o, final_q):
        final.drain()
    for group in (out_sum, e1_sum):
        for j in range(place.ys):
            group.core_copy(j).wait_send()
        for j in range(1, place.ys):
            group.y_copy(j, outp.at[j]).wait_send()
    for group in (g1, gq, go):
        group.drain()
    small.drain()
    for copy in keep:
        copy.wait()


def tail(place, vectors, sums, lse, middle, gmid, qt, kt, kn, vn, gb, mix, wo, wq, normed, x, part, g1, s2):
    seq, rows, _ = x.shape
    slots = seq * rows
    chunk = chunk_of(slots)
    joined = chunk // rows
    heads = kt.shape[0]
    wide = heads * HEAD_DIM
    share = D // place.dp
    width, units = g1.shape[2], s2.shape[0]
    ys, xs, zs = place.ys, max(place.xs - 1, 1), place.zs
    anyspace = pl.BlockSpec(memory_space=pl.ANY)
    inside = pl.BlockSpec(memory_space=pltpu.VMEM)
    vm = lambda *shape: pltpu.VMEM(shape, BF16)
    tall = 8 + 2 * seq
    hops = small_hops(place)
    outs = [
        ((rows, D), BF16, inside),
        ((rows, D), BF16, inside),
        ((tall, D), F32, inside),
        ((seq, share, width), BF16, anyspace),
        ((seq, units, D), BF16, anyspace),
        ((seq, share, 3 * wide), BF16, anyspace),
        ((seq, share, wide), BF16, anyspace),
    ]
    split = []
    if not whole_tiles(share):
        split = [vm(place.dp, share, 3 * wide), vm(place.dp, share, wide)]
    return pl.pallas_call(
        functools.partial(tail_kernel, place),
        in_specs=[inside] * 5 + [anyspace] * 13,
        out_specs=[spec for _, _, spec in outs],
        out_shape=[jax.ShapeDtypeStruct(shape, kind) for shape, kind, _ in outs],
        scratch_shapes=[
            vm(heads, 128, slots),
            vm(heads, HEAD_DIM, slots),
            vm(heads, slots, 128),
            vm(heads, slots, HEAD_DIM),
            vm(wide, slots),
            vm(seq, rows, D),
            vm(D, slots),
            vm(slots, D),
            vm(place.dp, share, 3 * wide),
            vm(slots, 3 * wide),
            vm(wide, D),
            vm(slots, wide),
            pltpu.VMEM((slots, HEAD_DIM), F32),
            pltpu.VMEM((slots, HEAD_DIM), F32),
            vm(2, joined, rows, D),
            vm(ys, rows, D),
            vm(ys, rows, D),
            vm(max(ys - 1, 1), rows, D),
            vm(ys, rows, D),
            vm(max(ys - 1, 1), rows, D),
            vm(D, 3 * wide),
            vm(D, wide),
            vm(zs, share, width),
            vm(xs, zs, share, 3 * wide),
            vm(xs, zs, share, wide),
            vm(xs, zs, share, width),
            vm(zs - 1, share, 3 * wide),
            vm(zs - 1, share, wide),
            vm(zs - 1, share, width),
            vm(share, width),
            vm(share, 3 * wide),
            vm(share, wide),
            pltpu.VMEM((4, tall, D), F32),
            pltpu.VMEM((hops, tall, D), F32),
        ]
        + split
        + dp_semaphores(place, 3)
        + seq_semaphores(place, 6)
        + [
            pltpu.SemaphoreType.DMA((hops,)),
            pltpu.SemaphoreType.DMA((hops,)),
            pltpu.SemaphoreType.DMA((24 + ys + zs,)),
        ],
        compiler_params=params(collective_id=2, has_side_effects=True),
        name="tail",
    )(vectors, sums, lse, middle, gmid, qt, kt, kn, vn, gb, mix, wo, wq, normed, x, part, g1, s2)


def prep_kernel(place, q_ref, k_ref, v_ref, w1_ref, vec_ref, b1_ref, small_ref, wqkv_ref, w1_out):
    place.locate()
    dp, seq = place.dp, place.seq
    share = D // dp
    wide = D // seq
    units = FF // (dp * seq)
    small_ref[...] = jnp.zeros_like(small_ref)
    for s in range(seq):

        @pl.when(place.s == s)
        def _():
            for i, ref in enumerate((q_ref, k_ref, v_ref)):
                wqkv_ref[:, i * wide : (i + 1) * wide] = ref[:, s * wide : (s + 1) * wide]
            for d in range(dp):
                first = d * (FF // dp) + s * units
                w1_out[:, d * units : (d + 1) * units] = w1_ref[:, first : first + units]

    vec = vec_ref[...]
    for d in range(dp):
        home = (d * share) // wide
        first = d * share - home * wide

        @pl.when(place.d == d)
        def _():
            small_ref[0:6, d * share : (d + 1) * share] = vec[0:6]
            small_ref[6:7, d * units : (d + 1) * units] = b1_ref[pl.ds(place.s, 1), :]

            @pl.when(place.s == home)
            def _():
                small_ref[8:10, first : first + share] = vec[6:8]


def prep(place, q, k, v, w1, vectors, b1):
    wide = D // place.seq
    share = q.shape[0]
    inside = pl.BlockSpec(memory_space=pltpu.VMEM)
    return pl.pallas_call(
        functools.partial(prep_kernel, place),
        in_specs=[inside] * 6,
        out_specs=[inside] * 3,
        out_shape=[
            jax.ShapeDtypeStruct((16, D), F32),
            jax.ShapeDtypeStruct((share, 3 * wide), BF16),
            jax.ShapeDtypeStruct((share, FF // place.seq), BF16),
        ],
        compiler_params=params(),
        name="prep",
    )(q, k, v, w1, vectors, b1)


def finish_kernel(
    place, w1_ref, w2_ref, wq_ref, wo_ref, total_ref, layer_ref, input_ref,
    layer_out, input_out, w1_out, w2_out, q_out, k_out, v_out, wo_out, g1_out, s1_out, bo_out, g2_out, s2_out, b2_out,
    bq_out, bv_out, b1_out, lines,
):
    place.locate()
    dp, seq = place.dp, place.seq
    share = D // dp
    wide = D // seq
    units = FF // (dp * seq)
    w2_out[...] = w2_ref[...].astype(F32)
    for s in range(seq):
        cols = slice(s * wide, (s + 1) * wide)
        for i, out in enumerate((q_out, k_out, v_out)):
            out[:, cols] = wq_ref[s, :, i * wide : (i + 1) * wide].astype(F32)
        wo_out[:, cols] = wo_ref[s].astype(F32)
        for d in range(dp):
            first = d * (FF // dp) + s * units
            w1_out[:, first : first + units] = w1_ref[s, :, d * units : (d + 1) * units].astype(F32)

    @pl.when(pl.program_id(0) == 0)
    def _():
        layer_out[...] = layer_ref[...]
        input_out[...] = input_ref[...]
        lines[...] = total_ref[0:8]
        for s in range(seq):
            cols = slice(s * wide, (s + 1) * wide)
            lines[6:7, cols] = total_ref[8 + s : 9 + s, :wide]
            lines[7:8, cols] = total_ref[8 + s : 9 + s, wide : 2 * wide]
        outs = (g1_out, s1_out, bo_out, g2_out, s2_out, b2_out, bq_out, bv_out)
        for d in range(dp):

            @pl.when(place.d == d)
            def _():
                for i, out in enumerate(outs):
                    out[...] = lines[i : i + 1, d * share : (d + 1) * share]
                for s in range(seq):
                    row = 8 + seq + s
                    b1_out[:, s * units : (s + 1) * units] = total_ref[
                        row : row + 1, d * units : (d + 1) * units
                    ]


def finish(place, w1, w2, wq, wo, totals, layer, grad):
    dp, seq = place.dp, place.seq
    share, units, wide = D // dp, w2.shape[1], D // seq
    tile = 32 if share % 32 == 0 and units == share else share
    steps = share // tile
    tall = units // steps
    mat = lambda *tail: pl.BlockSpec((seq, tile, *tail), lambda i: (0, i, 0))
    out = lambda cols: pl.BlockSpec((tile, cols), lambda i: (i, 0))
    small = pl.BlockSpec((1, share), lambda i: (0, 0))
    f32 = lambda *shape: jax.ShapeDtypeStruct(shape, F32)
    return pl.pallas_call(
        functools.partial(finish_kernel, place),
        grid=(steps,),
        in_specs=[
            mat(w1.shape[2]),
            pl.BlockSpec((seq, tall, D), lambda i: (0, i, 0)),
            mat(wq.shape[2]),
            mat(wo.shape[2]),
            pl.BlockSpec(totals.shape, lambda i: (0, 0)),
            pl.BlockSpec(layer.shape, lambda i: (0, 0)),
            pl.BlockSpec(layer.shape, lambda i: (0, 0)),
        ],
        out_specs=[pl.BlockSpec(layer.shape, lambda i: (0, 0))] * 2
        + [out(FF), pl.BlockSpec((seq, tall, D), lambda i: (0, i, 0))]
        + [out(D)] * 4
        + [small] * 8
        + [pl.BlockSpec((1, FF // dp), lambda i: (0, 0))],
        out_shape=[jax.ShapeDtypeStruct(layer.shape, BF16)] * 2
        + [f32(share, FF), f32(seq, units, D)]
        + [f32(share, D)] * 4
        + [f32(1, share)] * 8
        + [f32(1, FF // dp)],
        scratch_shapes=[pltpu.VMEM((8, D), F32)],
        compiler_params=params(),
        name="finish",
    )(w1, w2, wq, wo, totals, layer, grad)


def per_device(
    hidden_in, cotangent, clip_lengths, clip_order, first_gain, first_shift, query_weight,
    query_bias, key_weight, value_weight, value_bias, output_weight, output_bias, second_gain,
    second_shift, expand_weight, expand_bias, reduce_weight, reduce_bias,
):
    dp = lax.axis_size("dp")
    seq = lax.axis_size("seq")
    me = lax.axis_index("seq")
    slots = hidden_in.shape[1] * seq
    units = FF // (dp * seq)
    quarter = dp * units

    spot = Place(dp, seq)
    vectors = jnp.stack(
        [first_gain, first_shift, output_bias, second_gain, second_shift, reduce_bias, query_bias,
         value_bias]
    ).astype(F32)
    b1 = expand_bias.reshape(seq, units).astype(F32)
    small, wqkv_share, w1_share = prep(
        spot, query_weight, key_weight, value_weight, expand_weight, vectors, b1
    )
    x, vectors, w_qkv, w_out, w_expand, normed, qt, kt, keys, values, mix, lse = front(
        spot, clip_lengths, clip_order, hidden_in[0], small, wqkv_share, output_weight, w1_share
    )
    w_out = w_out.reshape(D, D)
    w_expand = w_expand.reshape(D, quarter)
    mix = mix.reshape(D, slots)
    if not whole_tiles(units):
        reduce_weight = lax.dynamic_slice_in_dim(reduce_weight, me * units, units, 0)
    grad_branch, middle, grad_middle, out_part, g1, s2, sums = feed(
        spot, clip_lengths, clip_order, x, mix, cotangent[0], w_out, w_expand, reduce_weight,
        vectors,
    )
    layer_output, input_grad, totals, w1_grad, w2_grad, qkv_grad, wo_grad = tail(
        spot, vectors, sums, lse, middle, grad_middle, qt, kt, keys, values, grad_branch, mix,
        w_out, w_qkv, normed, x, out_part, g1, s2,
    )
    results = finish(
        spot, w1_grad, w2_grad, qkv_grad, wo_grad, totals, layer_output, input_grad
    )
    layer_output, input_grad, *results = results
    (w1_grad, w2_grad, wq_grad, wk_grad, wv_grad, wo_grad) = results[:6]
    g1, s1, bo, g2, s2, b2, bq, bv, b1 = (value.reshape(-1) for value in results[6:])
    return (
        layer_output[None], input_grad[None], g1, s1, wq_grad, bq, wk_grad, wv_grad, bv, wo_grad,
        bo, g2, s2, w1_grad, b1, w2_grad.reshape(FF // dp, D), b2,
    )


def solution(mesh):
    clip = P("dp", "seq", None)
    vec = P("dp")
    mat = P("dp", None)
    return jax.shard_map(
        per_device,
        mesh=mesh,
        in_specs=(
            clip, clip, P(), vec, vec, vec, mat, vec, mat, mat, vec, mat, vec, vec, vec, mat, vec,
            mat, vec,
        ),
        out_specs=(
            clip, clip, vec, vec, mat, vec, mat, mat, vec, mat, vec, vec, vec, mat, vec, mat, vec,
        ),
        check_vma=False,
    )
```

```python
import functools

import jax
import jax.numpy as jnp
from jax import lax
from jax.experimental import pallas as pl
from jax.experimental.pallas import tpu as pltpu
from jax.sharding import PartitionSpec as P

D = 1280
FF = 5120
HEADS = 16
HEAD_DIM = D // HEADS
EPSILON = 1e-05
SCALE = HEAD_DIM ** (-0.5)
F32 = jnp.float32
BF16 = jnp.bfloat16
VMEM_LIMIT = 66_000_000
MESH = pl.DeviceIdType.MESH


def dot(left, right, contract=((1,), (0,))):
    return lax.dot_general(left, right, (contract, ((), ())), preferred_element_type=F32)


def normalize(values):
    average = jnp.mean(values, axis=-1, keepdims=True)
    centered = values - average
    variance = jnp.mean(centered * centered, axis=-1, keepdims=True)
    spread = lax.rsqrt(variance + EPSILON)
    return centered * spread, spread


def norm_backward(unit, spread, grad_unit):
    inner = jnp.mean(grad_unit * unit, axis=-1, keepdims=True)
    return spread * (grad_unit - jnp.mean(grad_unit, axis=-1, keepdims=True) - unit * inner)


def params(**extra):
    return pltpu.CompilerParams(vmem_limit_bytes=VMEM_LIMIT, **extra)


def whole(shape):
    return pl.BlockSpec(shape, lambda *_: (0,) * len(shape), pipeline_mode=pl.Buffered(1))


def chunk_of(slots):
    return slots // 4 if slots % 512 == 0 else slots


class Place:
    def __init__(self, dp, seq):
        self.dp, self.seq = dp, seq
        self.xs = 1 << ((dp.bit_length() - 1) // 2)
        self.zs = dp // self.xs
        self.ys = seq // 2
        self.z_order = sorted(range(1, self.zs), key=lambda k: min(k, self.zs - k))

    def locate(self):
        self.d, self.s = lax.axis_index("dp"), lax.axis_index("seq")
        self.z, self.x = self.d // self.xs, lax.rem(self.d, self.xs)
        self.y, self.c = self.s // 2, lax.rem(self.s, 2)
        self.partner = self.y * 2 + 1 - self.c

    def at_z(self, k):
        return lax.rem(self.z + k + self.zs, self.zs) * self.xs + self.x

    def block(self, k, j):
        return lax.rem(self.z - k + self.zs, self.zs) * self.xs + lax.rem(
            self.x - j + self.xs, self.xs
        )

    def at_x(self, j):
        return self.z * self.xs + lax.rem(self.x + j, self.xs)

    def at_y(self, j, core):
        return lax.rem(self.y + j + self.ys, self.ys) * 2 + core

    def peers(self, over_dp=True, over_seq=True):
        found = []
        if over_dp:
            found += [(self.at_z(k), self.s) for k in range(1, self.zs)]
            found += [(self.at_x(j), self.s) for j in range(1, self.xs)]
        if over_seq:
            found += [(self.d, self.partner)]
            found += [(self.d, self.at_y(j, self.c)) for j in range(1, self.ys)]
        return found

    def barrier(self, **which):
        semaphore = pltpu.get_barrier_semaphore()
        peers = self.peers(**which)
        for peer in peers:
            pl.semaphore_signal(semaphore, inc=1, device_id=peer, device_id_type=MESH)
        pl.semaphore_wait(semaphore, len(peers))


def send(src, dst, send_sem, recv_sem, device):
    return pltpu.make_async_remote_copy(
        src_ref=src, dst_ref=dst, send_sem=send_sem, recv_sem=recv_sem, device_id=device,
        device_id_type=MESH,
    )


def dp_semaphores(place, groups):
    return [
        pltpu.SemaphoreType.DMA((groups, place.zs)),
        pltpu.SemaphoreType.DMA((groups, place.zs)),
        pltpu.SemaphoreType.DMA((groups, place.zs, place.xs)),
        pltpu.SemaphoreType.DMA((groups, place.zs, place.xs)),
    ]


def seq_semaphores(place, groups):
    return [pltpu.SemaphoreType.DMA((groups, 2, place.ys))] * 2


class GatherDp:
    def __init__(self, place, group, sems, own, slab, on=None, ahead=()):
        self.p, self.g, self.own, self.slab, self.on = place, group, own, slab, on
        self.staged = on is None
        self.ahead = dict(zip(place.z_order, ahead))
        self.rest = place.z_order[len(self.ahead) :]
        self.zsend, self.zrecv, self.xsend, self.xrecv = sems

    def when(self, block, act):
        if self.on is None:
            act()
        else:
            pl.when(self.on(block))(act)

    def z_copy(self, k):
        return send(self.own, self.slab(self.p.d), self.zsend.at[self.g, k],
                    self.zrecv.at[self.g, k], (self.p.at_z(k), self.p.s))

    def x_copy(self, k, j):
        block = self.p.block(k, 0)
        src = self.own if k == 0 else self.ahead.get(k, self.slab(block))
        return send(src, self.slab(block), self.xsend.at[self.g, k, j],
                    self.xrecv.at[self.g, k, j], (self.p.at_x(j), self.p.s))

    def start_x(self):
        def act():
            for k in [0, *self.ahead]:
                for j in range(1, self.p.xs):
                    self.x_copy(k, j).start()

        self.when(self.p.d, act)

    def start_z(self):
        def act():
            for k in self.rest[:2] if self.staged else self.rest:
                self.z_copy(k).start()

        self.when(self.p.d, act)

    def forward(self, k):
        place = self.p

        def act():
            send(self.own, self.slab(place.block(k, 0)), self.zsend.at[self.g, k],
                 self.zrecv.at[self.g, k], (place.at_z(k), place.s)).wait_recv()
            for j in range(1, place.xs):
                self.x_copy(k, j).start()
            later = self.rest.index(k) + 2
            if self.staged and later < len(self.rest):
                self.z_copy(self.rest[later]).start()

        self.when(place.block(k, 0), act)

    def forward_all(self):
        for k in self.p.z_order:
            self.forward(k)

    def arrive(self):
        place = self.p
        for k in range(place.zs):
            for j in range(1, place.xs):
                wait = send(self.own, self.slab(place.block(k, j)), self.xsend.at[self.g, k, j],
                            self.xrecv.at[self.g, k, j], (place.at_x(j), place.s)).wait_recv
                self.when(place.block(k, j), wait)

    def drain(self):
        place = self.p

        def act():
            for k in self.rest:
                self.z_copy(k).wait_send()

        self.when(place.d, act)
        for k in range(place.zs):
            for j in range(1, place.xs):
                self.when(place.block(k, 0), self.x_copy(k, j).wait_send)


class GatherSeq:
    def __init__(self, place, group, sems, own, slab):
        self.p, self.g, self.own, self.slab = place, group, own, slab
        self.sends, self.recvs = sems

    def y_copy(self, j):
        place = self.p
        return send(self.own, self.slab(place.s), self.sends.at[self.g, 0, j],
                    self.recvs.at[self.g, 0, j], (place.d, place.at_y(j, place.c)))

    def core_copy(self, j):
        place = self.p
        block = place.at_y(-j, place.c)
        src = self.own if j == 0 else self.slab(block)
        return send(src, self.slab(block), self.sends.at[self.g, 1, j],
                    self.recvs.at[self.g, 1, j], (place.d, place.partner))

    def start(self):
        for j in range(1, self.p.ys):
            self.y_copy(j).start()
        self.core_copy(0).start()

    def arrive_y(self, j):
        place = self.p
        block = place.at_y(-j, place.c)
        send(self.own, self.slab(block), self.sends.at[self.g, 0, j], self.recvs.at[self.g, 0, j],
             (place.d, place.at_y(j, place.c))).wait_recv()
        self.core_copy(j).start()
        return block

    def arrive_core(self, j):
        place = self.p
        block = place.at_y(-j, 1 - place.c)
        send(self.own, self.slab(block), self.sends.at[self.g, 1, j], self.recvs.at[self.g, 1, j],
             (place.d, place.partner)).wait_recv()
        return block

    def drain(self):
        for j in range(1, self.p.ys):
            self.y_copy(j).wait_send()
        for j in range(self.p.ys):
            self.core_copy(j).wait_send()


LOG2E = 1.4426950408889634
QSCALE = SCALE * LOG2E


def own_rows(place, w2):
    units = FF // (place.dp * place.seq)
    if whole_tiles(units):
        return w2.at[pl.ds(pl.multiple_of(place.s * units, 16), units), :]
    return w2


def own_length(lengths_ref, order_ref):
    length = 0
    for clip in range(lengths_ref.shape[0]):
        length = length + jnp.where(order_ref[0] == clip, lengths_ref[clip], 0)
    return length


def front_kernel(
    place, lengths_ref, order_ref, x_in, sm_in, wq_in, wo_in, w1_in, w2_in,
    x_out, vec_out, wq_out, wo_out, w1_out, w2_out, normed_out, qt_out, kt_out, k_out,
    v_out, mix_out, lse_ref,
    xs, nr, nt, biases, sm, wq, wt, qt, kt, vt, kn, vn, mix,
    zsend, zrecv, xsend, xrecv, ssend, srecv, swap_send, swap_recv, local,
):
    place.locate()
    seq, rows = x_out.shape[0], x_out.shape[1]
    slots = seq * rows
    heads = k_out.shape[0]
    wide = heads * HEAD_DIM
    place.barrier()
    dp_sems = (zsend, zrecv, xsend, xrecv)
    seq_sems = (ssend, srecv)

    def over_dp(group, own, buffer):
        return GatherDp(place, group, dp_sems, own, lambda d: buffer.at[d])

    def over_seq(group, own, buffer):
        return GatherSeq(place, group, seq_sems, own, lambda s: buffer.at[s])

    g_sm = over_dp(0, sm_in, sm)
    g_wq = over_dp(1, wq_in, wq)
    g_wo = GatherDp(place, 2, dp_sems, wo_in, lambda d: wo_out.at[d],
                    lambda d: lax.rem(d, 2) == place.c)
    g_w1 = over_dp(3, w1_in, w1_out)
    g_x = over_seq(0, x_in, xs)

    swaps = [(k, j) for k in range(place.zs) for j in range(place.xs) if (k, j) != (0, 0)]

    def swap(k, j):
        slab = wo_out.at[place.block(k, j)]
        return send(slab, slab, swap_send.at[k, j], swap_recv.at[k, j], (place.d, place.partner))

    def swap_start():
        for k, j in swaps:
            pl.when(g_wo.on(place.block(k, j)))(swap(k, j).start)

    def swap_finish():
        for k, j in swaps:
            pl.when(g_wo.on(place.block(k, j)))(swap(k, j).wait_send)
            pl.when(~g_wo.on(place.block(k, j)))(swap(k, j).wait_recv)

    locals_in = [
        pltpu.make_async_copy(x_in, xs.at[place.s], local.at[0]),
        pltpu.make_async_copy(sm_in, sm.at[place.d], local.at[1]),
        pltpu.make_async_copy(wq_in, wq.at[place.d], local.at[2]),
    ]
    w1_own = pltpu.make_async_copy(w1_in, w1_out.at[place.d], local.at[5])
    wo_own = pltpu.make_async_copy(wo_in, wo_out.at[place.d], local.at[4])
    for copy in locals_in:
        copy.start()
    g_sm.start_x()
    g_sm.start_z()
    g_x.start()
    g_wq.start_x()
    g_wq.start_z()
    w1_own.start()
    wo_own.start()

    column = lax.broadcasted_iota(jnp.int32, (slots, 1), 0)
    penalty = jnp.where(column >= own_length(lengths_ref, order_ref), -1e30, 0.0).astype(BF16)
    ones_row = jnp.where(
        lax.broadcasted_iota(jnp.int32, (128 - HEAD_DIM, slots), 0) == 0, 1.0, 0.0
    ).astype(BF16)
    for head in range(heads):
        kn[head] = jnp.zeros((slots, 128), BF16)
        kn[head, :, HEAD_DIM : HEAD_DIM + 1] = penalty
        qt[head, HEAD_DIM:, :] = ones_row

    for copy in locals_in:
        copy.wait()
    turns = list(place.z_order)
    g_sm.forward(turns[0])
    for k in turns[1:2]:
        g_sm.forward(k)
    g_wq.forward(turns[0])
    for k in turns[2:]:
        g_sm.forward(k)
    turns.pop(0)
    if turns:
        g_wq.forward(turns.pop(0))
    g_sm.arrive()
    part, units = sm.shape[2], w1_in.shape[1] // place.dp
    vec_out[...] = jnp.zeros_like(vec_out)
    for d in range(place.dp):
        vec_out[0:6, d * part : (d + 1) * part] = sm[d, 0:6, :]
        vec_out[7:9, d * part : (d + 1) * part] = sm[d, 7:9, :]
        vec_out[6:7, d * units : (d + 1) * units] = sm[d, 6:7, :units]
    for s in range(seq):

        @pl.when(place.s == s)
        def _():
            biases[0:2] = vec_out[7:9, s * wide : (s + 1) * wide]

    gain, shift = vec_out[0:1], vec_out[1:2]

    def norm_block(block):
        unit, _ = normalize(xs[block].astype(F32))
        lines = pl.ds(pl.multiple_of(block * rows, 16), rows)
        nr[lines, :] = (unit * gain + shift).astype(BF16)

    norm_block(place.s)
    norm_block(g_x.arrive_core(0))
    for j in range(1, place.ys):
        if turns:
            g_wq.forward(turns.pop(0))
        norm_block(g_x.arrive_y(j))
    for k in turns:
        g_wq.forward(k)
    g_wo.start_z()
    for j in range(1, place.ys):
        norm_block(g_x.arrive_core(j))
    chunk = chunk_of(slots)

    def turn_block(block, _):
        spot = pl.ds(pl.multiple_of(block * chunk, 128), chunk)
        nt[:, spot] = jnp.transpose(nr[spot, :])
        return 0

    lax.fori_loop(0, slots // chunk, turn_block, 0)
    g_wq.arrive()
    g_wo.start_x()
    share = wq.shape[1]
    wt[...] = jnp.transpose(wq[...].reshape(place.dp * share, 3 * wide))
    bias = jnp.transpose(biases[...])
    g_wo.forward_all()
    g_w1.start_z()
    g_w1.start_x()

    def project_block(block, _):
        cols = pl.ds(pl.multiple_of(block * chunk, 128), chunk)
        tokens = dot(wt[...], nt[:, cols])
        for head in range(heads):
            first = 3 * head * HEAD_DIM
            part = slice(head * HEAD_DIM, (head + 1) * HEAD_DIM)
            query = tokens[first : first + HEAD_DIM] + bias[part, 0:1]
            key = tokens[first + HEAD_DIM : first + 2 * HEAD_DIM].astype(BF16)
            value = tokens[first + 2 * HEAD_DIM : first + 3 * HEAD_DIM] + bias[part, 1:2]
            value = value.astype(BF16)
            qt[head, :HEAD_DIM, cols] = query.astype(BF16)
            kt[head, :, cols] = key
            vt[head, :, cols] = value
            kn[head, cols, :HEAD_DIM] = jnp.transpose(key)
            vn[head, cols, :] = jnp.transpose(value)
        return 0

    lax.fori_loop(0, slots // chunk, project_block, 0)
    results = [
        pltpu.make_async_copy(src, dst, local.at[7 + i])
        for i, (src, dst) in enumerate(
            [(xs, x_out), (wq, wq_out), (nt, normed_out), (qt, qt_out), (kt, kt_out),
             (kn, k_out), (vn, v_out)]
        )
    ]
    for copy in results:
        copy.start()

    block = 256

    def attend(head):
        def one(i, _):
            if head == min(1, heads - 1):

                @pl.when(i == slots // block // 2)
                def _():
                    g_w1.forward(place.z_order[0])

            cols = pl.ds(pl.multiple_of(i * block, 128), block)
            scores = dot(kn[head], qt[head, :, cols])
            top = jnp.max(scores, axis=0, keepdims=True)
            exponent = jnp.exp2((scores - top) * QSCALE)
            total = jnp.sum(exponent, axis=0, keepdims=True)
            mixed = dot(vt[head], exponent.astype(BF16)) / total
            mix[place.s, head, :, cols] = mixed.astype(BF16)
            lse_ref[head, :, cols] = top * QSCALE + jnp.log2(total)
            return 0

        lax.fori_loop(0, slots // block, one, 0)

    g_mix = [
        GatherSeq(place, 1 + head, seq_sems, mix.at[place.s, head],
                  lambda s, head=head: mix.at[s, head])
        for head in range(heads)
    ]
    for head in range(heads):
        attend(head)
        g_mix[head].start()
        if head == min(1, heads - 1):
            g_wo.arrive()
            swap_start()
            g_w1.forward(place.z_order[1])
    for k in place.z_order[2:]:
        g_w1.forward(k)
    w2_own = own_rows(place, w2_in)
    w2_ahead = [
        send(w2_own, w2_out.at[i], zsend.at[4, k], zrecv.at[4, k], (place.at_z(k), place.s))
        for i, k in enumerate(place.z_order[:2])
    ]
    for copy in w2_ahead:
        copy.start()
    for head in range(heads):
        for j in range(1, place.ys):
            g_mix[head].arrive_y(j)
    for head in range(heads):
        for j in range(place.ys):
            g_mix[head].arrive_core(j)
    mix_copy = pltpu.make_async_copy(mix, mix_out, local.at[15])
    mix_copy.start()
    g_w1.arrive()
    swap_finish()
    for group in (g_sm, g_wq, g_wo, g_w1, g_x, *g_mix):
        group.drain()
    for copy in (*w2_ahead, w1_own, wo_own, *results, mix_copy):
        copy.wait()


def front(place, lengths, order, x, small, wqkv, wo, w1, w2):
    dp, seq = place.dp, place.seq
    rows = x.shape[0]
    slots = rows * seq
    heads = HEADS // seq
    share, width = wqkv.shape
    anyspace = pl.BlockSpec(memory_space=pl.ANY)
    shapes = [
        (seq, rows, D),
        (16, D),
        (dp, share, width),
        (dp, *wo.shape),
        (dp, *w1.shape),
        (len(place.z_order[:2]), FF // (dp * seq), D),
        (D, slots),
        (heads, 128, slots),
        (heads, HEAD_DIM, slots),
        (heads, slots, 128),
        (heads, slots, HEAD_DIM),
        (seq, heads, HEAD_DIM, slots),
    ]
    vm = lambda *shape: pltpu.VMEM(shape, BF16)
    return pl.pallas_call(
        functools.partial(front_kernel, place),
        in_specs=[pl.BlockSpec(memory_space=pltpu.SMEM)] * 2 + [anyspace] * 6,
        out_specs=[anyspace, pl.BlockSpec(memory_space=pltpu.VMEM)]
        + [anyspace] * (len(shapes) - 2)
        + [pl.BlockSpec(memory_space=pltpu.VMEM)],
        out_shape=[
            jax.ShapeDtypeStruct(shape, F32 if i == 1 else BF16) for i, shape in enumerate(shapes)
        ]
        + [jax.ShapeDtypeStruct((heads, 1, slots), F32)],
        scratch_shapes=[
            vm(seq, rows, D),
            vm(slots, D),
            vm(D, slots),
            pltpu.VMEM((8, heads * HEAD_DIM), F32),
            pltpu.VMEM((dp, *small.shape), F32),
            vm(dp, share, width),
            vm(width, D),
            vm(heads, 128, slots),
            vm(heads, HEAD_DIM, slots),
            vm(heads, HEAD_DIM, slots),
            vm(heads, slots, 128),
            vm(heads, slots, HEAD_DIM),
            vm(seq, heads, HEAD_DIM, slots),
        ]
        + dp_semaphores(place, 5)
        + seq_semaphores(place, 1 + heads)
        + [pltpu.SemaphoreType.DMA((place.zs, place.xs))] * 2
        + [pltpu.SemaphoreType.DMA((16,))],
        compiler_params=params(collective_id=0, has_side_effects=True),
        name="front",
    )(lengths, order, x, small, wqkv, wo, w1, w2)


class ScatterSeq:
    def __init__(self, place, group, sems, part, from_core, from_y):
        self.p, self.g, self.part, self.from_core, self.from_y = place, group, part, from_core, from_y
        self.sends, self.recvs = sems

    def core_copy(self, j):
        place = self.p
        return send(self.part(place.at_y(j, 1 - place.c)), self.from_core(j),
                    self.sends.at[self.g, 1, j], self.recvs.at[self.g, 1, j],
                    (place.d, place.partner))

    def y_copy(self, j, src):
        place = self.p
        return send(src, self.from_y(j), self.sends.at[self.g, 0, j], self.recvs.at[self.g, 0, j],
                    (place.d, place.at_y(j, place.c)))


class ScatterDp:
    def __init__(self, place, group, sems, out, part, from_x, from_z):
        self.p, self.g, self.out, self.part = place, group, out, part
        self.from_x, self.from_z = from_x, from_z
        self.zsend, self.zrecv, self.xsend, self.xrecv = sems
        self.order = place.z_order + [0]

    def block(self, k, j):
        place = self.p
        return lax.rem(place.z + k, place.zs) * place.xs + lax.rem(place.x + j, place.xs)

    def x_copy(self, j, k):
        return send(self.out(k, j, self.block(k, j)), self.from_x(j - 1, k),
                    self.xsend.at[self.g, k, j], self.xrecv.at[self.g, k, j],
                    (self.p.at_x(j), self.p.s))

    def start_x(self, steps=None):
        for k in self.order if steps is None else steps:
            for j in range(1, self.p.xs):
                self.x_copy(j, k).start()

    def z_copy(self, k):
        return send(self.part(k, self.block(k, 0)), self.from_z(k - 1),
                    self.zsend.at[self.g, k], self.zrecv.at[self.g, k], (self.p.at_z(k), self.p.s))

    def fold_x(self, k):
        own = self.part(k, self.block(k, 0))
        value = own[...].astype(F32)
        for j in range(1, self.p.xs):
            self.x_copy(j, k).wait_recv()
            value = value + self.from_x(j - 1, k)[...].astype(F32)
        own[...] = value.astype(own.dtype)

    def fold(self, k):
        self.fold_x(k)
        if k:
            self.z_copy(k).start()

    def fold_all(self):
        for k in self.order:
            self.fold(k)

    def finish(self):
        value = self.part(0, self.block(0, 0))[...].astype(F32)
        for k in range(1, self.p.zs):
            self.z_copy(k).wait_recv()
            value = value + self.from_z(k - 1)[...].astype(F32)
        return value.astype(self.part(0, self.block(0, 0)).dtype)

    def drain_x(self, steps=None):
        for k in self.order if steps is None else steps:
            for j in range(1, self.p.xs):
                self.x_copy(j, k).wait_send()

    def drain_z(self):
        for k in self.p.z_order:
            self.z_copy(k).wait_send()

    def drain(self):
        self.drain_x()
        self.drain_z()


def split_steps(place):
    order = place.z_order + [0]
    return order[: place.zs // 2], order[place.zs // 2 :]


def whole_tiles(*heights):
    return all(height % 16 == 0 for height in heights)


def feed_kernel(
    place, lengths_ref, order_ref, x_in, mix_in, cot_in, wo_in, w1_in, w2_in, ahead_in, vec_ref,
    gb_out, middle_out, grad_out, part_out, g1_out, s2_ref, sums_ref,
    xa, mixv, gv, wo, w1, w2, second, act, slope, unit, ds, own, from_core, from_y,
    from_x1, from_x2, from_z2, *rest,
):
    zsend, zrecv, xsend, xrecv, ssend, srecv, local = rest[-7:]
    gb = xa
    place.locate()
    seq, rows, _ = x_in.shape
    slots = seq * rows
    chunk = chunk_of(slots)
    joined = chunk // rows
    width = w1.shape[1]
    share = D // place.dp
    units = width // place.dp
    place.barrier()
    dp_sems = (zsend, zrecv, xsend, xrecv)
    seq_sems = (ssend, srecv)
    aligned = whole_tiles(share, units)
    if aligned:
        w2_part = lambda d: w2.at[pl.ds(pl.multiple_of(d * units, 16), units), :]
        g2_part = lambda d: wo.at[pl.ds(pl.multiple_of(d * units, 16), units), :]
        g1_part = lambda d: w1.at[pl.ds(pl.multiple_of(d * share, 16), share), :]
    else:
        w2_split, g2_split, g1_split = rest[:3]
        w2_part, g2_part = (lambda d: w2_split.at[d]), (lambda d: g2_split.at[d])
        g1_part = lambda d: g1_split.at[d]
    w2_in = own_rows(place, w2_in)
    ahead = [ahead_in.at[i] for i in range(len(place.z_order[:2]))]
    gather = GatherDp(place, 0, dp_sems, w2_in, w2_part, ahead=ahead)
    cots = GatherSeq(place, 2, seq_sems, cot_in, lambda s: gv.at[s])
    gather.start_x()
    gather.start_z()
    cots.start()
    loads = [
        pltpu.make_async_copy(src, dst, local.at[i])
        for i, (src, dst) in enumerate([(mix_in, mixv), (wo_in, wo), (w1_in, w1), (x_in, xa)])
    ]
    w2_own = pltpu.make_async_copy(w2_in, w2_part(place.d), local.at[5])
    cot_own = pltpu.make_async_copy(cot_in, gv.at[place.s], local.at[6])
    w2_ready = [
        pltpu.make_async_copy(src, w2_part(gather.p.block(k, 0)), local.at[7 + i])
        for i, (k, src) in enumerate(gather.ahead.items())
    ]
    for copy in (*loads, w2_own, cot_own, *w2_ready):
        copy.start()
    gain, shift, bias_out, bias1 = vec_ref[3:4], vec_ref[4:5], vec_ref[2:3], vec_ref[6:7, :width]
    own_chunk = place.s // joined
    sums_ref[...] = jnp.zeros_like(sums_ref)
    for copy in loads:
        copy.wait()

    def lines_of(index, size, step=16):
        return pl.ds(pl.multiple_of(index * size, step), size)

    def forward(i, _):
        lines = lines_of(i, chunk)
        hidden = xa[pl.ds(i * joined, joined)].reshape(chunk, D).astype(F32)
        cols = pl.ds(pl.multiple_of(i * chunk, 128), chunk)
        middle = hidden + (dot(mixv[:, cols], wo[...], ((0,), (0,))) + bias_out)

        @pl.when(i == own_chunk)
        def _():
            own[...] = middle

        normal, _ = normalize(middle)
        unit[lines, :] = normal.astype(BF16)
        tokens = (normal * gain + shift).astype(BF16)
        second[lines, :] = tokens
        expanded = dot(tokens, w1[...]) + bias1
        phi = 0.5 * (1.0 + lax.erf(expanded * (0.5**0.5)))
        act[lines, :] = (expanded * phi).astype(BF16)
        density = jnp.exp(-0.5 * expanded * expanded) * 0.3989422804014327
        slope[lines, :] = (phi + expanded * density).astype(BF16)
        @pl.when(i == slots // chunk - 1)
        def _():
            for k in gather.rest[:1]:
                gather.forward(k)

        return 0

    lax.fori_loop(0, slots // chunk, forward, 0)
    cot_own.wait()
    for j in range(1, place.ys):
        cots.arrive_y(j)
    for j in range(place.ys):
        cots.arrive_core(j)
    cots.drain()

    length = own_length(lengths_ref, order_ref)

    def mask(i, _):
        valid = i * chunk + lax.broadcasted_iota(jnp.int32, (chunk, 1), 0) < length
        cot = gv[pl.ds(i * joined, joined)].reshape(chunk, D)
        gv[pl.ds(i * joined, joined)] = jnp.where(valid, cot.astype(F32), 0.0).astype(BF16).reshape(
            joined, rows, D
        )
        return 0

    lax.fori_loop(0, slots // chunk, mask, 0)

    step = 256 if width % 256 == 0 else 128

    def w2_grad(i, _):
        cols = pl.ds(pl.multiple_of(i * step, 128), step)
        value = dot(act[:, cols], gv[...].reshape(slots, D), ((0,), (0,)))
        wo[pl.ds(pl.multiple_of(i * step, 128), step), :] = value.astype(BF16)
        return 0

    lax.fori_loop(0, width // step, w2_grad, 0)
    for k in gather.rest[1:]:
        gather.forward(k)
    if not aligned:
        for d in range(place.dp):
            g2_split[d] = wo[d * units : (d + 1) * units, :]
    r2 = ScatterDp(place, 1, dp_sems, lambda k, j, d: g2_part(d), lambda k, d: g2_part(d),
                   lambda j, k: from_x2.at[j, k], lambda k: from_z2.at[k])
    r2.start_x()
    for copy in (w2_own, *w2_ready):
        copy.wait()
    gather.arrive()
    if not aligned:
        for d in range(place.dp):
            w2[d * units : (d + 1) * units, :] = w2_split[d]

    scatter = ScatterSeq(place, 0, seq_sems, lambda s: ds.at[s], lambda j: from_core.at[j],
                         lambda j: from_y.at[j - 1])
    def backward(i):
        lines = lines_of(i, chunk)
        grad_two = gv[pl.ds(i * joined, joined)].reshape(chunk, D)
        grad_act = dot(grad_two, w2[...], ((1,), (1,)))
        grad_expanded = (grad_act * slope[lines, :].astype(F32)).astype(BF16)
        slope[lines, :] = grad_expanded
        grad_second = dot(grad_expanded, w1[...], ((1,), (1,)))
        ds[pl.ds(i * joined, joined)] = grad_second.astype(BF16).reshape(joined, rows, D)
        sums_ref[3:4] += jnp.sum(grad_second * unit[lines, :].astype(F32), axis=0, keepdims=True)
        sums_ref[4:5] += jnp.sum(grad_second, axis=0, keepdims=True)
        sums_ref[7:8, :width] += jnp.sum(grad_expanded.astype(F32), axis=0, keepdims=True)

    def fold_y(j):
        block = place.at_y(j, place.c)
        scatter.core_copy(j).wait_recv()
        ds[block] = (ds[block].astype(F32) + from_core[j].astype(F32)).astype(BF16)
        scatter.y_copy(j, ds.at[block]).start()

    turns = list(r2.order[:-1])
    for j in list(range(1, place.ys)) + [0]:
        if joined == 1:
            backward(place.at_y(j, 1 - place.c))
            scatter.core_copy(j).start()
            if turns and j != 1:
                r2.fold(turns.pop(0))
            backward(place.at_y(j, place.c))
        else:
            backward(lax.rem(place.y + j, place.ys))
            scatter.core_copy(j).start()
        if j:
            fold_y(j)
            if turns:
                r2.fold(turns.pop(0))

    gather.drain()

    def w1_grad(i, _):
        cols = pl.ds(pl.multiple_of(i * 256, 128), 256)
        value = dot(second[:, cols], slope[...], ((0,), (0,)))
        keep1[pl.ds(pl.multiple_of(i * 256, 128), 256), :] = value.astype(BF16)
        return 0

    keep1 = w1
    lax.fori_loop(0, D // 256, w1_grad, 0)
    if not aligned:
        for d in range(place.dp):
            g1_split[d] = w1[d * share : (d + 1) * share, :]
    r1 = ScatterDp(place, 2, dp_sems, lambda k, j, d: g1_part(d), lambda k, d: g1_part(d),
                   lambda j, k: from_x1.at[j, k], None)
    early, late = split_steps(place)
    r1.start_x(early)
    keep = [
        pltpu.make_async_copy(
            g1_part(r1.block(k, j)), g1_out.at[k, j], local.at[9 + seq + k * place.xs + j]
        )
        for k in late
        for j in range(place.xs)
    ]
    for copy in keep:
        copy.start()
    for k in turns:
        r2.fold(k)

    scatter.core_copy(0).wait_recv()
    value = ds[place.s].astype(F32) + from_core[0].astype(F32)
    for j in range(1, place.ys):
        scatter.y_copy(j, ds.at[place.s]).wait_recv()
        value = value + from_y[j - 1].astype(F32)
    mine = pl.ds(pl.multiple_of(lax.rem(place.s, joined) * rows, 8), rows)
    middle = own[mine, :]
    normal, spread = normalize(middle)
    grad_two = gv[place.s].astype(F32)
    grad_middle = grad_two + norm_backward(normal, spread, value * gain)
    branch = grad_middle.astype(BF16)
    gb[place.s] = branch
    sums_ref[5:6] = jnp.sum(grad_two, axis=0, keepdims=True)
    sums_ref[2:3] = jnp.sum(branch.astype(F32), axis=0, keepdims=True)
    spread_out = GatherSeq(place, 1, seq_sems, gb.at[place.s], lambda s: gb.at[s])
    spread_out.start()
    middle_out[...] = middle
    grad_out[...] = grad_middle

    def emit(i, _):
        lines = lines_of(i, chunk)
        unit[lines, :] = dot(act[lines, :], w2[...]).astype(BF16)
        return 0

    lax.fori_loop(0, slots // chunk, emit, 0)
    keep_parts = [
        pltpu.make_async_copy(
            unit.at[pl.ds(i * rows, rows), :], part_out.at[i], local.at[9 + i]
        )
        for i in range(seq)
    ]
    for copy in keep_parts:
        copy.start()
    r2.fold(0)
    for k in early:
        r1.fold_x(k)
        keep.append(
            pltpu.make_async_copy(
                g1_part(r1.block(k, 0)), g1_out.at[k, 0], local.at[9 + seq + k * place.xs]
            )
        )
        keep[-1].start()
    for j in range(1, place.ys):
        spread_out.arrive_y(j)
    s2_ref[...] = r2.finish()
    for j in range(place.ys):
        spread_out.arrive_core(j)
    save = pltpu.make_async_copy(gb, gb_out, local.at[8])
    save.start()
    for j in range(place.ys):
        scatter.core_copy(j).wait_send()
    for j in range(1, place.ys):
        scatter.y_copy(j, ds.at[place.s]).wait_send()
    spread_out.drain()
    r2.drain()
    r1.drain_x(early)
    for copy in (*keep_parts, *keep, save):
        copy.wait()


def feed(place, lengths, order, x, mix, cot, wo, w1, w2, ahead, vectors):
    seq, rows, _ = x.shape
    slots = seq * rows
    chunk = chunk_of(slots)
    width = w1.shape[1]
    share, units = D // place.dp, width // place.dp
    split = []
    anyspace = pl.BlockSpec(memory_space=pl.ANY)
    inside = pl.BlockSpec(memory_space=pltpu.VMEM)
    vm = lambda *shape: pltpu.VMEM(shape, BF16)
    if not whole_tiles(share, units):
        split = [
            vm(place.dp, units, D), vm(place.dp, units, D), vm(place.dp, share, width),
        ]
    outs = [
        ((seq, rows, D), BF16, anyspace),
        ((rows, D), F32, inside),
        ((rows, D), F32, inside),
        ((seq, rows, D), BF16, anyspace),
        ((place.zs, place.xs, share, width), BF16, anyspace),
        ((units, D), BF16, inside),
        ((8, D), F32, inside),
    ]
    return pl.pallas_call(
        functools.partial(feed_kernel, place),
        in_specs=[pl.BlockSpec(memory_space=pltpu.SMEM)] * 2 + [anyspace] * 7 + [inside],
        out_specs=[spec for _, _, spec in outs],
        out_shape=[jax.ShapeDtypeStruct(shape, kind) for shape, kind, _ in outs],
        scratch_shapes=[
            vm(seq, rows, D),
            vm(D, slots),
            vm(seq, rows, D),
            vm(D, D),
            vm(D, width),
            vm(width, D),
            vm(slots, D),
            vm(slots, width),
            vm(slots, width),
            vm(slots, D),
            vm(seq, rows, D),
            pltpu.VMEM((chunk, D), F32),
            vm(place.ys, rows, D),
            vm(max(place.ys - 1, 1), rows, D),
            vm(max(place.xs - 1, 1), place.zs, share, width),
            vm(max(place.xs - 1, 1), place.zs, units, D),
            vm(place.zs - 1, units, D),
        ]
        + split
        + dp_semaphores(place, 3)
        + seq_semaphores(place, 3)
        + [pltpu.SemaphoreType.DMA((9 + seq + place.dp,))],
        compiler_params=params(collective_id=1, has_side_effects=True),
        name="feed",
    )(lengths, order, x, mix, cot, wo, w1, w2, ahead, vectors)


def tail_kernel(
    place, vec_ref, sums_ref, lse_ref, middle_ref, gmid_ref,
    qt_in, kt_in, k_in, v_in, gb_in, mix_in, wo_in, wq_in, normed_in, x_in, part_in, g1_in, s2_in,
    layer_ref, input_ref, total_ref, w1_out, w2_out, wq_out, wo_out,
    qt, kt, kn, vn, got, gbv, mixv, normed, wq, dqkv, wo_rows, gbs, dk_sum, dv_sum, xbuf, outp,
    core_a, y_a, core_b, y_b, pq, ours, po, p1, x1, xq, xo, zq, zo, z1, r1, r2, rq, ro,
    line, ps, xsm, zsm, hop, far, *rest,
):
    zsend, zrecv, xsend, xrecv, ssend, srecv, local = rest[-7:]
    place.locate()
    seq, rows, _ = x_in.shape
    slots = seq * rows
    chunk = chunk_of(slots)
    joined = chunk // rows
    count = slots // chunk
    heads = kt.shape[0]
    wide = heads * HEAD_DIM
    share = D // place.dp
    units = s2_in.shape[0]
    place.barrier()
    dp_sems, seq_sems = (zsend, zrecv, xsend, xrecv), (ssend, srecv)
    e1 = gbv
    triple = 3 * HEAD_DIM
    groups = pq.shape[0]
    each = heads // groups
    if whole_tiles(share):
        q_part = lambda h, d: pq.at[h, pl.ds(pl.multiple_of(d * share, 16), share), :]
        o_part = lambda d: po.at[pl.ds(pl.multiple_of(d * share, 16), share), :]
    else:
        pq_split, po_split = rest[:2]
        q_part, o_part = (lambda h, d: pq_split.at[h, d]), (lambda d: po_split.at[d])
    early, late = split_steps(place)
    g1 = ScatterDp(place, 0, dp_sems, lambda k, j, d: g1_in.at[k, j],
                   lambda k, d: p1.at[late.index(k)] if k in late else g1_in.at[k, 0],
                   lambda j, k: x1.at[j, late.index(k)], lambda k: z1.at[k])
    go = ScatterDp(place, 1, dp_sems, lambda k, j, d: o_part(d), lambda k, d: o_part(d),
                   lambda j, k: xo.at[j, k], lambda k: zo.at[k])
    small = ScatterDp(place, 2, dp_sems, lambda k, j, d: ps.at[d], lambda k, d: ps.at[d],
                      lambda j, k: xsm.at[j, k], lambda k: zsm.at[k])
    gq = [
        ScatterDp(place, 3 + h, dp_sems, lambda k, j, d, h=h: q_part(h, d),
                  lambda k, d, h=h: q_part(h, d), lambda j, k, h=h: xq.at[h, j, k],
                  lambda k, h=h: zq.at[h, k])
        for h in range(groups)
    ]
    out_sum = ScatterSeq(place, 0, seq_sems, lambda s: part_in.at[s], lambda j: core_a.at[j],
                         lambda j: y_a.at[j - 1])
    e1_sum = ScatterSeq(place, 1, seq_sems, lambda s: e1.at[s], lambda j: core_b.at[j],
                        lambda j: y_b.at[j - 1])
    final2 = GatherSeq(place, 2, seq_sems, r2, lambda s: w2_out.at[s])
    final1 = GatherSeq(place, 3, seq_sems, r1, lambda s: w1_out.at[s])
    final_o = GatherSeq(place, 4, seq_sems, ro, lambda s: wo_out.at[s])
    final_q = [
        GatherSeq(place, 7 + h, seq_sems, rq.at[h], lambda s, h=h: wq_out.at[s, h])
        for h in range(groups)
    ]

    first = [(gb_in, gbv), (wo_in.at[pl.ds(pl.multiple_of(place.s * wide, 16), wide), :], wo_rows),
             (mix_in, mixv), (qt_in, qt), (kt_in, kt), (k_in, kn), (v_in, vn)]
    later = [(normed_in, normed), (wq_in, wq)]
    later += [(s2_in, r2)] + [(g1_in.at[k, 0], p1.at[i]) for i, k in enumerate(late)]
    later += [(part_in.at[place.at_y(j, place.c)], outp.at[j]) for j in range(place.ys)]
    loads = [
        pltpu.make_async_copy(src, dst, local.at[i]) for i, (src, dst) in enumerate(first + later)
    ]
    free = len(loads)
    for copy in loads:
        copy.start()
    for k in early:
        g1.z_copy(k).start()
    g1.start_x(late)
    for j in list(range(1, place.ys)) + [0]:
        out_sum.core_copy(j).start()
    for copy in loads[:2]:
        copy.wait()

    def lines_of(index, size, step=16):
        return pl.ds(pl.multiple_of(index * size, step), size)

    def turn(i, _):
        cols = pl.ds(pl.multiple_of(i * chunk, 128), chunk)
        branch = gbv[pl.ds(i * joined, joined)].reshape(chunk, D)
        got[:, cols] = dot(wo_rows[...], branch, ((1,), (1,))).astype(BF16)
        for s in range(seq):

            @pl.when(place.s == s)
            def _():
                gbs[lines_of(i, chunk), :] = branch[:, s * wide : (s + 1) * wide]

        return 0

    lax.fori_loop(0, count, turn, 0)
    loads[2].wait()

    def wo_grad(i, _):
        lines = pl.ds(pl.multiple_of(i * 256, 128), 256)
        po[lines, :] = dot(mixv[lines, :], gbs[...]).astype(BF16)
        return 0

    lax.fori_loop(0, D // 256, wo_grad, 0)
    if not whole_tiles(share):
        for d in range(place.dp):
            po_split[d] = po[d * share : (d + 1) * share, :]
    go.start_x()

    block = 256

    def head_back(head):
        part = slice(head * HEAD_DIM, (head + 1) * HEAD_DIM)
        first = head * triple
        dk_sum[...] = jnp.zeros_like(dk_sum)
        dv_sum[...] = jnp.zeros_like(dv_sum)

        def one(i, _):
            cols = pl.ds(pl.multiple_of(i * block, 128), block)
            grad = got[part, cols]
            own_rows = pl.ds(pl.multiple_of(place.s * wide + head * HEAD_DIM, 16), HEAD_DIM)
            mixed = mixv[own_rows, cols]
            delta = jnp.sum(grad.astype(F32) * mixed.astype(F32), axis=0, keepdims=True)
            probs = jnp.exp2(dot(kn[head], qt[head, :, cols]) * QSCALE - lse_ref[head, :, cols])
            grad_scores = (probs * (dot(vn[head], grad) - delta)).astype(BF16)
            dv_sum[...] += dot(probs.astype(BF16), grad, ((1,), (1,)))
            dk_sum[...] += dot(grad_scores, qt[head, :HEAD_DIM, cols], ((1,), (1,)))
            turned = dot(kt[head], grad_scores) * SCALE
            lines = pl.ds(pl.multiple_of(i * block, 128), block)
            dqkv[lines, first : first + HEAD_DIM] = jnp.transpose(turned).astype(BF16)
            return 0

        lax.fori_loop(0, slots // block, one, 0)
        dqkv[:, first + HEAD_DIM : first + 2 * HEAD_DIM] = (dk_sum[...] * SCALE).astype(BF16)
        dqkv[:, first + 2 * HEAD_DIM : first + triple] = dv_sum[...].astype(BF16)

    def q_grads(group):
        ours[...] = dqkv[:, group * each * triple : (group + 1) * each * triple]

        def q_grad(i, _):
            lines = pl.ds(pl.multiple_of(i * 256, 128), 256)
            pq[group, lines, :] = dot(normed[lines, :], ours[...]).astype(BF16)
            return 0

        lax.fori_loop(0, D // 256, q_grad, 0)
        if not whole_tiles(share):
            for d in range(place.dp):
                pq_split[group, d] = pq[group, d * share : (d + 1) * share, :]
        gq[group].start_x()

    def out_fold():
        for j in range(1, place.ys):
            out_sum.core_copy(j).wait_recv()
            outp[j] = (outp[j].astype(F32) + core_a[j].astype(F32)).astype(BF16)
            out_sum.y_copy(j, outp.at[j]).start()

    def publish(group, result, final):
        result[...] = group.finish()
        final.start()

    for copy in loads[3:]:
        copy.wait()
    out_fold()
    final2.start()
    for head in range(heads):
        head_back(head)
        if head == 0:
            for k in late:
                g1.fold(k)
        if head == min(1, heads - 1):
            go.fold_all()
        if (head + 1) % each == 0:
            q_grads(head // each)
        if head == min(2, heads - 1):
            publish(g1, r1, final1)
        if head == heads - 1:
            for group in range(groups - 1):
                gq[group].fold_all()
            publish(go, ro, final_o)

    line[...] = jnp.zeros_like(line)
    line[0:6] = sums_ref[0:6]
    bias_sum = jnp.sum(dqkv[...].astype(F32), axis=0, keepdims=True)
    for s in range(seq):

        @pl.when(place.s == s)
        def _():
            for head in range(heads):
                to = slice(s * wide + head * HEAD_DIM, s * wide + (head + 1) * HEAD_DIM)
                at = head * triple
                line[6:7, to] = bias_sum[:, at : at + HEAD_DIM]
                line[7:8, to] = bias_sum[:, at + 2 * HEAD_DIM : at + triple]

    order = []
    for j in list(range(1, place.ys)) + [0]:
        if joined == 1:
            order += [(place.at_y(j, 1 - place.c), j, False), (place.at_y(j, place.c), j, True)]
        else:
            order += [(lax.rem(place.y + j, place.ys), j, True)]

    def x_load(at, slot):
        return pltpu.make_async_copy(
            x_in.at[pl.ds(at * joined, joined)], xbuf.at[slot], local.at[free + slot]
        )

    x_load(order[0][0], 0).start()
    for step, (at, j, both) in enumerate(order):
        slot = step % 2
        if step + 1 < len(order):
            x_load(order[step + 1][0], 1 - slot).start()
        x_load(at, slot).wait()
        grad = dot(dqkv[lines_of(at, chunk), :], wq[...].reshape(D, 3 * wide), ((1,), (1,)))
        normal, spread = normalize(xbuf[slot].reshape(chunk, D).astype(F32))
        line[0:1] += jnp.sum(grad * normal, axis=0, keepdims=True)
        line[1:2] += jnp.sum(grad, axis=0, keepdims=True)
        e1[pl.ds(at * joined, joined)] = grad.astype(BF16).reshape(joined, rows, D)
        if joined == 2 or not both:
            e1_sum.core_copy(j).start()
        if both and j:
            target = place.at_y(j, place.c)
            e1_sum.core_copy(j).wait_recv()
            e1[target] = (e1[target].astype(F32) + core_b[j].astype(F32)).astype(BF16)
            e1_sum.y_copy(j, e1.at[target]).start()
    for d in range(place.dp):
        ps[d] = jnp.zeros_like(ps[d])
        ps[d, 0:8] = line[:, d * share : (d + 1) * share]
        ps[d, pl.ds(8 + place.s, 1), :units] = sums_ref[7:8, d * units : (d + 1) * units]
    small.start_x()
    small.fold_all()
    gq[groups - 1].fold_all()
    for group in range(groups - 1):
        publish(gq[group], rq.at[group], final_q[group])
    value = outp[0].astype(F32)
    out_sum.core_copy(0).wait_recv()
    value = value + core_a[0].astype(F32)
    for j in range(1, place.ys):
        out_sum.y_copy(j, outp.at[j]).wait_recv()
        value = value + y_a[j - 1].astype(F32)
    layer_ref[...] = (middle_ref[...] + (value + vec_ref[5:6])).astype(BF16)

    hop[0] = small.finish()
    near = send(hop.at[0], far.at[0], ssend.at[5, 1, 0], srecv.at[5, 1, 0],
                (place.d, place.partner))
    near.start()
    for final in (final2, final1, final_o):
        for j in range(1, place.ys):
            final.arrive_y(j)
    near.wait_recv()
    hop[1] = hop[0] + far[0]
    across = [
        send(hop.at[1], far.at[j], ssend.at[5, 0, j], srecv.at[5, 0, j],
             (place.d, place.at_y(j, place.c)))
        for j in range(1, place.ys)
    ]
    for copy in across:
        copy.start()
    keep = [
        pltpu.make_async_copy(src, dst.at[place.s], local.at[free + 2 + i])
        for i, (src, dst) in enumerate([(r1, w1_out), (r2, w2_out), (ro, wo_out), (rq, wq_out)])
    ]
    for copy in keep[:3]:
        copy.start()
    publish(gq[groups - 1], rq.at[groups - 1], final_q[groups - 1])
    keep[3].start()

    value = e1[place.s].astype(F32)
    e1_sum.core_copy(0).wait_recv()
    value = value + core_b[0].astype(F32)
    for j in range(1, place.ys):
        e1_sum.y_copy(j, e1.at[place.s]).wait_recv()
        value = value + y_b[j - 1].astype(F32)
    last = (len(order) - 1) % 2
    hidden = xbuf[last, lax.rem(place.s, joined)].astype(F32)
    normal, spread = normalize(hidden)
    input_ref[...] = (gmid_ref[...] + norm_backward(normal, spread, value * vec_ref[0:1])).astype(
        BF16
    )
    for final in final_q:
        for j in range(1, place.ys):
            final.arrive_y(j)
    value = hop[1]
    for j, copy in enumerate(across):
        copy.wait_recv()
        value = value + far[j + 1]
    total_ref[...] = value
    finals = (final1, final2, final_o, *final_q)
    for final in finals:
        for j in range(place.ys):
            final.arrive_core(j)
    for final in finals:
        final.drain()
    for group in (out_sum, e1_sum):
        for j in range(place.ys):
            group.core_copy(j).wait_send()
        for j in range(1, place.ys):
            group.y_copy(j, outp.at[j]).wait_send()
    for group in (*gq, go, small):
        group.drain()
    g1.drain_x(late)
    g1.drain_z()
    for copy in (near, *across):
        copy.wait_send()
    for copy in keep:
        copy.wait()


def tail(place, vectors, sums, lse, middle, gmid, qt, kt, kn, vn, gb, mix, wo, wq, normed, x, part, g1, s2):
    seq, rows, _ = x.shape
    slots = seq * rows
    chunk = chunk_of(slots)
    joined = chunk // rows
    heads = kt.shape[0]
    wide = heads * HEAD_DIM
    share = D // place.dp
    width, units = g1.shape[3], s2.shape[0]
    ys, xs, zs = place.ys, max(place.xs - 1, 1), place.zs
    anyspace = pl.BlockSpec(memory_space=pl.ANY)
    inside = pl.BlockSpec(memory_space=pltpu.VMEM)
    vm = lambda *shape: pltpu.VMEM(shape, BF16)
    tall = 16
    each = 2 if heads % 2 == 0 else 1
    groups, triple = heads // each, 3 * HEAD_DIM * each
    outs = [
        ((rows, D), BF16, inside),
        ((rows, D), BF16, inside),
        ((tall, share), F32, inside),
        ((seq, share, width), BF16, anyspace),
        ((seq, units, D), BF16, anyspace),
        ((seq, groups, share, triple), BF16, anyspace),
        ((seq, share, wide), BF16, anyspace),
    ]
    split = []
    if not whole_tiles(share):
        split = [vm(groups, place.dp, share, triple), vm(place.dp, share, wide)]
    return pl.pallas_call(
        functools.partial(tail_kernel, place),
        in_specs=[inside] * 5 + [anyspace] * 13,
        out_specs=[spec for _, _, spec in outs],
        out_shape=[jax.ShapeDtypeStruct(shape, kind) for shape, kind, _ in outs],
        scratch_shapes=[
            vm(heads, 128, slots),
            vm(heads, HEAD_DIM, slots),
            vm(heads, slots, 128),
            vm(heads, slots, HEAD_DIM),
            vm(wide, slots),
            vm(seq, rows, D),
            vm(D, slots),
            vm(D, slots),
            vm(place.dp, share, 3 * wide),
            vm(slots, 3 * wide),
            vm(wide, D),
            vm(slots, wide),
            pltpu.VMEM((slots, HEAD_DIM), F32),
            pltpu.VMEM((slots, HEAD_DIM), F32),
            vm(2, joined, rows, D),
            vm(ys, rows, D),
            vm(ys, rows, D),
            vm(max(ys - 1, 1), rows, D),
            vm(ys, rows, D),
            vm(max(ys - 1, 1), rows, D),
            vm(groups, D, triple),
            vm(slots, triple),
            vm(D, wide),
            vm(zs - zs // 2, share, width),
            vm(xs, zs - zs // 2, share, width),
            vm(groups, xs, zs, share, triple),
            vm(xs, zs, share, wide),
            vm(groups, zs - 1, share, triple),
            vm(zs - 1, share, wide),
            vm(zs - 1, share, width),
            vm(share, width),
            vm(units, D),
            vm(groups, share, triple),
            vm(share, wide),
            pltpu.VMEM((8, D), F32),
            pltpu.VMEM((place.dp, tall, share), F32),
            pltpu.VMEM((xs, zs, tall, share), F32),
            pltpu.VMEM((zs - 1, tall, share), F32),
            pltpu.VMEM((2, tall, share), F32),
            pltpu.VMEM((ys, tall, share), F32),
        ]
        + split
        + dp_semaphores(place, 3 + heads)
        + seq_semaphores(place, 7 + heads)
        + [pltpu.SemaphoreType.DMA((24 + ys,))],
        compiler_params=params(collective_id=2, has_side_effects=True),
        name="tail",
    )(vectors, sums, lse, middle, gmid, qt, kt, kn, vn, gb, mix, wo, wq, normed, x, part, g1, s2)


def prep_kernel(place, q_ref, k_ref, v_ref, w1_ref, wqkv_ref, w1_out):
    place.locate()
    dp, seq = place.dp, place.seq
    wide = D // seq
    units = FF // (dp * seq)
    for s in range(seq):

        @pl.when(place.s == s)
        def _():
            for i, ref in enumerate((q_ref, k_ref, v_ref)):
                for head in range(wide // HEAD_DIM):
                    to = (3 * head + i) * HEAD_DIM
                    at = s * wide + head * HEAD_DIM
                    wqkv_ref[:, to : to + HEAD_DIM] = ref[:, at : at + HEAD_DIM]
            for d in range(dp):
                first = d * (FF // dp) + s * units
                w1_out[:, d * units : (d + 1) * units] = w1_ref[:, first : first + units]


def prep(place, q, k, v, w1):
    wide = D // place.seq
    share = q.shape[0]
    inside = pl.BlockSpec(memory_space=pltpu.VMEM)
    return pl.pallas_call(
        functools.partial(prep_kernel, place),
        in_specs=[inside] * 4,
        out_specs=[inside] * 2,
        out_shape=[
            jax.ShapeDtypeStruct((share, 3 * wide), BF16),
            jax.ShapeDtypeStruct((share, FF // place.seq), BF16),
        ],
        compiler_params=params(),
        name="prep",
    )(q, k, v, w1)


def finish_kernel(
    place, w1_ref, w2_ref, wq_ref, wo_ref, total_ref, layer_ref, input_ref,
    layer_out, input_out, w1_out, w2_out, q_out, k_out, v_out, wo_out, g1_out, s1_out, bo_out, g2_out, s2_out, b2_out,
    bq_out, bv_out, b1_out,
):
    place.locate()
    dp, seq = place.dp, place.seq
    share = D // dp
    wide = D // seq
    units = FF // (dp * seq)
    each = wide // HEAD_DIM // wq_ref.shape[1]
    w2_out[...] = w2_ref[...].astype(F32)
    for s in range(seq):
        cols = slice(s * wide, (s + 1) * wide)
        for head in range(wide // HEAD_DIM):
            to = slice(s * wide + head * HEAD_DIM, s * wide + (head + 1) * HEAD_DIM)
            for i, out in enumerate((q_out, k_out, v_out)):
                first = ((head % each) * 3 + i) * HEAD_DIM
                part = wq_ref[s, head // each, :, first : first + HEAD_DIM]
                out[:, to] = part.astype(F32)
        wo_out[:, cols] = wo_ref[s].astype(F32)
        for d in range(dp):
            first = d * (FF // dp) + s * units
            w1_out[:, first : first + units] = w1_ref[s, :, d * units : (d + 1) * units].astype(F32)

    @pl.when(pl.program_id(0) == 0)
    def _():
        layer_out[...] = layer_ref[...]
        input_out[...] = input_ref[...]
        outs = (g1_out, s1_out, bo_out, g2_out, s2_out, b2_out, bq_out, bv_out)
        for i, out in enumerate(outs):
            out[...] = total_ref[i : i + 1]
        for s in range(seq):
            b1_out[:, s * units : (s + 1) * units] = total_ref[8 + s : 9 + s, :units]


def finish(place, w1, w2, wq, wo, totals, layer, grad):
    dp, seq = place.dp, place.seq
    share, units, wide = D // dp, w2.shape[1], D // seq
    tile = 32 if share % 32 == 0 and units == share else share
    steps = share // tile
    tall = units // steps
    mat = lambda *tail: pl.BlockSpec((seq, tile, *tail), lambda i: (0, i, 0))
    out = lambda cols: pl.BlockSpec((tile, cols), lambda i: (i, 0))
    small = pl.BlockSpec((1, share), lambda i: (0, 0))
    f32 = lambda *shape: jax.ShapeDtypeStruct(shape, F32)
    return pl.pallas_call(
        functools.partial(finish_kernel, place),
        grid=(steps,),
        in_specs=[
            mat(w1.shape[2]),
            pl.BlockSpec((seq, tall, D), lambda i: (0, i, 0)),
            pl.BlockSpec((seq, wq.shape[1], tile, wq.shape[3]), lambda i: (0, 0, i, 0)),
            mat(wo.shape[2]),
            pl.BlockSpec(totals.shape, lambda i: (0, 0)),
            pl.BlockSpec(layer.shape, lambda i: (0, 0)),
            pl.BlockSpec(layer.shape, lambda i: (0, 0)),
        ],
        out_specs=[pl.BlockSpec(layer.shape, lambda i: (0, 0))] * 2
        + [out(FF), pl.BlockSpec((seq, tall, D), lambda i: (0, i, 0))]
        + [out(D)] * 4
        + [small] * 8
        + [pl.BlockSpec((1, FF // dp), lambda i: (0, 0))],
        out_shape=[jax.ShapeDtypeStruct(layer.shape, BF16)] * 2
        + [f32(share, FF), f32(seq, units, D)]
        + [f32(share, D)] * 4
        + [f32(1, share)] * 8
        + [f32(1, FF // dp)],
        compiler_params=params(),
        name="finish",
    )(w1, w2, wq, wo, totals, layer, grad)


def per_device(
    hidden_in, cotangent, clip_lengths, clip_order, first_gain, first_shift, query_weight,
    query_bias, key_weight, value_weight, value_bias, output_weight, output_bias, second_gain,
    second_shift, expand_weight, expand_bias, reduce_weight, reduce_bias,
):
    dp = lax.axis_size("dp")
    seq = lax.axis_size("seq")
    me = lax.axis_index("seq")
    slots = hidden_in.shape[1] * seq
    units = FF // (dp * seq)
    quarter = dp * units

    spot = Place(dp, seq)
    b1 = lax.dynamic_slice_in_dim(expand_bias, me * units, units, 0)
    rows = [first_gain, first_shift, output_bias, second_gain, second_shift, reduce_bias,
            jnp.pad(b1, (0, D // dp - units)), query_bias, value_bias]
    small = jnp.pad(jnp.stack(rows).astype(F32), ((0, 16 - len(rows)), (0, 0)))
    if not whole_tiles(units):
        reduce_weight = lax.dynamic_slice_in_dim(reduce_weight, me * units, units, 0)
    wqkv_share, w1_share = prep(spot, query_weight, key_weight, value_weight, expand_weight)
    x, vectors, w_qkv, w_out, w_expand, w2_ahead, normed, qt, kt, keys, values, mix, lse = front(
        spot, clip_lengths, clip_order, hidden_in[0], small, wqkv_share, output_weight, w1_share,
        reduce_weight,
    )
    w_out = w_out.reshape(D, D)
    w_expand = w_expand.reshape(D, quarter)
    mix = mix.reshape(D, slots)
    grad_branch, middle, grad_middle, out_part, g1, s2, sums = feed(
        spot, clip_lengths, clip_order, x, mix, cotangent[0], w_out, w_expand, reduce_weight,
        w2_ahead, vectors,
    )
    layer_output, input_grad, totals, w1_grad, w2_grad, qkv_grad, wo_grad = tail(
        spot, vectors, sums, lse, middle, grad_middle, qt, kt, keys, values, grad_branch, mix,
        w_out, w_qkv, normed, x, out_part, g1, s2,
    )
    results = finish(
        spot, w1_grad, w2_grad, qkv_grad, wo_grad, totals, layer_output, input_grad
    )
    layer_output, input_grad, *results = results
    (w1_grad, w2_grad, wq_grad, wk_grad, wv_grad, wo_grad) = results[:6]
    g1, s1, bo, g2, s2, b2, bq, bv, b1 = (value.reshape(-1) for value in results[6:])
    return (
        layer_output[None], input_grad[None], g1, s1, wq_grad, bq, wk_grad, wv_grad, bv, wo_grad,
        bo, g2, s2, w1_grad, b1, w2_grad.reshape(FF // dp, D), b2,
    )


def solution(mesh):
    clip = P("dp", "seq", None)
    vec = P("dp")
    mat = P("dp", None)
    return jax.shard_map(
        per_device,
        mesh=mesh,
        in_specs=(
            clip, clip, P(), vec, vec, vec, mat, vec, mat, mat, vec, mat, vec, vec, vec, mat, vec,
            mat, vec,
        ),
        out_specs=(
            clip, clip, vec, vec, mat, vec, mat, mat, vec, mat, vec, vec, vec, mat, vec, mat, vec,
        ),
        check_vma=False,
    )
```

```python
import functools

import jax
import jax.numpy as jnp
from jax import lax
from jax.experimental import pallas as pl
from jax.experimental.pallas import tpu as pltpu
from jax.sharding import PartitionSpec as P

D = 1280
FF = 5120
HEADS = 16
HEAD_DIM = D // HEADS
EPSILON = 1e-05
SCALE = HEAD_DIM ** (-0.5)
F32 = jnp.float32
BF16 = jnp.bfloat16
VMEM_LIMIT = 66_000_000
MESH = pl.DeviceIdType.MESH


def dot(left, right, contract=((1,), (0,))):
    return lax.dot_general(left, right, (contract, ((), ())), preferred_element_type=F32)


def normalize(values):
    average = jnp.mean(values, axis=-1, keepdims=True)
    centered = values - average
    variance = jnp.mean(centered * centered, axis=-1, keepdims=True)
    spread = lax.rsqrt(variance + EPSILON)
    return centered * spread, spread


def norm_backward(unit, spread, grad_unit):
    inner = jnp.mean(grad_unit * unit, axis=-1, keepdims=True)
    return spread * (grad_unit - jnp.mean(grad_unit, axis=-1, keepdims=True) - unit * inner)


def params(**extra):
    return pltpu.CompilerParams(vmem_limit_bytes=VMEM_LIMIT, **extra)


def whole(shape):
    return pl.BlockSpec(shape, lambda *_: (0,) * len(shape), pipeline_mode=pl.Buffered(1))


def chunk_of(slots):
    return slots // 4 if slots % 512 == 0 else slots


class Place:
    def __init__(self, dp, seq):
        self.dp, self.seq = dp, seq
        self.xs = 1 << ((dp.bit_length() - 1) // 2)
        self.zs = dp // self.xs
        self.ys = seq // 2
        self.z_order = sorted(range(1, self.zs), key=lambda k: min(k, self.zs - k))

    def locate(self):
        self.d, self.s = lax.axis_index("dp"), lax.axis_index("seq")
        self.z, self.x = self.d // self.xs, lax.rem(self.d, self.xs)
        self.y, self.c = self.s // 2, lax.rem(self.s, 2)
        self.partner = self.y * 2 + 1 - self.c

    def at_z(self, k):
        return lax.rem(self.z + k + self.zs, self.zs) * self.xs + self.x

    def block(self, k, j):
        return lax.rem(self.z - k + self.zs, self.zs) * self.xs + lax.rem(
            self.x - j + self.xs, self.xs
        )

    def at_x(self, j):
        return self.z * self.xs + lax.rem(self.x + j, self.xs)

    def at_y(self, j, core):
        return lax.rem(self.y + j + self.ys, self.ys) * 2 + core

    def peers(self, over_dp=True, over_seq=True):
        found = []
        if over_dp:
            found += [(self.at_z(k), self.s) for k in range(1, self.zs)]
            found += [(self.at_x(j), self.s) for j in range(1, self.xs)]
        if over_seq:
            found += [(self.d, self.partner)]
            found += [(self.d, self.at_y(j, self.c)) for j in range(1, self.ys)]
        return found

    def barrier(self, **which):
        semaphore = pltpu.get_barrier_semaphore()
        peers = self.peers(**which)
        for peer in peers:
            pl.semaphore_signal(semaphore, inc=1, device_id=peer, device_id_type=MESH)
        pl.semaphore_wait(semaphore, len(peers))


def send(src, dst, send_sem, recv_sem, device):
    return pltpu.make_async_remote_copy(
        src_ref=src, dst_ref=dst, send_sem=send_sem, recv_sem=recv_sem, device_id=device,
        device_id_type=MESH,
    )


def dp_semaphores(place, groups):
    return [
        pltpu.SemaphoreType.DMA((groups, place.zs)),
        pltpu.SemaphoreType.DMA((groups, place.zs)),
        pltpu.SemaphoreType.DMA((groups, place.zs, place.xs)),
        pltpu.SemaphoreType.DMA((groups, place.zs, place.xs)),
    ]


def seq_semaphores(place, groups):
    return [pltpu.SemaphoreType.DMA((groups, 2, place.ys))] * 2


class GatherDp:
    def __init__(self, place, group, sems, own, slab, on=None, ahead=()):
        self.p, self.g, self.own, self.slab, self.on = place, group, own, slab, on
        self.staged = on is None
        self.ahead = dict(zip(place.z_order, ahead))
        self.rest = place.z_order[len(self.ahead) :]
        self.zsend, self.zrecv, self.xsend, self.xrecv = sems

    def when(self, block, act):
        if self.on is None:
            act()
        else:
            pl.when(self.on(block))(act)

    def z_copy(self, k):
        return send(self.own, self.slab(self.p.d), self.zsend.at[self.g, k],
                    self.zrecv.at[self.g, k], (self.p.at_z(k), self.p.s))

    def x_copy(self, k, j):
        block = self.p.block(k, 0)
        src = self.own if k == 0 else self.ahead.get(k, self.slab(block))
        return send(src, self.slab(block), self.xsend.at[self.g, k, j],
                    self.xrecv.at[self.g, k, j], (self.p.at_x(j), self.p.s))

    def start_x(self):
        def act():
            for k in [0, *self.ahead]:
                for j in range(1, self.p.xs):
                    self.x_copy(k, j).start()

        self.when(self.p.d, act)

    def start_z(self):
        def act():
            for k in self.rest[:2] if self.staged else self.rest:
                self.z_copy(k).start()

        self.when(self.p.d, act)

    def forward(self, k):
        place = self.p

        def act():
            send(self.own, self.slab(place.block(k, 0)), self.zsend.at[self.g, k],
                 self.zrecv.at[self.g, k], (place.at_z(k), place.s)).wait_recv()
            for j in range(1, place.xs):
                self.x_copy(k, j).start()
            later = self.rest.index(k) + 2
            if self.staged and later < len(self.rest):
                self.z_copy(self.rest[later]).start()

        self.when(place.block(k, 0), act)

    def forward_all(self):
        for k in self.p.z_order:
            self.forward(k)

    def arrive(self):
        place = self.p
        for k in range(place.zs):
            for j in range(1, place.xs):
                wait = send(self.own, self.slab(place.block(k, j)), self.xsend.at[self.g, k, j],
                            self.xrecv.at[self.g, k, j], (place.at_x(j), place.s)).wait_recv
                self.when(place.block(k, j), wait)

    def drain(self):
        place = self.p

        def act():
            for k in self.rest:
                self.z_copy(k).wait_send()

        self.when(place.d, act)
        for k in range(place.zs):
            for j in range(1, place.xs):
                self.when(place.block(k, 0), self.x_copy(k, j).wait_send)


class GatherSeq:
    def __init__(self, place, group, sems, own, slab):
        self.p, self.g, self.own, self.slab = place, group, own, slab
        self.sends, self.recvs = sems

    def y_copy(self, j):
        place = self.p
        return send(self.own, self.slab(place.s), self.sends.at[self.g, 0, j],
                    self.recvs.at[self.g, 0, j], (place.d, place.at_y(j, place.c)))

    def core_copy(self, j):
        place = self.p
        block = place.at_y(-j, place.c)
        src = self.own if j == 0 else self.slab(block)
        return send(src, self.slab(block), self.sends.at[self.g, 1, j],
                    self.recvs.at[self.g, 1, j], (place.d, place.partner))

    def start(self):
        for j in range(1, self.p.ys):
            self.y_copy(j).start()
        self.core_copy(0).start()

    def arrive_y(self, j):
        place = self.p
        block = place.at_y(-j, place.c)
        send(self.own, self.slab(block), self.sends.at[self.g, 0, j], self.recvs.at[self.g, 0, j],
             (place.d, place.at_y(j, place.c))).wait_recv()
        self.core_copy(j).start()
        return block

    def arrive_core(self, j):
        place = self.p
        block = place.at_y(-j, 1 - place.c)
        send(self.own, self.slab(block), self.sends.at[self.g, 1, j], self.recvs.at[self.g, 1, j],
             (place.d, place.partner)).wait_recv()
        return block

    def drain(self):
        for j in range(1, self.p.ys):
            self.y_copy(j).wait_send()
        for j in range(self.p.ys):
            self.core_copy(j).wait_send()


LOG2E = 1.4426950408889634
QSCALE = SCALE * LOG2E


def own_rows(place, w2):
    units = FF // (place.dp * place.seq)
    if whole_tiles(units):
        return w2.at[pl.ds(pl.multiple_of(place.s * units, 16), units), :]
    return w2


def own_length(lengths_ref, order_ref):
    length = 0
    for clip in range(lengths_ref.shape[0]):
        length = length + jnp.where(order_ref[0] == clip, lengths_ref[clip], 0)
    return length


def front_kernel(
    place, lengths_ref, order_ref, x_in, sm_in, wq_in, wo_in, w1_in, w2_in,
    x_out, vec_out, wq_out, wo_out, w1_out, w2_out, normed_out, qt_out, kt_out, k_out,
    v_out, mix_out, lse_ref,
    xs, nr, nt, biases, sm, wq, wt, qt, kt, vt, kn, vn, mix,
    zsend, zrecv, xsend, xrecv, ssend, srecv, swap_send, swap_recv, local,
):
    place.locate()
    seq, rows = x_out.shape[0], x_out.shape[1]
    slots = seq * rows
    heads = k_out.shape[0]
    wide = heads * HEAD_DIM
    place.barrier()
    dp_sems = (zsend, zrecv, xsend, xrecv)
    seq_sems = (ssend, srecv)

    def over_dp(group, own, buffer):
        return GatherDp(place, group, dp_sems, own, lambda d: buffer.at[d])

    def over_seq(group, own, buffer):
        return GatherSeq(place, group, seq_sems, own, lambda s: buffer.at[s])

    g_sm = over_dp(0, sm_in, sm)
    g_wq = over_dp(1, wq_in, wq)
    g_wo = GatherDp(place, 2, dp_sems, wo_in, lambda d: wo_out.at[d],
                    lambda d: lax.rem(d, 2) == place.c)
    g_w1 = over_dp(3, w1_in, w1_out)
    g_x = over_seq(0, x_in, xs)

    swaps = [(k, j) for k in range(place.zs) for j in range(place.xs) if (k, j) != (0, 0)]

    def swap(k, j):
        slab = wo_out.at[place.block(k, j)]
        return send(slab, slab, swap_send.at[k, j], swap_recv.at[k, j], (place.d, place.partner))

    def swap_start():
        for k, j in swaps:
            pl.when(g_wo.on(place.block(k, j)))(swap(k, j).start)

    def swap_finish():
        for k, j in swaps:
            pl.when(g_wo.on(place.block(k, j)))(swap(k, j).wait_send)
            pl.when(~g_wo.on(place.block(k, j)))(swap(k, j).wait_recv)

    locals_in = [
        pltpu.make_async_copy(x_in, xs.at[place.s], local.at[0]),
        pltpu.make_async_copy(sm_in, sm.at[place.d], local.at[1]),
        pltpu.make_async_copy(wq_in, wq.at[place.d], local.at[2]),
    ]
    w1_own = pltpu.make_async_copy(w1_in, w1_out.at[place.d], local.at[5])
    wo_own = pltpu.make_async_copy(wo_in, wo_out.at[place.d], local.at[4])
    for copy in locals_in:
        copy.start()
    g_sm.start_x()
    g_sm.start_z()
    g_x.start()
    g_wq.start_x()
    g_wq.start_z()
    w1_own.start()
    wo_own.start()

    column = lax.broadcasted_iota(jnp.int32, (slots, 1), 0)
    penalty = jnp.where(column >= own_length(lengths_ref, order_ref), -1e30, 0.0).astype(BF16)
    ones_row = jnp.where(
        lax.broadcasted_iota(jnp.int32, (128 - HEAD_DIM, slots), 0) == 0, 1.0, 0.0
    ).astype(BF16)
    for head in range(heads):
        kn[head] = jnp.zeros((slots, 128), BF16)
        kn[head, :, HEAD_DIM : HEAD_DIM + 1] = penalty
        qt[head, HEAD_DIM:, :] = ones_row

    for copy in locals_in:
        copy.wait()
    turns = list(place.z_order)
    g_sm.forward(turns[0])
    for k in turns[1:2]:
        g_sm.forward(k)
    g_wq.forward(turns[0])
    for k in turns[2:]:
        g_sm.forward(k)
    turns.pop(0)
    if turns:
        g_wq.forward(turns.pop(0))
    g_sm.arrive()
    part, units = sm.shape[2], w1_in.shape[1] // place.dp
    vec_out[...] = jnp.zeros_like(vec_out)
    for d in range(place.dp):
        vec_out[0:6, d * part : (d + 1) * part] = sm[d, 0:6, :]
        vec_out[7:9, d * part : (d + 1) * part] = sm[d, 7:9, :]
        vec_out[6:7, d * units : (d + 1) * units] = sm[d, 6:7, :units]
    for s in range(seq):

        @pl.when(place.s == s)
        def _():
            biases[0:2] = vec_out[7:9, s * wide : (s + 1) * wide]

    gain, shift = vec_out[0:1], vec_out[1:2]

    def norm_block(block):
        unit, _ = normalize(xs[block].astype(F32))
        lines = pl.ds(pl.multiple_of(block * rows, 16), rows)
        nr[lines, :] = (unit * gain + shift).astype(BF16)

    norm_block(place.s)
    norm_block(g_x.arrive_core(0))
    for j in range(1, place.ys):
        if turns:
            g_wq.forward(turns.pop(0))
        norm_block(g_x.arrive_y(j))
    for k in turns:
        g_wq.forward(k)
    g_wo.start_z()
    for j in range(1, place.ys):
        norm_block(g_x.arrive_core(j))
    chunk = chunk_of(slots)

    def turn_block(block, _):
        spot = pl.ds(pl.multiple_of(block * chunk, 128), chunk)
        nt[:, spot] = jnp.transpose(nr[spot, :])
        return 0

    lax.fori_loop(0, slots // chunk, turn_block, 0)
    g_wq.arrive()
    g_wo.start_x()
    share = wq.shape[1]
    wt[...] = jnp.transpose(wq[...].reshape(place.dp * share, 3 * wide))
    bias = jnp.transpose(biases[...])
    g_wo.forward_all()
    g_w1.start_z()
    g_w1.start_x()

    def project_block(block, _):
        cols = pl.ds(pl.multiple_of(block * chunk, 128), chunk)
        tokens = dot(wt[...], nt[:, cols])
        for head in range(heads):
            first = 3 * head * HEAD_DIM
            part = slice(head * HEAD_DIM, (head + 1) * HEAD_DIM)
            query = tokens[first : first + HEAD_DIM] + bias[part, 0:1]
            key = tokens[first + HEAD_DIM : first + 2 * HEAD_DIM].astype(BF16)
            value = tokens[first + 2 * HEAD_DIM : first + 3 * HEAD_DIM] + bias[part, 1:2]
            value = value.astype(BF16)
            qt[head, :HEAD_DIM, cols] = query.astype(BF16)
            kt[head, :, cols] = key
            vt[head, :, cols] = value
            kn[head, cols, :HEAD_DIM] = jnp.transpose(key)
            vn[head, cols, :] = jnp.transpose(value)
        return 0

    lax.fori_loop(0, slots // chunk, project_block, 0)
    results = [
        pltpu.make_async_copy(src, dst, local.at[7 + i])
        for i, (src, dst) in enumerate(
            [(xs, x_out), (wq, wq_out), (nt, normed_out), (qt, qt_out), (kt, kt_out),
             (kn, k_out), (vn, v_out)]
        )
    ]
    for copy in results:
        copy.start()

    block = 256

    def attend(head):
        def one(i, _):
            if head == min(1, heads - 1):

                @pl.when(i == slots // block // 2)
                def _():
                    g_w1.forward(place.z_order[0])

            cols = pl.ds(pl.multiple_of(i * block, 128), block)
            scores = dot(kn[head], qt[head, :, cols])
            top = jnp.max(scores, axis=0, keepdims=True)
            exponent = jnp.exp2((scores - top) * QSCALE)
            total = jnp.sum(exponent, axis=0, keepdims=True)
            mixed = dot(vt[head], exponent.astype(BF16)) / total
            mix[place.s, head, :, cols] = mixed.astype(BF16)
            lse_ref[head, :, cols] = top * QSCALE + jnp.log2(total)
            return 0

        lax.fori_loop(0, slots // block, one, 0)

    g_mix = [
        GatherSeq(place, 1 + head, seq_sems, mix.at[place.s, head],
                  lambda s, head=head: mix.at[s, head])
        for head in range(heads)
    ]
    for head in range(heads):
        attend(head)
        g_mix[head].start()
        if head == min(1, heads - 1):
            g_wo.arrive()
            swap_start()
            g_w1.forward(place.z_order[1])
    for k in place.z_order[2:]:
        g_w1.forward(k)
    w2_own = own_rows(place, w2_in)
    w2_ahead = [
        send(w2_own, w2_out.at[i], zsend.at[4, k], zrecv.at[4, k], (place.at_z(k), place.s))
        for i, k in enumerate(place.z_order[:2])
    ]
    for copy in w2_ahead:
        copy.start()
    for head in range(heads):
        for j in range(1, place.ys):
            g_mix[head].arrive_y(j)
    for head in range(heads):
        for j in range(place.ys):
            g_mix[head].arrive_core(j)
    mix_copy = pltpu.make_async_copy(mix, mix_out, local.at[15])
    mix_copy.start()
    g_w1.arrive()
    swap_finish()
    for group in (g_sm, g_wq, g_wo, g_w1, g_x, *g_mix):
        group.drain()
    for copy in (*w2_ahead, w1_own, wo_own, *results, mix_copy):
        copy.wait()


def front(place, lengths, order, x, small, wqkv, wo, w1, w2):
    dp, seq = place.dp, place.seq
    rows = x.shape[0]
    slots = rows * seq
    heads = HEADS // seq
    share, width = wqkv.shape
    anyspace = pl.BlockSpec(memory_space=pl.ANY)
    shapes = [
        (seq, rows, D),
        (16, D),
        (dp, share, width),
        (dp, *wo.shape),
        (dp, *w1.shape),
        (len(place.z_order[:2]), FF // (dp * seq), D),
        (D, slots),
        (heads, 128, slots),
        (heads, HEAD_DIM, slots),
        (heads, slots, 128),
        (heads, slots, HEAD_DIM),
        (seq, heads, HEAD_DIM, slots),
    ]
    vm = lambda *shape: pltpu.VMEM(shape, BF16)
    return pl.pallas_call(
        functools.partial(front_kernel, place),
        in_specs=[pl.BlockSpec(memory_space=pltpu.SMEM)] * 2 + [anyspace] * 6,
        out_specs=[anyspace, pl.BlockSpec(memory_space=pltpu.VMEM)]
        + [anyspace] * (len(shapes) - 2)
        + [pl.BlockSpec(memory_space=pltpu.VMEM)],
        out_shape=[
            jax.ShapeDtypeStruct(shape, F32 if i == 1 else BF16) for i, shape in enumerate(shapes)
        ]
        + [jax.ShapeDtypeStruct((heads, 1, slots), F32)],
        scratch_shapes=[
            vm(seq, rows, D),
            vm(slots, D),
            vm(D, slots),
            pltpu.VMEM((8, heads * HEAD_DIM), F32),
            pltpu.VMEM((dp, *small.shape), F32),
            vm(dp, share, width),
            vm(width, D),
            vm(heads, 128, slots),
            vm(heads, HEAD_DIM, slots),
            vm(heads, HEAD_DIM, slots),
            vm(heads, slots, 128),
            vm(heads, slots, HEAD_DIM),
            vm(seq, heads, HEAD_DIM, slots),
        ]
        + dp_semaphores(place, 5)
        + seq_semaphores(place, 1 + heads)
        + [pltpu.SemaphoreType.DMA((place.zs, place.xs))] * 2
        + [pltpu.SemaphoreType.DMA((16,))],
        compiler_params=params(collective_id=0, has_side_effects=True),
        name="front",
    )(lengths, order, x, small, wqkv, wo, w1, w2)


class ScatterSeq:
    def __init__(self, place, group, sems, part, from_core, from_y):
        self.p, self.g, self.part, self.from_core, self.from_y = place, group, part, from_core, from_y
        self.sends, self.recvs = sems

    def core_copy(self, j):
        place = self.p
        return send(self.part(place.at_y(j, 1 - place.c)), self.from_core(j),
                    self.sends.at[self.g, 1, j], self.recvs.at[self.g, 1, j],
                    (place.d, place.partner))

    def y_copy(self, j, src):
        place = self.p
        return send(src, self.from_y(j), self.sends.at[self.g, 0, j], self.recvs.at[self.g, 0, j],
                    (place.d, place.at_y(j, place.c)))


class ScatterDp:
    def __init__(self, place, group, sems, out, part, from_x, from_z):
        self.p, self.g, self.out, self.part = place, group, out, part
        self.from_x, self.from_z = from_x, from_z
        self.zsend, self.zrecv, self.xsend, self.xrecv = sems
        self.order = place.z_order + [0]

    def block(self, k, j):
        place = self.p
        return lax.rem(place.z + k, place.zs) * place.xs + lax.rem(place.x + j, place.xs)

    def x_copy(self, j, k):
        return send(self.out(k, j, self.block(k, j)), self.from_x(j - 1, k),
                    self.xsend.at[self.g, k, j], self.xrecv.at[self.g, k, j],
                    (self.p.at_x(j), self.p.s))

    def start_x(self, steps=None):
        for k in self.order if steps is None else steps:
            for j in range(1, self.p.xs):
                self.x_copy(j, k).start()

    def z_copy(self, k):
        return send(self.part(k, self.block(k, 0)), self.from_z(k - 1),
                    self.zsend.at[self.g, k], self.zrecv.at[self.g, k], (self.p.at_z(k), self.p.s))

    def fold_x(self, k):
        own = self.part(k, self.block(k, 0))
        value = own[...].astype(F32)
        for j in range(1, self.p.xs):
            self.x_copy(j, k).wait_recv()
            value = value + self.from_x(j - 1, k)[...].astype(F32)
        own[...] = value.astype(own.dtype)

    def fold(self, k):
        self.fold_x(k)
        if k:
            self.z_copy(k).start()

    def fold_all(self):
        for k in self.order:
            self.fold(k)

    def finish(self):
        value = self.part(0, self.block(0, 0))[...].astype(F32)
        for k in range(1, self.p.zs):
            self.z_copy(k).wait_recv()
            value = value + self.from_z(k - 1)[...].astype(F32)
        return value.astype(self.part(0, self.block(0, 0)).dtype)

    def drain_x(self, steps=None):
        for k in self.order if steps is None else steps:
            for j in range(1, self.p.xs):
                self.x_copy(j, k).wait_send()

    def drain_z(self):
        for k in self.p.z_order:
            self.z_copy(k).wait_send()

    def drain(self):
        self.drain_x()
        self.drain_z()


def split_steps(place):
    order = place.z_order + [0]
    return order[: place.zs // 2], order[place.zs // 2 :]


def whole_tiles(*heights):
    return all(height % 16 == 0 for height in heights)


def feed_kernel(
    place, lengths_ref, order_ref, x_in, mix_in, cot_in, wo_in, w1_in, w2_in, ahead_in, vec_ref,
    gb_out, middle_out, grad_out, part_out, g1_out, s2_ref, sums_ref,
    xa, mixv, gv, wo, w1, w2, second, act, slope, unit, ds, own, from_core, from_y,
    from_x1, from_x2, from_z2, *rest,
):
    zsend, zrecv, xsend, xrecv, ssend, srecv, local = rest[-7:]
    gb = xa
    place.locate()
    seq, rows, _ = x_in.shape
    slots = seq * rows
    chunk = chunk_of(slots)
    joined = chunk // rows
    width = w1.shape[1]
    share = D // place.dp
    units = width // place.dp
    place.barrier()
    dp_sems = (zsend, zrecv, xsend, xrecv)
    seq_sems = (ssend, srecv)
    aligned = whole_tiles(share, units)
    if aligned:
        w2_part = lambda d: w2.at[pl.ds(pl.multiple_of(d * units, 16), units), :]
        g2_part = lambda d: wo.at[pl.ds(pl.multiple_of(d * units, 16), units), :]
        g1_part = lambda d: w1.at[pl.ds(pl.multiple_of(d * share, 16), share), :]
    else:
        w2_split, g2_split, g1_split = rest[:3]
        w2_part, g2_part = (lambda d: w2_split.at[d]), (lambda d: g2_split.at[d])
        g1_part = lambda d: g1_split.at[d]
    w2_in = own_rows(place, w2_in)
    ahead = [ahead_in.at[i] for i in range(len(place.z_order[:2]))]
    gather = GatherDp(place, 0, dp_sems, w2_in, w2_part, ahead=ahead)
    cots = GatherSeq(place, 2, seq_sems, cot_in, lambda s: gv.at[s])
    gather.start_x()
    gather.start_z()
    cots.start()
    loads = [
        pltpu.make_async_copy(src, dst, local.at[i])
        for i, (src, dst) in enumerate([(mix_in, mixv), (wo_in, wo), (w1_in, w1), (x_in, xa)])
    ]
    w2_own = pltpu.make_async_copy(w2_in, w2_part(place.d), local.at[5])
    cot_own = pltpu.make_async_copy(cot_in, gv.at[place.s], local.at[6])
    w2_ready = [
        pltpu.make_async_copy(src, w2_part(gather.p.block(k, 0)), local.at[7 + i])
        for i, (k, src) in enumerate(gather.ahead.items())
    ]
    for copy in (*loads, w2_own, cot_own, *w2_ready):
        copy.start()
    gain, shift, bias_out, bias1 = vec_ref[3:4], vec_ref[4:5], vec_ref[2:3], vec_ref[6:7, :width]
    own_chunk = place.s // joined
    sums_ref[...] = jnp.zeros_like(sums_ref)
    for copy in loads:
        copy.wait()

    def lines_of(index, size, step=16):
        return pl.ds(pl.multiple_of(index * size, step), size)

    def forward(i, _):
        lines = lines_of(i, chunk)
        hidden = xa[pl.ds(i * joined, joined)].reshape(chunk, D).astype(F32)
        cols = pl.ds(pl.multiple_of(i * chunk, 128), chunk)
        middle = hidden + (dot(mixv[:, cols], wo[...], ((0,), (0,))) + bias_out)

        @pl.when(i == own_chunk)
        def _():
            own[...] = middle

        normal, _ = normalize(middle)
        unit[lines, :] = normal.astype(BF16)
        tokens = (normal * gain + shift).astype(BF16)
        second[lines, :] = tokens
        expanded = dot(tokens, w1[...]) + bias1
        phi = 0.5 * (1.0 + lax.erf(expanded * (0.5**0.5)))
        act[lines, :] = (expanded * phi).astype(BF16)
        density = jnp.exp(-0.5 * expanded * expanded) * 0.3989422804014327
        slope[lines, :] = (phi + expanded * density).astype(BF16)
        @pl.when(i == slots // chunk - 1)
        def _():
            for k in gather.rest[:1]:
                gather.forward(k)

        return 0

    lax.fori_loop(0, slots // chunk, forward, 0)
    cot_own.wait()
    for j in range(1, place.ys):
        cots.arrive_y(j)
    for j in range(place.ys):
        cots.arrive_core(j)
    cots.drain()

    length = own_length(lengths_ref, order_ref)

    def mask(i, _):
        valid = i * chunk + lax.broadcasted_iota(jnp.int32, (chunk, 1), 0) < length
        cot = gv[pl.ds(i * joined, joined)].reshape(chunk, D)
        gv[pl.ds(i * joined, joined)] = jnp.where(valid, cot.astype(F32), 0.0).astype(BF16).reshape(
            joined, rows, D
        )
        return 0

    lax.fori_loop(0, slots // chunk, mask, 0)

    step = 256 if width % 256 == 0 else 128

    def w2_grad(i, _):
        cols = pl.ds(pl.multiple_of(i * step, 128), step)
        value = dot(act[:, cols], gv[...].reshape(slots, D), ((0,), (0,)))
        wo[pl.ds(pl.multiple_of(i * step, 128), step), :] = value.astype(BF16)
        return 0

    lax.fori_loop(0, width // step, w2_grad, 0)
    for k in gather.rest[1:]:
        gather.forward(k)
    if not aligned:
        for d in range(place.dp):
            g2_split[d] = wo[d * units : (d + 1) * units, :]
    r2 = ScatterDp(place, 1, dp_sems, lambda k, j, d: g2_part(d), lambda k, d: g2_part(d),
                   lambda j, k: from_x2.at[j, k], lambda k: from_z2.at[k])
    r2.start_x()
    for copy in (w2_own, *w2_ready):
        copy.wait()
    gather.arrive()
    if not aligned:
        for d in range(place.dp):
            w2[d * units : (d + 1) * units, :] = w2_split[d]

    scatter = ScatterSeq(place, 0, seq_sems, lambda s: ds.at[s], lambda j: from_core.at[j],
                         lambda j: from_y.at[j - 1])
    def backward(i):
        lines = lines_of(i, chunk)
        grad_two = gv[pl.ds(i * joined, joined)].reshape(chunk, D)
        grad_act = dot(grad_two, w2[...], ((1,), (1,)))
        grad_expanded = (grad_act * slope[lines, :].astype(F32)).astype(BF16)
        slope[lines, :] = grad_expanded
        grad_second = dot(grad_expanded, w1[...], ((1,), (1,)))
        ds[pl.ds(i * joined, joined)] = grad_second.astype(BF16).reshape(joined, rows, D)
        sums_ref[3:4] += jnp.sum(grad_second * unit[lines, :].astype(F32), axis=0, keepdims=True)
        sums_ref[4:5] += jnp.sum(grad_second, axis=0, keepdims=True)
        sums_ref[7:8, :width] += jnp.sum(grad_expanded.astype(F32), axis=0, keepdims=True)

    def fold_y(j):
        block = place.at_y(j, place.c)
        scatter.core_copy(j).wait_recv()
        ds[block] = (ds[block].astype(F32) + from_core[j].astype(F32)).astype(BF16)
        scatter.y_copy(j, ds.at[block]).start()

    turns = list(r2.order[:-1])
    for j in list(range(1, place.ys)) + [0]:
        if joined == 1:
            backward(place.at_y(j, 1 - place.c))
            scatter.core_copy(j).start()
            backward(place.at_y(j, place.c))
        else:
            backward(lax.rem(place.y + j, place.ys))
            scatter.core_copy(j).start()
        if j:
            fold_y(j)

    gather.drain()
    r2.fold(turns.pop(0))

    def w1_grad(i, _):
        cols = pl.ds(pl.multiple_of(i * 256, 128), 256)
        value = dot(second[:, cols], slope[...], ((0,), (0,)))
        keep1[pl.ds(pl.multiple_of(i * 256, 128), 256), :] = value.astype(BF16)
        return 0

    keep1 = w1
    lax.fori_loop(0, D // 256, w1_grad, 0)
    if not aligned:
        for d in range(place.dp):
            g1_split[d] = w1[d * share : (d + 1) * share, :]
    r1 = ScatterDp(place, 2, dp_sems, lambda k, j, d: g1_part(d), lambda k, d: g1_part(d),
                   lambda j, k: from_x1.at[j, k], None)
    early, late = split_steps(place)
    r1.start_x(early)
    keep = [
        pltpu.make_async_copy(
            g1_part(r1.block(k, j)), g1_out.at[k, j], local.at[9 + seq + k * place.xs + j]
        )
        for k in late
        for j in range(place.xs)
    ]
    for copy in keep:
        copy.start()
    for k in turns:
        r2.fold(k)

    scatter.core_copy(0).wait_recv()
    value = ds[place.s].astype(F32) + from_core[0].astype(F32)
    for j in range(1, place.ys):
        scatter.y_copy(j, ds.at[place.s]).wait_recv()
        value = value + from_y[j - 1].astype(F32)
    mine = pl.ds(pl.multiple_of(lax.rem(place.s, joined) * rows, 8), rows)
    middle = own[mine, :]
    normal, spread = normalize(middle)
    grad_two = gv[place.s].astype(F32)
    grad_middle = grad_two + norm_backward(normal, spread, value * gain)
    branch = grad_middle.astype(BF16)
    gb[place.s] = branch
    sums_ref[5:6] = jnp.sum(grad_two, axis=0, keepdims=True)
    sums_ref[2:3] = jnp.sum(branch.astype(F32), axis=0, keepdims=True)
    spread_out = GatherSeq(place, 1, seq_sems, gb.at[place.s], lambda s: gb.at[s])
    spread_out.start()
    middle_out[...] = middle
    grad_out[...] = grad_middle

    def emit(i, _):
        lines = lines_of(i, chunk)
        unit[lines, :] = dot(act[lines, :], w2[...]).astype(BF16)
        return 0

    lax.fori_loop(0, slots // chunk, emit, 0)
    keep_parts = [
        pltpu.make_async_copy(
            unit.at[pl.ds(i * rows, rows), :], part_out.at[i], local.at[9 + i]
        )
        for i in range(seq)
    ]
    for copy in keep_parts:
        copy.start()
    r2.fold(0)
    for k in early:
        r1.fold_x(k)
        keep.append(
            pltpu.make_async_copy(
                g1_part(r1.block(k, 0)), g1_out.at[k, 0], local.at[9 + seq + k * place.xs]
            )
        )
        keep[-1].start()
    for j in range(1, place.ys):
        spread_out.arrive_y(j)
    s2_ref[...] = r2.finish()
    for j in range(place.ys):
        spread_out.arrive_core(j)
    save = pltpu.make_async_copy(gb, gb_out, local.at[8])
    save.start()
    for j in range(place.ys):
        scatter.core_copy(j).wait_send()
    for j in range(1, place.ys):
        scatter.y_copy(j, ds.at[place.s]).wait_send()
    spread_out.drain()
    r2.drain()
    r1.drain_x(early)
    for copy in (*keep_parts, *keep, save):
        copy.wait()


def feed(place, lengths, order, x, mix, cot, wo, w1, w2, ahead, vectors):
    seq, rows, _ = x.shape
    slots = seq * rows
    chunk = chunk_of(slots)
    width = w1.shape[1]
    share, units = D // place.dp, width // place.dp
    split = []
    anyspace = pl.BlockSpec(memory_space=pl.ANY)
    inside = pl.BlockSpec(memory_space=pltpu.VMEM)
    vm = lambda *shape: pltpu.VMEM(shape, BF16)
    if not whole_tiles(share, units):
        split = [
            vm(place.dp, units, D), vm(place.dp, units, D), vm(place.dp, share, width),
        ]
    outs = [
        ((seq, rows, D), BF16, anyspace),
        ((rows, D), F32, inside),
        ((rows, D), F32, inside),
        ((seq, rows, D), BF16, anyspace),
        ((place.zs, place.xs, share, width), BF16, anyspace),
        ((units, D), BF16, inside),
        ((8, D), F32, inside),
    ]
    return pl.pallas_call(
        functools.partial(feed_kernel, place),
        in_specs=[pl.BlockSpec(memory_space=pltpu.SMEM)] * 2 + [anyspace] * 7 + [inside],
        out_specs=[spec for _, _, spec in outs],
        out_shape=[jax.ShapeDtypeStruct(shape, kind) for shape, kind, _ in outs],
        scratch_shapes=[
            vm(seq, rows, D),
            vm(D, slots),
            vm(seq, rows, D),
            vm(D, D),
            vm(D, width),
            vm(width, D),
            vm(slots, D),
            vm(slots, width),
            vm(slots, width),
            vm(slots, D),
            vm(seq, rows, D),
            pltpu.VMEM((chunk, D), F32),
            vm(place.ys, rows, D),
            vm(max(place.ys - 1, 1), rows, D),
            vm(max(place.xs - 1, 1), place.zs, share, width),
            vm(max(place.xs - 1, 1), place.zs, units, D),
            vm(place.zs - 1, units, D),
        ]
        + split
        + dp_semaphores(place, 3)
        + seq_semaphores(place, 3)
        + [pltpu.SemaphoreType.DMA((9 + seq + place.dp,))],
        compiler_params=params(collective_id=1, has_side_effects=True),
        name="feed",
    )(lengths, order, x, mix, cot, wo, w1, w2, ahead, vectors)


def tail_kernel(
    place, vec_ref, sums_ref, lse_ref, middle_ref, gmid_ref,
    qt_in, kt_in, k_in, v_in, gb_in, mix_in, wo_in, wq_in, normed_in, x_in, part_in, g1_in, s2_in,
    layer_ref, input_ref, total_ref, w1_out, w2_out, wq_out, wo_out,
    qt, kt, kn, vn, got, gbv, mixv, normed, wq, dqkv, wo_rows, gbs, dk_sum, dv_sum, xbuf, outp,
    core_a, y_a, core_b, y_b, pq, ours, po, p1, x1, xq, xo, zq, zo, z1, r1, r2, rq, ro,
    line, ps, xsm, zsm, hop, far, *rest,
):
    zsend, zrecv, xsend, xrecv, ssend, srecv, local = rest[-7:]
    place.locate()
    seq, rows, _ = x_in.shape
    slots = seq * rows
    chunk = chunk_of(slots)
    joined = chunk // rows
    count = slots // chunk
    heads = kt.shape[0]
    wide = heads * HEAD_DIM
    share = D // place.dp
    units = s2_in.shape[0]
    place.barrier()
    dp_sems, seq_sems = (zsend, zrecv, xsend, xrecv), (ssend, srecv)
    e1 = gbv
    triple = 3 * HEAD_DIM
    groups = pq.shape[0]
    each = heads // groups
    if whole_tiles(share):
        q_part = lambda h, d: pq.at[h, pl.ds(pl.multiple_of(d * share, 16), share), :]
        o_part = lambda d: po.at[pl.ds(pl.multiple_of(d * share, 16), share), :]
    else:
        pq_split, po_split = rest[:2]
        q_part, o_part = (lambda h, d: pq_split.at[h, d]), (lambda d: po_split.at[d])
    early, late = split_steps(place)
    g1 = ScatterDp(place, 0, dp_sems, lambda k, j, d: g1_in.at[k, j],
                   lambda k, d: p1.at[late.index(k)] if k in late else g1_in.at[k, 0],
                   lambda j, k: x1.at[j, late.index(k)], lambda k: z1.at[k])
    go = ScatterDp(place, 1, dp_sems, lambda k, j, d: o_part(d), lambda k, d: o_part(d),
                   lambda j, k: xo.at[j, k], lambda k: zo.at[k])
    small = ScatterDp(place, 2, dp_sems, lambda k, j, d: ps.at[d], lambda k, d: ps.at[d],
                      lambda j, k: xsm.at[j, k], lambda k: zsm.at[k])
    gq = [
        ScatterDp(place, 3 + h, dp_sems, lambda k, j, d, h=h: q_part(h, d),
                  lambda k, d, h=h: q_part(h, d), lambda j, k, h=h: xq.at[h, j, k],
                  lambda k, h=h: zq.at[h, k])
        for h in range(groups)
    ]
    out_sum = ScatterSeq(place, 0, seq_sems, lambda s: part_in.at[s], lambda j: core_a.at[j],
                         lambda j: y_a.at[j - 1])
    e1_sum = ScatterSeq(place, 1, seq_sems, lambda s: e1.at[s], lambda j: core_b.at[j],
                        lambda j: y_b.at[j - 1])
    final2 = GatherSeq(place, 2, seq_sems, r2, lambda s: w2_out.at[s])
    final1 = GatherSeq(place, 3, seq_sems, r1, lambda s: w1_out.at[s])
    final_o = GatherSeq(place, 4, seq_sems, ro, lambda s: wo_out.at[s])
    final_q = [
        GatherSeq(place, 7 + h, seq_sems, rq.at[h], lambda s, h=h: wq_out.at[s, h])
        for h in range(groups)
    ]

    first = [(gb_in, gbv), (wo_in.at[pl.ds(pl.multiple_of(place.s * wide, 16), wide), :], wo_rows),
             (mix_in, mixv), (qt_in, qt), (kt_in, kt), (k_in, kn), (v_in, vn)]
    later = [(normed_in, normed), (wq_in, wq)]
    later += [(s2_in, r2)] + [(g1_in.at[k, 0], p1.at[i]) for i, k in enumerate(late)]
    later += [(part_in.at[place.at_y(j, place.c)], outp.at[j]) for j in range(place.ys)]
    loads = [
        pltpu.make_async_copy(src, dst, local.at[i]) for i, (src, dst) in enumerate(first + later)
    ]
    free = len(loads)
    for copy in loads:
        copy.start()
    for k in early:
        g1.z_copy(k).start()
    g1.start_x(late)
    for j in list(range(1, place.ys)) + [0]:
        out_sum.core_copy(j).start()
    for copy in loads[:2]:
        copy.wait()

    def lines_of(index, size, step=16):
        return pl.ds(pl.multiple_of(index * size, step), size)

    def turn(i, _):
        cols = pl.ds(pl.multiple_of(i * chunk, 128), chunk)
        branch = gbv[pl.ds(i * joined, joined)].reshape(chunk, D)
        got[:, cols] = dot(wo_rows[...], branch, ((1,), (1,))).astype(BF16)
        for s in range(seq):

            @pl.when(place.s == s)
            def _():
                gbs[lines_of(i, chunk), :] = branch[:, s * wide : (s + 1) * wide]

        return 0

    lax.fori_loop(0, count, turn, 0)
    loads[2].wait()

    def wo_grad(i, _):
        lines = pl.ds(pl.multiple_of(i * 256, 128), 256)
        po[lines, :] = dot(mixv[lines, :], gbs[...]).astype(BF16)
        return 0

    lax.fori_loop(0, D // 256, wo_grad, 0)
    if not whole_tiles(share):
        for d in range(place.dp):
            po_split[d] = po[d * share : (d + 1) * share, :]
    go.start_x()

    block = 256

    def head_back(head):
        part = slice(head * HEAD_DIM, (head + 1) * HEAD_DIM)
        first = head * triple
        dk_sum[...] = jnp.zeros_like(dk_sum)
        dv_sum[...] = jnp.zeros_like(dv_sum)

        def one(i, _):
            cols = pl.ds(pl.multiple_of(i * block, 128), block)
            grad = got[part, cols]
            own_rows = pl.ds(pl.multiple_of(place.s * wide + head * HEAD_DIM, 16), HEAD_DIM)
            mixed = mixv[own_rows, cols]
            delta = jnp.sum(grad.astype(F32) * mixed.astype(F32), axis=0, keepdims=True)
            probs = jnp.exp2(dot(kn[head], qt[head, :, cols]) * QSCALE - lse_ref[head, :, cols])
            grad_scores = (probs * (dot(vn[head], grad) - delta)).astype(BF16)
            dv_sum[...] += dot(probs.astype(BF16), grad, ((1,), (1,)))
            dk_sum[...] += dot(grad_scores, qt[head, :HEAD_DIM, cols], ((1,), (1,)))
            turned = dot(kt[head], grad_scores) * SCALE
            lines = pl.ds(pl.multiple_of(i * block, 128), block)
            dqkv[lines, first : first + HEAD_DIM] = jnp.transpose(turned).astype(BF16)
            return 0

        lax.fori_loop(0, slots // block, one, 0)
        dqkv[:, first + HEAD_DIM : first + 2 * HEAD_DIM] = (dk_sum[...] * SCALE).astype(BF16)
        dqkv[:, first + 2 * HEAD_DIM : first + triple] = dv_sum[...].astype(BF16)

    def q_grads(group):
        ours[...] = dqkv[:, group * each * triple : (group + 1) * each * triple]

        def q_grad(i, _):
            lines = pl.ds(pl.multiple_of(i * 256, 128), 256)
            pq[group, lines, :] = dot(normed[lines, :], ours[...]).astype(BF16)
            return 0

        lax.fori_loop(0, D // 256, q_grad, 0)
        if not whole_tiles(share):
            for d in range(place.dp):
                pq_split[group, d] = pq[group, d * share : (d + 1) * share, :]
        gq[group].start_x()

    def out_fold():
        for j in range(1, place.ys):
            out_sum.core_copy(j).wait_recv()
            outp[j] = (outp[j].astype(F32) + core_a[j].astype(F32)).astype(BF16)
            out_sum.y_copy(j, outp.at[j]).start()

    def publish(group, result, final):
        result[...] = group.finish()
        final.start()

    for copy in loads[3:]:
        copy.wait()
    out_fold()
    final2.start()
    for head in range(heads):
        head_back(head)
        if head == 0:
            for k in late:
                g1.fold(k)
        if head == min(1, heads - 1):
            go.fold_all()
        if (head + 1) % each == 0:
            q_grads(head // each)
        if head == min(2, heads - 1):
            publish(g1, r1, final1)
        if head == heads - 1:
            for group in range(groups - 1):
                gq[group].fold_all()
            publish(go, ro, final_o)

    line[...] = jnp.zeros_like(line)
    line[0:6] = sums_ref[0:6]
    bias_sum = jnp.sum(dqkv[...].astype(F32), axis=0, keepdims=True)
    for s in range(seq):

        @pl.when(place.s == s)
        def _():
            for head in range(heads):
                to = slice(s * wide + head * HEAD_DIM, s * wide + (head + 1) * HEAD_DIM)
                at = head * triple
                line[6:7, to] = bias_sum[:, at : at + HEAD_DIM]
                line[7:8, to] = bias_sum[:, at + 2 * HEAD_DIM : at + triple]

    order = []
    for j in list(range(1, place.ys)) + [0]:
        if joined == 1:
            order += [(place.at_y(j, 1 - place.c), j, False), (place.at_y(j, place.c), j, True)]
        else:
            order += [(lax.rem(place.y + j, place.ys), j, True)]

    def x_load(at, slot):
        return pltpu.make_async_copy(
            x_in.at[pl.ds(at * joined, joined)], xbuf.at[slot], local.at[free + slot]
        )

    x_load(order[0][0], 0).start()
    last_folds = list(gq[groups - 1].order)
    for step, (at, j, both) in enumerate(order):
        slot = step % 2
        if step + 1 < len(order):
            x_load(order[step + 1][0], 1 - slot).start()
        x_load(at, slot).wait()
        grad = dot(dqkv[lines_of(at, chunk), :], wq[...].reshape(D, 3 * wide), ((1,), (1,)))
        normal, spread = normalize(xbuf[slot].reshape(chunk, D).astype(F32))
        line[0:1] += jnp.sum(grad * normal, axis=0, keepdims=True)
        line[1:2] += jnp.sum(grad, axis=0, keepdims=True)
        e1[pl.ds(at * joined, joined)] = grad.astype(BF16).reshape(joined, rows, D)
        if joined == 2 or not both:
            e1_sum.core_copy(j).start()
        if both and j:
            target = place.at_y(j, place.c)
            e1_sum.core_copy(j).wait_recv()
            e1[target] = (e1[target].astype(F32) + core_b[j].astype(F32)).astype(BF16)
            e1_sum.y_copy(j, e1.at[target]).start()
        if both and len(last_folds) > 2:
            gq[groups - 1].fold(last_folds.pop(0))
    for d in range(place.dp):
        ps[d] = jnp.zeros_like(ps[d])
        ps[d, 0:8] = line[:, d * share : (d + 1) * share]
        ps[d, pl.ds(8 + place.s, 1), :units] = sums_ref[7:8, d * units : (d + 1) * units]
    small.start_x()
    for k in last_folds:
        gq[groups - 1].fold(k)
    small.fold_all()
    for group in range(groups - 1):
        publish(gq[group], rq.at[group], final_q[group])
    value = outp[0].astype(F32)
    out_sum.core_copy(0).wait_recv()
    value = value + core_a[0].astype(F32)
    for j in range(1, place.ys):
        out_sum.y_copy(j, outp.at[j]).wait_recv()
        value = value + y_a[j - 1].astype(F32)
    layer_ref[...] = (middle_ref[...] + (value + vec_ref[5:6])).astype(BF16)

    hop[0] = small.finish()
    near = send(hop.at[0], far.at[0], ssend.at[5, 1, 0], srecv.at[5, 1, 0],
                (place.d, place.partner))
    near.start()
    for final in (final2, final1, final_o):
        for j in range(1, place.ys):
            final.arrive_y(j)
    near.wait_recv()
    hop[1] = hop[0] + far[0]
    across = [
        send(hop.at[1], far.at[j], ssend.at[5, 0, j], srecv.at[5, 0, j],
             (place.d, place.at_y(j, place.c)))
        for j in range(1, place.ys)
    ]
    for copy in across:
        copy.start()
    keep = [
        pltpu.make_async_copy(src, dst.at[place.s], local.at[free + 2 + i])
        for i, (src, dst) in enumerate([(r1, w1_out), (r2, w2_out), (ro, wo_out), (rq, wq_out)])
    ]
    for copy in keep[:3]:
        copy.start()
    publish(gq[groups - 1], rq.at[groups - 1], final_q[groups - 1])
    keep[3].start()

    value = e1[place.s].astype(F32)
    e1_sum.core_copy(0).wait_recv()
    value = value + core_b[0].astype(F32)
    for j in range(1, place.ys):
        e1_sum.y_copy(j, e1.at[place.s]).wait_recv()
        value = value + y_b[j - 1].astype(F32)
    last = (len(order) - 1) % 2
    hidden = xbuf[last, lax.rem(place.s, joined)].astype(F32)
    normal, spread = normalize(hidden)
    input_ref[...] = (gmid_ref[...] + norm_backward(normal, spread, value * vec_ref[0:1])).astype(
        BF16
    )
    for final in final_q:
        for j in range(1, place.ys):
            final.arrive_y(j)
    value = hop[1]
    for j, copy in enumerate(across):
        copy.wait_recv()
        value = value + far[j + 1]
    total_ref[...] = value
    finals = (final1, final2, final_o, *final_q)
    for final in finals:
        for j in range(place.ys):
            final.arrive_core(j)
    for final in finals:
        final.drain()
    for group in (out_sum, e1_sum):
        for j in range(place.ys):
            group.core_copy(j).wait_send()
        for j in range(1, place.ys):
            group.y_copy(j, outp.at[j]).wait_send()
    for group in (*gq, go, small):
        group.drain()
    g1.drain_x(late)
    g1.drain_z()
    for copy in (near, *across):
        copy.wait_send()
    for copy in keep:
        copy.wait()


def tail(place, vectors, sums, lse, middle, gmid, qt, kt, kn, vn, gb, mix, wo, wq, normed, x, part, g1, s2):
    seq, rows, _ = x.shape
    slots = seq * rows
    chunk = chunk_of(slots)
    joined = chunk // rows
    heads = kt.shape[0]
    wide = heads * HEAD_DIM
    share = D // place.dp
    width, units = g1.shape[3], s2.shape[0]
    ys, xs, zs = place.ys, max(place.xs - 1, 1), place.zs
    anyspace = pl.BlockSpec(memory_space=pl.ANY)
    inside = pl.BlockSpec(memory_space=pltpu.VMEM)
    vm = lambda *shape: pltpu.VMEM(shape, BF16)
    tall = 16
    each = 2 if heads % 2 == 0 else 1
    groups, triple = heads // each, 3 * HEAD_DIM * each
    outs = [
        ((rows, D), BF16, inside),
        ((rows, D), BF16, inside),
        ((tall, share), F32, inside),
        ((seq, share, width), BF16, anyspace),
        ((seq, units, D), BF16, anyspace),
        ((seq, groups, share, triple), BF16, anyspace),
        ((seq, share, wide), BF16, anyspace),
    ]
    split = []
    if not whole_tiles(share):
        split = [vm(groups, place.dp, share, triple), vm(place.dp, share, wide)]
    return pl.pallas_call(
        functools.partial(tail_kernel, place),
        in_specs=[inside] * 5 + [anyspace] * 13,
        out_specs=[spec for _, _, spec in outs],
        out_shape=[jax.ShapeDtypeStruct(shape, kind) for shape, kind, _ in outs],
        scratch_shapes=[
            vm(heads, 128, slots),
            vm(heads, HEAD_DIM, slots),
            vm(heads, slots, 128),
            vm(heads, slots, HEAD_DIM),
            vm(wide, slots),
            vm(seq, rows, D),
            vm(D, slots),
            vm(D, slots),
            vm(place.dp, share, 3 * wide),
            vm(slots, 3 * wide),
            vm(wide, D),
            vm(slots, wide),
            pltpu.VMEM((slots, HEAD_DIM), F32),
            pltpu.VMEM((slots, HEAD_DIM), F32),
            vm(2, joined, rows, D),
            vm(ys, rows, D),
            vm(ys, rows, D),
            vm(max(ys - 1, 1), rows, D),
            vm(ys, rows, D),
            vm(max(ys - 1, 1), rows, D),
            vm(groups, D, triple),
            vm(slots, triple),
            vm(D, wide),
            vm(zs - zs // 2, share, width),
            vm(xs, zs - zs // 2, share, width),
            vm(groups, xs, zs, share, triple),
            vm(xs, zs, share, wide),
            vm(groups, zs - 1, share, triple),
            vm(zs - 1, share, wide),
            vm(zs - 1, share, width),
            vm(share, width),
            vm(units, D),
            vm(groups, share, triple),
            vm(share, wide),
            pltpu.VMEM((8, D), F32),
            pltpu.VMEM((place.dp, tall, share), F32),
            pltpu.VMEM((xs, zs, tall, share), F32),
            pltpu.VMEM((zs - 1, tall, share), F32),
            pltpu.VMEM((2, tall, share), F32),
            pltpu.VMEM((ys, tall, share), F32),
        ]
        + split
        + dp_semaphores(place, 3 + heads)
        + seq_semaphores(place, 7 + heads)
        + [pltpu.SemaphoreType.DMA((24 + ys,))],
        compiler_params=params(collective_id=2, has_side_effects=True),
        name="tail",
    )(vectors, sums, lse, middle, gmid, qt, kt, kn, vn, gb, mix, wo, wq, normed, x, part, g1, s2)


def prep_kernel(place, q_ref, k_ref, v_ref, w1_ref, b1_ref, *refs):
    *vec_refs, small_ref, wqkv_ref, w1_out = refs
    place.locate()
    dp, seq = place.dp, place.seq
    wide = D // seq
    units = FF // (dp * seq)
    small_ref[...] = jnp.zeros_like(small_ref)
    for i, ref in zip((0, 1, 2, 3, 4, 5, 7, 8), vec_refs):
        small_ref[i : i + 1, :] = ref[...].astype(F32).reshape(1, D // dp)
    b1 = b1_ref[...].astype(F32).reshape(1, FF // dp)
    for s in range(seq):

        @pl.when(place.s == s)
        def _():
            small_ref[6:7, :units] = b1[:, s * units : (s + 1) * units]
            for i, ref in enumerate((q_ref, k_ref, v_ref)):
                for head in range(wide // HEAD_DIM):
                    to = (3 * head + i) * HEAD_DIM
                    at = s * wide + head * HEAD_DIM
                    wqkv_ref[:, to : to + HEAD_DIM] = ref[:, at : at + HEAD_DIM]
            for d in range(dp):
                first = d * (FF // dp) + s * units
                w1_out[:, d * units : (d + 1) * units] = w1_ref[:, first : first + units]


def prep(place, q, k, v, w1, b1, *vectors):
    wide = D // place.seq
    share = q.shape[0]
    inside = pl.BlockSpec(memory_space=pltpu.VMEM)
    return pl.pallas_call(
        functools.partial(prep_kernel, place),
        in_specs=[inside] * (5 + len(vectors)),
        out_specs=[inside] * 3,
        out_shape=[
            jax.ShapeDtypeStruct((16, share), F32),
            jax.ShapeDtypeStruct((share, 3 * wide), BF16),
            jax.ShapeDtypeStruct((share, FF // place.seq), BF16),
        ],
        compiler_params=params(),
        name="prep",
    )(q, k, v, w1, b1, *vectors)


def finish_kernel(
    place, w1_ref, w2_ref, wq_ref, wo_ref, total_ref, layer_ref, input_ref,
    layer_out, input_out, w1_out, w2_out, q_out, k_out, v_out, wo_out, g1_out, s1_out, bo_out, g2_out, s2_out, b2_out,
    bq_out, bv_out, b1_out, line,
):
    place.locate()
    dp, seq = place.dp, place.seq
    share = D // dp
    wide = D // seq
    units = FF // (dp * seq)
    each = wide // HEAD_DIM // wq_ref.shape[1]
    w2_out[...] = w2_ref[...].astype(F32)
    for s in range(seq):
        cols = slice(s * wide, (s + 1) * wide)
        for head in range(wide // HEAD_DIM):
            to = slice(s * wide + head * HEAD_DIM, s * wide + (head + 1) * HEAD_DIM)
            for i, out in enumerate((q_out, k_out, v_out)):
                first = ((head % each) * 3 + i) * HEAD_DIM
                part = wq_ref[s, head // each, :, first : first + HEAD_DIM]
                out[:, to] = part.astype(F32)
        wo_out[:, cols] = wo_ref[s].astype(F32)
        for d in range(dp):
            first = d * (FF // dp) + s * units
            w1_out[:, first : first + units] = w1_ref[s, :, d * units : (d + 1) * units].astype(F32)

    @pl.when(pl.program_id(0) == 0)
    def _():
        layer_out[...] = layer_ref[...]
        input_out[...] = input_ref[...]
        outs = (g1_out, s1_out, bo_out, g2_out, s2_out, b2_out, bq_out, bv_out)
        for i, out in enumerate(outs):
            out[...] = total_ref[i : i + 1].reshape(share)
        for s in range(seq):
            line[:, s * units : (s + 1) * units] = total_ref[8 + s : 9 + s, :units]
        b1_out[...] = line[...].reshape(FF // dp)


def finish(place, w1, w2, wq, wo, totals, layer, grad):
    dp, seq = place.dp, place.seq
    share, units, wide = D // dp, w2.shape[1], D // seq
    tile = 32 if share % 32 == 0 and units == share else share
    steps = share // tile
    tall = units // steps
    mat = lambda *tail: pl.BlockSpec((seq, tile, *tail), lambda i: (0, i, 0))
    out = lambda cols: pl.BlockSpec((tile, cols), lambda i: (i, 0))
    small = pl.BlockSpec((share,), lambda i: (0,))
    f32 = lambda *shape: jax.ShapeDtypeStruct(shape, F32)
    return pl.pallas_call(
        functools.partial(finish_kernel, place),
        grid=(steps,),
        in_specs=[
            mat(w1.shape[2]),
            pl.BlockSpec((seq, tall, D), lambda i: (0, i, 0)),
            pl.BlockSpec((seq, wq.shape[1], tile, wq.shape[3]), lambda i: (0, 0, i, 0)),
            mat(wo.shape[2]),
            pl.BlockSpec(totals.shape, lambda i: (0, 0)),
            pl.BlockSpec(layer.shape, lambda i: (0, 0)),
            pl.BlockSpec(layer.shape, lambda i: (0, 0)),
        ],
        out_specs=[pl.BlockSpec(layer.shape, lambda i: (0, 0))] * 2
        + [out(FF), pl.BlockSpec((seq, tall, D), lambda i: (0, i, 0))]
        + [out(D)] * 4
        + [small] * 8
        + [pl.BlockSpec((FF // dp,), lambda i: (0,))],
        out_shape=[jax.ShapeDtypeStruct(layer.shape, BF16)] * 2
        + [f32(share, FF), f32(seq, units, D)]
        + [f32(share, D)] * 4
        + [f32(share)] * 8
        + [f32(FF // dp)],
        scratch_shapes=[pltpu.VMEM((1, FF // dp), F32)],
        compiler_params=params(),
        name="finish",
    )(w1, w2, wq, wo, totals, layer, grad)


def per_device(
    hidden_in, cotangent, clip_lengths, clip_order, first_gain, first_shift, query_weight,
    query_bias, key_weight, value_weight, value_bias, output_weight, output_bias, second_gain,
    second_shift, expand_weight, expand_bias, reduce_weight, reduce_bias,
):
    dp = lax.axis_size("dp")
    seq = lax.axis_size("seq")
    me = lax.axis_index("seq")
    slots = hidden_in.shape[1] * seq
    units = FF // (dp * seq)
    quarter = dp * units

    spot = Place(dp, seq)
    if not whole_tiles(units):
        reduce_weight = lax.dynamic_slice_in_dim(reduce_weight, me * units, units, 0)
    small, wqkv_share, w1_share = prep(
        spot, query_weight, key_weight, value_weight, expand_weight, expand_bias, first_gain,
        first_shift, output_bias, second_gain, second_shift, reduce_bias, query_bias, value_bias,
    )
    x, vectors, w_qkv, w_out, w_expand, w2_ahead, normed, qt, kt, keys, values, mix, lse = front(
        spot, clip_lengths, clip_order, hidden_in[0], small, wqkv_share, output_weight, w1_share,
        reduce_weight,
    )
    w_out = w_out.reshape(D, D)
    w_expand = w_expand.reshape(D, quarter)
    mix = mix.reshape(D, slots)
    grad_branch, middle, grad_middle, out_part, g1, s2, sums = feed(
        spot, clip_lengths, clip_order, x, mix, cotangent[0], w_out, w_expand, reduce_weight,
        w2_ahead, vectors,
    )
    layer_output, input_grad, totals, w1_grad, w2_grad, qkv_grad, wo_grad = tail(
        spot, vectors, sums, lse, middle, grad_middle, qt, kt, keys, values, grad_branch, mix,
        w_out, w_qkv, normed, x, out_part, g1, s2,
    )
    results = finish(
        spot, w1_grad, w2_grad, qkv_grad, wo_grad, totals, layer_output, input_grad
    )
    layer_output, input_grad, *results = results
    (w1_grad, w2_grad, wq_grad, wk_grad, wv_grad, wo_grad) = results[:6]
    g1, s1, bo, g2, s2, b2, bq, bv, b1 = results[6:]
    return (
        layer_output[None], input_grad[None], g1, s1, wq_grad, bq, wk_grad, wv_grad, bv, wo_grad,
        bo, g2, s2, w1_grad, b1, w2_grad.reshape(FF // dp, D), b2,
    )


def solution(mesh):
    clip = P("dp", "seq", None)
    vec = P("dp")
    mat = P("dp", None)
    return jax.shard_map(
        per_device,
        mesh=mesh,
        in_specs=(
            clip, clip, P(), vec, vec, vec, mat, vec, mat, mat, vec, mat, vec, vec, vec, mat, vec,
            mat, vec,
        ),
        out_specs=(
            clip, clip, vec, vec, mat, vec, mat, mat, vec, mat, vec, vec, vec, mat, vec, mat, vec,
        ),
        check_vma=False,
    )
```
